128 devices in a mesh: seq: 16 (over x, y_lo, core), tp: 8 (over z, y_hi).
Axes of the slice: x: 4, y: 4 (y_hi: 2, y_lo: 2; y = y_hi * 2 + y_lo), z: 4, core: 2. Of those that a mesh axis runs over, the one named last changes fastest.
Arguments:
- x_old: bfloat16 [8192, 4608], P('seq', 'tp'), may hold values from -6 to 6
- old_blocks: int32 [16], replicated, may hold values from 1 to 4, 32 in all
- new_blocks: int32 [16], replicated, may hold values from 1 to 4, 32 in all
- order: int32 [16], replicated, may hold values from 0 to 15, as said below
- pre_gain: float32 [4608], replicated, may hold values from 0.25 to 1.75
- post_gain: float32 [4608], replicated, may hold values from 0.25 to 1.75
- w_query: bfloat16 [4608, 4096], P('seq', 'tp'), may hold values from -0.59765625 to 0.59765625
- w_key: bfloat16 [4608, 2048], P('seq', 'tp'), may hold values from -0.09375 to 0.09375
- w_value: bfloat16 [4608, 2048], P('seq', 'tp'), may hold values from -0.09375 to 0.09375
- w_out_t: bfloat16 [4608, 4096], P('seq', 'tp'), may hold values from -0.09375 to 0.09375
Outputs:
- layer_out: bfloat16 [8192, 4608], P(('seq', 'tp'))
The draws below stay inside these ranges and needn't reach their ends.
Inputs may be any that keep to these rules, and one draw needn't show every extreme that they name: `old_blocks`: counts of 128-row blocks, at least one each; they sum to 32, and the largest is exactly 4. `new_blocks`: counts of 128-row blocks, at least one each; they sum to 32, and the largest is exactly 4. A permutation of the seq indices with order[15] = 0 and order[7] = 15; the other indices, taken in increasing order, hold 1 to 14 in increasing order, except that aligned pairs of them (first and second, third and fourth, and so on) are swapped or not, pair by pair.
All inputs are finite; a program needn't handle non-finite values.
Results may differ from the reference program's by a relative error of at most 0.013.
Values may be sent and summed in bfloat16 or wider, within the bound.
A program may use at most 128 MiB of HBM per device.

```python
import math
import jax
import jax.numpy as jnp
import numpy as np
from jax import lax

D = 4608
HEADS = 32
KV_HEADS = 16
HEAD = 128
BLOCK = 128
CAP = 512
TOKENS = 4096
SLOTS = 8192
N_SEQ = 16
N_TP = 8


def draw_order(key, part):
    middle = N_SEQ - 2
    kept = [place for place in range(N_SEQ) if place != N_SEQ - 1 and place != N_SEQ // 2 - 1]
    flips = jax.random.randint(jax.random.fold_in(key, 7), (middle // 2,), 0, 2).astype(jnp.int32)
    ranks = jnp.arange(middle, dtype=jnp.int32)
    shards = (jnp.bitwise_xor(ranks, jnp.repeat(flips, 2)) + 1).astype(jnp.int32)
    result = jnp.zeros((N_SEQ,), jnp.int32)
    result = result.at[jnp.array(kept, dtype=jnp.int32)].set(shards)
    result = result.at[N_SEQ - 1].set(0)
    result = result.at[N_SEQ // 2 - 1].set(N_SEQ - 1)
    return result.astype(jnp.int32)


def block_levels(rng, shape, cuts, least, largest):
    factor_of = 1.0
    for axis_at, shards_of in cuts:
        steps = jax.random.uniform(jax.random.fold_in(jax.random.fold_in(rng, 6), axis_at), (shards_of,), jnp.float32, least / len(cuts), largest / len(cuts))
        factor_of = factor_of * jnp.repeat(jnp.exp(steps), shape[axis_at] // shards_of).reshape((-1,) + (1,) * (len(shape) - 1 - axis_at))
    return factor_of


def split_up(number_of, total, reach, slope):
    portions = [(1 << 20) // math.isqrt(standing ** slope) + 1 for standing in range(2, number_of + 1)]
    rest, holding = total - reach - (number_of - 1), [1] * (number_of - 1)
    while rest > 0:
        movable = [i for i in range(number_of - 1) if holding[i] < reach]
        pool, left = sum([portions[i] for i in movable]), rest
        for i in movable:
            addition = min(reach - holding[i], max(1, left * portions[i] // pool), rest)
            holding[i] = holding[i] + addition
            rest = rest - addition
    return np.array([reach] + holding)


def uneven_parts(rng, number_of, total, reach, skew):
    if number_of == 2:
        one = jax.random.randint(rng, (), max(1, total - reach), min(reach, total - 1) + 1)
        return jnp.stack([one, total - one])
    lengths = jnp.asarray(split_up(number_of, total, reach, skew), jnp.int32)
    twos = (number_of - 1) // 2
    donor, receiver = lengths[1:1 + 2 * twos:2], lengths[2:2 + 2 * twos:2]
    room = jnp.minimum(donor - 1, reach - receiver)
    shifted = jax.random.randint(jax.random.fold_in(rng, 1), (twos,), 0, 1 << 20) % (room + 1)
    lengths = lengths.at[1:1 + 2 * twos:2].set(donor - shifted).at[2:2 + 2 * twos:2].set(receiver + shifted)
    return lengths[jax.random.permutation(jax.random.fold_in(rng, 2), number_of)]


def noise(key, shape, scale, bound, pieces=(), kind=jnp.bfloat16):
    values = jax.random.normal(key, shape, jnp.float32) * scale
    if len(pieces) > 0:
        values = block_levels(key, shape, pieces, -0.22, 0.18) * values
    return jnp.clip(values, min=-bound, max=bound).astype(kind)


def setup_inputs(seed: int = 0) -> dict:
    key_list = jax.random.split(jax.random.key(seed), 11)
    return {
        "x_old": noise(key_list[0], (SLOTS, D), 1.0, 6.0, ((0, 16), (1, 8))),
        "old_blocks": uneven_parts(key_list[1], N_SEQ, TOKENS // BLOCK, CAP // BLOCK, 1).astype(jnp.int32),
        "new_blocks": uneven_parts(key_list[2], N_SEQ, TOKENS // BLOCK, CAP // BLOCK, 2).astype(jnp.int32),
        "order": draw_order(jax.random.fold_in(key_list[10], 71), 0),
        "pre_gain": jnp.clip(1.0 + 0.15 * jax.random.normal(key_list[4], (D,), jnp.float32), 0.25, 1.75),
        "post_gain": jnp.clip(1.0 + 0.15 * jax.random.normal(key_list[5], (D,), jnp.float32), 0.25, 1.75),
        "w_query": noise(key_list[6], (D, HEADS * HEAD), 0.1, 0.59765625, ((0, 16), (1, 8))),
        "w_key": noise(key_list[7], (D, KV_HEADS * HEAD), D ** -0.5, 0.09375, ((0, 16), (1, 8))),
        "w_value": noise(key_list[8], (D, KV_HEADS * HEAD), D ** -0.5, 0.09375, ((0, 16), (1, 8))),
        "w_out_t": noise(key_list[9], (D, HEADS * HEAD), (HEADS * HEAD) ** -0.5, 0.09375, ((0, 16), (1, 8))),
    }


EPS = 1e-06

def offsets(blocks):
    return ((jnp.cumsum(blocks) - blocks) * BLOCK).astype(jnp.int32)

def rotate(values, places):
    half = values.shape[-1] // 2
    inverse = jnp.exp(jnp.arange(half, dtype=jnp.float32) * (-2.0 * math.log(10000.0) / values.shape[-1]))
    angles = places.astype(jnp.float32)[:, None] * inverse[None, :]
    cosine = jnp.cos(angles)[:, None, :]
    sine = jnp.sin(angles)[:, None, :]
    first = values[..., :half]
    second = values[..., half:]
    return jnp.concatenate([first * cosine - second * sine, second * cosine + first * sine], axis=-1)

def rms_scale(values, gain):
    return values * lax.rsqrt(lax.optimization_barrier(jnp.mean(values * values, axis=-1, keepdims=True)) + EPS) * gain

def reference(x_old, old_blocks, new_blocks, order, pre_gain, post_gain, w_query, w_key, w_value, w_out_t):
    old_start = offsets(old_blocks)
    new_start = offsets(new_blocks)
    seq_rows = jnp.arange(TOKENS, dtype=jnp.int32)
    shard = (lax.optimization_barrier(jnp.sum((old_start[None, :] <= seq_rows[:, None]).astype(jnp.int32), axis=1)) - 1).astype(jnp.int32)
    devices = jnp.arange(N_SEQ, dtype=jnp.int32)
    holder = lax.optimization_barrier(jnp.sum(devices[None, :] * (order[None, :] == shard[:, None]).astype(jnp.int32), axis=1)).astype(jnp.int32)
    source = (holder * CAP + seq_rows - old_start[shard]).astype(jnp.int32)
    resident = x_old[source]
    resident_f = resident.astype(jnp.float32)
    normed = rms_scale(resident_f, pre_gain).astype(jnp.bfloat16)
    query = jnp.dot(normed, w_query, preferred_element_type=jnp.float32).reshape(TOKENS, HEADS, HEAD)
    query = (rotate(query, seq_rows) * (D // HEADS) ** (-0.5)).astype(jnp.bfloat16)
    key = jnp.dot(normed, w_key, preferred_element_type=jnp.float32).reshape(TOKENS, KV_HEADS, HEAD)
    key = rotate(key, seq_rows).astype(jnp.bfloat16)
    value = jnp.dot(normed, w_value, preferred_element_type=jnp.float32).reshape(TOKENS, KV_HEADS, HEAD).astype(jnp.bfloat16)
    group = HEADS // KV_HEADS
    query_heads = jnp.transpose(query, (1, 0, 2)).astype(jnp.float32)
    key_heads = jnp.repeat(jnp.transpose(key, (1, 0, 2)), group, axis=0).astype(jnp.float32)
    value_heads = jnp.repeat(jnp.transpose(value, (1, 0, 2)), group, axis=0).astype(jnp.float32)
    causal = seq_rows[None, :] <= seq_rows[:, None]

    def one_head(operands):
        query_one, key_one, value_one = operands
        score = jnp.dot(query_one, key_one.T)
        capped = 50.0 * jnp.tanh(score / 50.0)
        weight = jnp.where(causal, jnp.exp(capped), 0.0)
        total = lax.optimization_barrier(jnp.sum(weight, axis=1))
        weight_b = weight.astype(jnp.bfloat16).astype(jnp.float32)
        numer = jnp.dot(weight_b, value_one)
        return (numer / total[:, None]).astype(jnp.bfloat16)
    context = lax.map(one_head, (query_heads, key_heads, value_heads))
    context = jnp.transpose(context, (1, 0, 2)).reshape(TOKENS, HEADS * HEAD)
    span = HEADS * HEAD // N_TP
    projected = jnp.zeros((TOKENS, D), jnp.float32)
    for group_index in range(N_TP):
        columns = context[:, group_index * span:(group_index + 1) * span]
        weights_part = w_out_t[:, group_index * span:(group_index + 1) * span]
        partial_sum = lax.dot_general(columns, weights_part, (((1,), (1,)), ((), ())), preferred_element_type=jnp.float32)
        projected = projected + lax.optimization_barrier(partial_sum.astype(jnp.bfloat16)).astype(jnp.float32)
    refreshed = (resident_f + rms_scale(projected, post_gain)).astype(jnp.bfloat16)
    slots = jnp.arange(N_SEQ * CAP, dtype=jnp.int32)
    owner = (slots // CAP).astype(jnp.int32)
    within = (slots - owner * CAP).astype(jnp.int32)
    valid = within < new_blocks[owner] * BLOCK
    target = jnp.clip(new_start[owner] + within, 0, TOKENS - 1).astype(jnp.int32)
    return jnp.where(valid[:, None], refreshed[target], jnp.zeros((), jnp.bfloat16)).astype(jnp.bfloat16)
```

```python
import functools
import math

import jax
import jax.numpy as jnp
from jax import lax
from jax.experimental import pallas as pl
from jax.experimental.pallas import tpu as pltpu
from jax.sharding import Mesh
from jax.sharding import PartitionSpec as P

D = 4608
HEADS = 32
HEAD = 128
BLOCK = 128
EPS = 1e-06
BF = jnp.bfloat16
F32 = jnp.float32
VM = pltpu.VMEM
DMA = pltpu.SemaphoreType.DMA


def kept(at, c):
    return 2 * at + lax.rem(at + c, 2)


def coords():
    return tuple(lax.axis_index(name) for name in ("x", "yl", "c", "z", "yh"))


def copy_to(src, dst, send_sem, recv_sem, device):
    return pltpu.make_async_remote_copy(
        src_ref=src,
        dst_ref=dst,
        send_sem=send_sem,
        recv_sem=recv_sem,
        device_id=device,
        device_id_type=pl.DeviceIdType.MESH,
    )


def greet(devices):
    sem = pltpu.get_barrier_semaphore()
    for device in devices:
        pl.semaphore_signal(sem, inc=1, device_id=device, device_id_type=pl.DeviceIdType.MESH)
    pl.semaphore_wait(sem, len(devices))


def mod4(v):
    return lax.rem(v + 4, 4)


class Gather4:
    def __init__(self, views, axis, me, send, recv):
        one, two = me + 1 - 2 * lax.rem(me, 2), 3 - me
        far = two + 1 - 2 * lax.rem(two, 2)
        self.moves = [
            (me, one, 0, one),
            (me, two, 1, two),
            (me, two, 0, two),
            (me, one, 1, one),
            (one, far, 0, two),
            (two, far, 1, one),
        ]
        self.views, self.axis, self.send, self.recv = views, axis, send, recv

    def each(self, move, got):
        sent, received, half, partner = self.moves[move]
        for n, view in enumerate(self.views):
            ref = view(received if got else sent, half)
            at = n * 6 + move
            yield copy_to(ref, ref, self.send.at[at], self.recv.at[at], {self.axis: partner})

    def go(self, *moves):
        for move in moves:
            for copy in self.each(move, False):
                copy.start()

    def got(self, *moves):
        for move in moves:
            for copy in self.each(move, True):
                copy.wait_recv()

    def sent(self):
        for move in range(6):
            for copy in self.each(move, False):
                copy.wait_send()


def rows(ref, start, size, unit=16):
    return ref.at[pl.ds(pl.multiple_of(start, unit), size)]


def lanes(start, size):
    return pl.ds(pl.multiple_of(start, 128), size)


def kernel_in(
    old_ref, order_ref, xt, gain, cos, sin, wq_in, wk_in, wv_in, wo_in,
    q_out, kv_out, xs, wo,
    wq, wk, wv, slots, landed, normed, squares, near, other, to_y, from_y, mine,
    s_w, s_one, r_one, s_two, r_two, s_three, r_three, s_wg, r_wg, s_z, r_z, s_q, r_q, s_c, r_c, s_y, r_y,
):
    x, yl, c, z, yh = coords()
    at = pl.ds(pl.multiple_of(x * 288, 16), 288)
    owns = [
        pltpu.make_async_copy(src, dst.at[at], s_w.at[n])
        for n, (src, dst) in enumerate(((wq_in, wq), (wk_in, wk), (wv_in, wv), (wo_in, wo)))
    ]
    for copy in owns:
        copy.start()
    starts, total = [], 0
    for m in range(16):
        starts.append(total)
        total = total + old_ref[m]
    k = order_ref[x * 4 + yl * 2 + c]
    first = sum([jnp.where(k > m, old_ref[m], 0) for m in range(15)])
    for r in range(4):
        b = lax.rem(r - first + 64, 4)
        for h in range(2):
            part = [xt[h * 288:(h + 1) * 288, n * 128:(n + 1) * 128] for n in range(4)]
            low = jnp.where(b == 0, part[0], part[1])
            slots[r * 2 + h] = jnp.where(b < 2, low, jnp.where(b == 2, part[2], part[3]))
    ring_peers = [
        {"x": lax.rem(x + dx, 4), "c": c + dc - 2 * c * dc} for dx in range(4) for dc in range(2)
    ][1:]
    y_one = {"yl": 1 - yl}
    y_two = {"yl": 1 - yl, "yh": 1 - yh}
    group = [
        {"z": lax.rem(z + dz, 4), "yl": yl + dy - 2 * yl * dy, "c": c + dc - 2 * c * dc}
        for dz in range(4) for dy in range(2) for dc in range(2)
    ][1:]
    greet(ring_peers + [y_two] + group)
    here = x * 2 + c
    landed[here] = slots[here]
    one = []
    for d, peer in enumerate(ring_peers, 1):
        copy = copy_to(slots.at[peer["x"] * 2 + peer["c"]], landed.at[here], s_one.at[d], r_one.at[d], peer)
        copy.start()
        one.append(copy)
    for copy in owns:
        copy.wait()

    def half_rows(ref):
        return lambda chunk, half: rows(ref, chunk * 288 + half * 144, 144)

    weights = Gather4([half_rows(r) for r in (wq, wk, wv, wo)], "x", x, s_wg, r_wg)
    weights.go(0, 1, 2, 3)
    straight = yl == yh
    two, three = [], []
    for d in range(8):
        dx, dc = d // 2, d % 2
        slot = mod4(x - dx) * 2 + c + dc - 2 * c * dc
        if d > 0:
            copy_to(slots.at[slot], landed.at[slot], s_one.at[d], r_one.at[d], y_one).wait_recv()
        copy = copy_to(landed.at[slot], landed.at[8 + slot], s_two.at[d], r_two.at[d], y_two)
        copy.start()
        two.append(copy)
        copy = copy_to(landed.at[slot], landed.at[16 + slot], s_three.at[d], r_three.at[d], y_one)
        relay = copy_to(landed.at[8 + slot], landed.at[16 + slot], s_three.at[d], r_three.at[d], y_one)
        three.append((copy, relay))
        pl.when(jnp.logical_not(straight))(copy.start)
    for d in range(8):
        two[d].wait_recv()
        pl.when(straight)(three[d][1].start)
    weights.got(0, 1)
    weights.go(4, 5)
    for d in range(8):
        three[d][0].wait_recv()
    me = z * 4 + yl * 2 + c
    first_buffer = jnp.where(straight, 0, 1)
    for place in range(8):
        g = x + 4 * kept(place % 4, place // 4)
        shard = sum([jnp.where(starts[m] <= g, 1, 0) for m in range(16)]) - 1
        holder = sum([jnp.where(order_ref[p] == shard, p, 0) for p in range(16)])
        y_source = lax.rem(lax.div(holder, 2), 2)
        source = jnp.where(y_source == yh, first_buffer, 2) * 8 + lax.div(holder, 4) * 2 + lax.rem(holder, 2)
        block = landed[source]
        xs[pl.ds(pl.multiple_of(z * 288, 16), 288), place * 128:(place + 1) * 128] = block
        wide = block.astype(F32)
        squares[me, place:place + 1, :] = jnp.sum(wide * wide, axis=0, keepdims=True)
    gather = Gather4([half_rows(xs)], "z", z, s_z, r_z)
    gather.go(0, 1, 2, 3)
    sums = []
    for e, peer in enumerate(group, 1):
        copy = copy_to(squares.at[me], squares.at[me], s_q.at[e], r_q.at[e], peer)
        copy.start()
        sums.append(copy)
    gather.got(0, 1)
    gather.go(4, 5)
    for copy in sums:
        copy.wait_recv()
    gather.got(2, 3, 4, 5)
    weights.got(2, 3, 4, 5)
    factor = lax.rsqrt(jnp.sum(squares[...], axis=0) * (1.0 / D) + EPS)
    for place in range(8):
        scale = factor[place:place + 1, :]

        def norm_rows(n, _, place=place, scale=scale):
            part = pl.ds(pl.multiple_of(n * 144, 16), 144)
            at = (part, slice(place * 128, (place + 1) * 128))
            normed[at] = (xs[at].astype(F32) * scale * gain[part, :]).astype(BF)
            return 0

        lax.fori_loop(0, 8, norm_rows, 0)

    def quarter(dst, y, core):
        right = normed[:, lanes(core * 512, 512)]

        def dot(left):
            return lax.dot_general(left, right, (((0,), (0,)), ((), ())), preferred_element_type=F32)

        dst[0:256, :] = dot(wq[:, lanes(y * 256, 256)])
        dst[256:384, :] = dot(wk[:, lanes(y * 128, 128)])
        dst[384:512, :] = dot(wv[:, lanes(y * 128, 128)])

    core = {"c": 1 - c}
    quarter(near.at[0], 1 - yl, 1 - c)
    to_core = [copy_to(near.at[n], other.at[n], s_c.at[n], r_c.at[n], core) for n in range(2)]
    to_core[0].start()
    quarter(mine, 1 - yl, c)
    to_core[0].wait_recv()
    to_partner = []
    for n in range(4):
        part = slice(n * 128, (n + 1) * 128)
        to_y[part, :] = (mine[part, :] + other[0, part, :]).astype(BF)
        copy = copy_to(to_y.at[part], from_y.at[part], s_y.at[n], r_y.at[n], y_one)
        to_partner.append(copy)
        copy.start()
    quarter(near.at[1], yl, 1 - c)
    to_core[1].start()
    quarter(mine, yl, c)
    to_core[1].wait_recv()
    scale_q = (D // HEADS) ** (-0.5)
    for n in range(4):
        part = slice(n * 128, (n + 1) * 128)
        to_partner[n].wait_recv()
        value = mine[part, :] + other[1, part, :] + from_y[part, :].astype(F32)
        if n < 3:
            a, b = value[:64], value[64:]
            value = jnp.concatenate([a * cos[...] - b * sin[...], b * cos[...] + a * sin[...]], axis=0)
        if n < 2:
            q_out[part, :] = (value * scale_q).astype(BF)
        else:
            for p in range(4):
                kv_out[p, (n - 2) * 128:(n - 1) * 128, :] = value[:, p * 128:(p + 1) * 128].astype(BF)
    for copy in one + two + sums + to_core + to_partner:
        copy.wait_send()
    for copy, _ in three:
        copy.wait_send()
    weights.sent()
    gather.sent()


def run_in(old_blocks, order, xt, gain, cos, sin, w_query, w_key, w_value, w_out_t):
    smem = pl.BlockSpec(memory_space=pltpu.SMEM)
    vmem = pl.BlockSpec(memory_space=pltpu.VMEM)
    hbm = pl.BlockSpec(memory_space=pltpu.HBM)
    return pl.pallas_call(
        kernel_in,
        name="project",
        out_shape=[
            jax.ShapeDtypeStruct((256, 512), BF),
            jax.ShapeDtypeStruct((4, 256, 128), BF),
            jax.ShapeDtypeStruct((1152, 1024), BF),
            jax.ShapeDtypeStruct((1152, 512), BF),
        ],
        in_specs=[smem, smem, vmem, vmem, vmem, vmem, hbm, hbm, hbm, hbm],
        out_specs=[vmem] * 4,
        scratch_shapes=[
            VM((1152, 512), BF), VM((1152, 256), BF), VM((1152, 256), BF),
            VM((8, 288, 128), BF), VM((24, 288, 128), BF), VM((1152, 1024), BF), VM((16, 8, 128), F32),
            VM((2, 512, 512), F32), VM((2, 512, 512), F32), VM((512, 512), BF), VM((512, 512), BF), VM((512, 512), F32),
            DMA((4,)), DMA((8,)), DMA((8,)), DMA((8,)), DMA((8,)), DMA((8,)), DMA((8,)),
            DMA((24,)), DMA((24,)), DMA((6,)), DMA((6,)), DMA((16,)), DMA((16,)), DMA((2,)), DMA((2,)), DMA((4,)), DMA((4,)),
        ],
        compiler_params=pltpu.CompilerParams(collective_id=0, has_side_effects=True, vmem_limit_bytes=60 * 2**20),
    )(old_blocks, order, xt, gain, cos, sin, w_query, w_key, w_value, w_out_t)


def kernel_attend(q_ref, kv_ref, ctx, kvs, qs, acc, den, s_x, r_x, s_c, r_c, s_y, r_y, s_o, r_o):
    x, yl, c, z, yh = coords()
    for p in range(4):
        kvs[kept(p, c), :, lanes(x * 128, 128)] = kv_ref[p]
    core, y_one = {"c": 1 - c}, {"yl": 1 - yl}
    greet([{"x": x + 1 - 2 * lax.rem(x, 2)}, {"x": 3 - x}, core, y_one])

    def block(n):
        return lambda chunk, half: kvs.at[kept(half * 2 + n, c), :, lanes(chunk * 128, 128)]

    gather = Gather4([block(n) for n in range(2)], "x", x, s_x, r_x)
    gather.go(0, 1, 2, 3)
    for p in range(4):
        for h in range(2):
            part = q_ref[h * 128:(h + 1) * 128, p * 128:(p + 1) * 128].astype(F32)
            qs[p, h * 128:(h + 1) * 128, :] = part.T.astype(BF)
    acc[...] = jnp.zeros_like(acc)
    den[...] = jnp.zeros_like(den)
    gather.got(0, 1)
    gather.go(4, 5)
    gather.got(2, 4, 3, 5)
    across = []
    for p in range(4):
        ref = kvs.at[kept(p, c)]
        copy = copy_to(ref, ref, s_c.at[p], r_c.at[p], core)
        copy.start()
        across.append(copy)

    def tile(p, group, masked):
        keys = kvs[group, :128, :]
        values = kvs[group, 128:, :]
        for h in range(2):
            part = slice(h * 128, (h + 1) * 128)
            score = jnp.dot(qs[p, part, :], keys, preferred_element_type=F32)
            weight = jnp.exp(50.0 * jnp.tanh(score * (1.0 / 50.0)))
            if masked:
                row = lax.broadcasted_iota(jnp.int32, (128, 512), 0) + x * 128
                col = lax.broadcasted_iota(jnp.int32, (128, 512), 1)
                weight = jnp.where(col <= row, weight, 0.0)
            den[p, part, :] += (weight[:, :128] + weight[:, 128:256]) + (weight[:, 256:384] + weight[:, 384:])
            acc[p, part, :] += lax.dot_general(
                weight.astype(BF), values, (((1,), (1,)), ((), ())), preferred_element_type=F32
            )

    def same_core(p, _):
        def earlier(e, _):
            tile(p, kept(e, c), False)
            return 0

        lax.fori_loop(0, p, earlier, 0)
        tile(p, kept(p, c), True)
        return 0

    lax.fori_loop(0, 4, same_core, 0)
    for p in range(4):
        ref = kvs.at[kept(p, 1 - c)]
        copy_to(ref, ref, s_c.at[p], r_c.at[p], core).wait_recv()

    def other_core(p, _):
        def earlier(e, _):
            tile(p, kept(e, 1 - c), False)
            return 0

        lax.fori_loop(0, p + lax.rem(p + c, 2), earlier, 0)
        return 0

    lax.fori_loop(0, 4, other_core, 0)
    for p in range(4):
        for h in range(2):
            part = slice(h * 128, (h + 1) * 128)
            total = jnp.sum(den[p, part, :], axis=1, keepdims=True)
            value = (acc[p, part, :] / total).astype(BF)
            cols = lanes(yl * 256 + h * 128, 128)
            ctx[c * 4 + p, :, cols] = value[:64]
            ctx[8 + c * 4 + p, :, cols] = value[64:]

    def region(core_at, y_at, half):
        return ctx.at[pl.ds(half * 8 + core_at * 4, 4), :, lanes(y_at * 256, 256)]

    to_y, to_core = [], []
    for half in range(2):
        ref = region(c, yl, half)
        copy = copy_to(ref, ref, s_y.at[half], r_y.at[half], y_one)
        copy.start()
        to_y.append(copy)
    for half in range(2):
        ref = region(c, yl, half)
        copy = copy_to(ref, ref, s_o.at[half], r_o.at[half], core)
        copy.start()
        to_core.append(copy)
    for half in range(2):
        ref = region(c, 1 - yl, half)
        copy_to(ref, ref, s_y.at[half], r_y.at[half], y_one).wait_recv()
        copy = copy_to(ref, ref, s_o.at[2 + half], r_o.at[2 + half], core)
        copy.start()
        to_core.append(copy)
    for n in range(4):
        ref = region(1 - c, yl if n < 2 else 1 - yl, n % 2)
        copy_to(ref, ref, s_o.at[n], r_o.at[n], core).wait_recv()
    for copy in across + to_y + to_core:
        copy.wait_send()
    gather.sent()


def run_attend(q, kv):
    vmem = pl.BlockSpec(memory_space=pltpu.VMEM)
    return pl.pallas_call(
        kernel_attend,
        name="attend",
        out_shape=jax.ShapeDtypeStruct((16, 64, 512), BF),
        in_specs=[vmem, vmem],
        out_specs=vmem,
        scratch_shapes=[
            VM((8, 256, 512), BF), VM((4, 256, 128), BF), VM((4, 256, 128), F32), VM((4, 256, 128), F32),
            DMA((12,)), DMA((12,)), DMA((4,)), DMA((4,)), DMA((2,)), DMA((2,)), DMA((4,)), DMA((4,)),
        ],
        compiler_params=pltpu.CompilerParams(collective_id=1, has_side_effects=True, vmem_limit_bytes=40 * 2**20),
    )(q, kv)


def kernel_out(
    new_ref, ctx, xs, wo, gain, fin,
    send_a, send_b, got_a, got_b, more_a, more_b, more_got_a, more_got_b, total, half_out, relay, half_in,
    squares, fresh, f1, f1_got, f2,
    s_1, r_1, s_2, r_2, s_y, r_y, s_q, r_q, s_f, r_f, s_g, r_g, s_c, r_c,
):
    x, yl, c, z, yh = coords()
    core = {"c": 1 - c}
    y_one, y_two = {"yl": 1 - yl}, {"yl": 1 - yl, "yh": 1 - yh}
    group = [
        {"z": lax.rem(z + dz, 4), "yl": yl + dy - 2 * yl * dy, "c": c + dc - 2 * c * dc}
        for dz in range(4) for dy in range(2) for dc in range(2)
    ][1:]
    others = [{"x": lax.rem(x + dx, 4)} for dx in range(1, 4)]
    greet(group + others + [y_two])
    one, two = z + 1 - 2 * lax.rem(z, 2), 3 - z
    far = two + 1 - 2 * lax.rem(two, 2)

    def piece(chunk, half):
        left = wo[pl.ds(pl.multiple_of(chunk * 288, 16), 288), :]
        right = ctx[half * 8:(half + 1) * 8].reshape(512, 512)
        return lax.dot_general(left, right, (((1,), (1,)), ((), ())), preferred_element_type=F32)

    first = []
    send_a[1] = piece(far, 0).astype(BF)
    send_b[1] = piece(far, 1).astype(BF)
    for n, (src, dst, peer) in enumerate(((send_a, got_a, one), (send_b, got_b, two))):
        first.append(copy_to(src.at[1], dst.at[1], s_1.at[n], r_1.at[n], {"z": peer}))
        first[-1].start()
    send_a[0] = piece(one, 0).astype(BF)
    send_b[0] = piece(two, 1).astype(BF)
    for n, (src, dst, peer) in enumerate(((send_a, got_a, one), (send_b, got_b, two))):
        first.append(copy_to(src.at[0], dst.at[0], s_1.at[2 + n], r_1.at[2 + n], {"z": peer}))
        first[-1].start()
    total[0] = piece(two, 0)
    total[1] = piece(one, 1)
    second = []
    for n, (src, got, dst, peer) in enumerate(
        ((more_a, got_a, more_got_a, two), (more_b, got_b, more_got_b, one))
    ):
        first[n].wait_recv()
        src[...] = (total[n] + got[1].astype(F32)).astype(BF)
        second.append(copy_to(src, dst, s_2.at[n], r_2.at[n], {"z": peer}))
        second[-1].start()
    total[0] = piece(z, 0)
    total[1] = piece(z, 1)
    for n, got in enumerate((got_a, got_b)):
        first[2 + n].wait_recv()
        total[n] = total[n] + got[0].astype(F32)
    for n, got in enumerate((more_got_a, more_got_b)):
        second[n].wait_recv()
        total[n] = total[n] + got[...].astype(F32)
    half_out[...] = total[1 - yh].astype(BF)
    hop = []
    for n, peer in enumerate((y_one, y_two)):
        part = slice(n * 144, (n + 1) * 144)
        hop.append(copy_to(half_out.at[part], relay.at[part], s_y.at[n], r_y.at[n], peer))
        hop[-1].start()
    for n, peer in enumerate((y_two, y_one)):
        part = slice(n * 144, (n + 1) * 144)
        hop[n].wait_recv()
        hop.append(copy_to(relay.at[part], half_in.at[part], s_y.at[2 + n], r_y.at[2 + n], peer))
        hop[-1].start()
    for n in range(2):
        hop[2 + n].wait_recv()
    me = z * 4 + yl * 2 + c
    for m in range(4):
        cols = slice(m * 128, (m + 1) * 128)
        value = total[yh, :, cols] + half_in[:, cols].astype(F32)
        total[yh, :, cols] = value
        squares[me, m:m + 1, :] = jnp.sum(value * value, axis=0, keepdims=True)
    sums = []
    for e, peer in enumerate(group, 1):
        copy = copy_to(squares.at[me], squares.at[me], s_q.at[e], r_q.at[e], peer)
        copy.start()
        sums.append(copy)
    low = lax.broadcasted_iota(jnp.int32, (288, 128), 1) < 64

    def pair(m):
        at = pl.ds(pl.multiple_of(z * 288, 16), 288)
        a = xs[at, m * 256:m * 256 + 128].astype(F32)
        b = xs[at, m * 256 + 128:m * 256 + 256].astype(F32)
        upper, lower = pltpu.roll(a, 64, 1), pltpu.roll(b, 64, 1)
        return jnp.where(low, jnp.where(yh == 0, a, upper), jnp.where(yh == 0, lower, b))

    for copy in sums:
        copy.wait_recv()
    factor = lax.rsqrt(jnp.sum(squares[...], axis=0) * (1.0 / D) + EPS)
    for m in range(4):
        fresh[m] = pair(m) + total[yh, :, m * 128:(m + 1) * 128] * factor[m:m + 1, :] * gain[...]
    starts, so_far = [], 0
    for j in range(16):
        starts.append(so_far)
        so_far = so_far + new_ref[j]
    for n in range(8):
        sides = []
        for side in range(2):
            j = 2 * n + side
            within = lax.rem(x - starts[j] + 64, 4)
            i = jnp.minimum(lax.div(starts[j] + within - x, 4), 7)
            at = lax.div(i, 2)
            place = lax.rem(i + at, 2) * 4 + at
            value = fresh[lax.div(place, 2)]
            value = jnp.where(lax.rem(place, 2) == side, value, pltpu.roll(value, 64, 1))
            sides.append(jnp.where(within < new_ref[j], value, 0.0))
        f1[n] = jnp.where(low, sides[0], sides[1]).astype(BF)
    here = pl.ds(x * 2, 2)
    f1_got[here] = f1[here]
    over_x = []
    for d, peer in enumerate(others):
        copy = copy_to(f1.at[pl.ds(peer["x"] * 2, 2)], f1_got.at[here], s_f.at[d], r_f.at[d], peer)
        copy.start()
        over_x.append(copy)
    mine = [sum([jnp.where(x * 4 + n > m, new_ref[m], 0) for m in range(15)]) for n in range(4)]
    for copy in over_x:
        copy.wait_recv()
    out = []
    for e in range(8):
        dz, dy = e // 2, e % 2
        tz, ty = lax.rem(z + dz, 4), yl + dy - 2 * yl * dy
        sides = []
        for side in range(2):
            start = jnp.where(ty == 0, mine[side], mine[2 + side])
            sides.append(f1_got[lax.rem(start + tz, 4) * 2 + ty].astype(F32))
        value = jnp.where(low, sides[0], sides[1]).astype(BF)
        at = (z * 2 + yl) * 2 + c
        if e == 0:
            fin[at] = value
        else:
            f2[e] = value
            copy = copy_to(f2.at[e], fin.at[at], s_g.at[e], r_g.at[e], {"z": tz, "yl": ty})
            copy.start()
            out.append(copy)
    swap = []
    for e in range(8):
        dz, dy = e // 2, e % 2
        at = (mod4(z - dz) * 2 + yl + dy - 2 * yl * dy) * 2 + c
        if e > 0:
            copy_to(fin.at[at], fin.at[at], s_g.at[e], r_g.at[e], core).wait_recv()
        copy = copy_to(fin.at[at], fin.at[at], s_c.at[e], r_c.at[e], core)
        copy.start()
        swap.append(copy)
    for copy in swap:
        copy.wait_recv()
    for copy in first + second + hop + sums + over_x + out + swap:
        copy.wait_send()


def run_out(new_blocks, ctx, xs, wo, gain):
    smem = pl.BlockSpec(memory_space=pltpu.SMEM)
    vmem = pl.BlockSpec(memory_space=pltpu.VMEM)
    return pl.pallas_call(
        kernel_out,
        name="finish",
        out_shape=jax.ShapeDtypeStruct((16, 288, 128), BF),
        in_specs=[smem, vmem, vmem, vmem, vmem],
        out_specs=vmem,
        scratch_shapes=[VM((2, 288, 512), BF)] * 4
        + [VM((288, 512), BF)] * 4
        + [VM((2, 288, 512), F32), VM((288, 512), BF), VM((288, 512), BF), VM((288, 512), BF)]
        + [VM((16, 4, 128), F32), VM((4, 288, 128), F32), VM((8, 288, 128), BF), VM((8, 288, 128), BF)]
        + [VM((8, 288, 128), BF)]
        + [DMA((4,)), DMA((4,)), DMA((2,)), DMA((2,)), DMA((4,)), DMA((4,)), DMA((16,)), DMA((16,))]
        + [DMA((3,)), DMA((3,)), DMA((8,)), DMA((8,)), DMA((8,)), DMA((8,))],
        compiler_params=pltpu.CompilerParams(collective_id=2, has_side_effects=True, vmem_limit_bytes=56 * 2**20),
    )(new_blocks, ctx, xs, wo, gain)


def per_device(
    x_old, old_blocks, new_blocks, order, pre_gain, post_gain, w_query, w_key, w_value, w_out_t
):
    x, yl, c, z, yh = coords()
    gain = pre_gain.reshape(4, 2, 2, 288)[:, yl, c].reshape(1152, 1)
    gain = jnp.broadcast_to(gain, (1152, 128))
    gain_out = jnp.broadcast_to(post_gain.reshape(16, 288)[z * 4 + yl * 2 + c][:, None], (288, 128))
    half = HEAD // 2
    inverse = jnp.exp(jnp.arange(half, dtype=F32) * (-2.0 * math.log(10000.0) / HEAD))
    at = jnp.arange(512, dtype=jnp.int32)
    place = at // 128
    block = 2 * place + (place + c) % 2
    positions = (x + 4 * block) * BLOCK + at % 128
    angles = inverse[:, None] * positions.astype(F32)[None, :]
    q, kv, xs, wo = run_in(
        old_blocks, order, x_old.T, gain, jnp.cos(angles), jnp.sin(angles), w_query, w_key, w_value, w_out_t
    )
    ctx = run_attend(q, kv)
    fin = run_out(new_blocks, ctx, xs, wo, gain_out)
    return lax.dynamic_slice(fin, (0, 0, c * 64), (16, 288, 64)).reshape(4608, 64).T


def solution(mesh):
    torus = Mesh(mesh.devices.reshape(4, 2, 2, 4, 2), ("x", "yl", "c", "z", "yh"))
    seq, tp = ("x", "yl", "c"), ("z", "yh")
    both = P(seq, tp)
    in_specs = (both, P(), P(), P(), P(), P(), both, both, both, both)
    return jax.shard_map(
        per_device, mesh=torus, in_specs=in_specs, out_specs=P(seq + tp, None), check_vma=False
    )
```

```python
import functools
import math

import jax
import jax.numpy as jnp
from jax import lax
from jax.experimental import pallas as pl
from jax.experimental.pallas import tpu as pltpu
from jax.sharding import Mesh
from jax.sharding import PartitionSpec as P

D = 4608
HEADS = 32
HEAD = 128
BLOCK = 128
EPS = 1e-06
BF = jnp.bfloat16
F32 = jnp.float32
VM = pltpu.VMEM
DMA = pltpu.SemaphoreType.DMA


def kept(at, c):
    return 2 * at + lax.rem(at + c, 2)


def coords():
    return tuple(lax.axis_index(name) for name in ("x", "yl", "c", "z", "yh"))


def copy_to(src, dst, send_sem, recv_sem, device):
    return pltpu.make_async_remote_copy(
        src_ref=src,
        dst_ref=dst,
        send_sem=send_sem,
        recv_sem=recv_sem,
        device_id=device,
        device_id_type=pl.DeviceIdType.MESH,
    )


def greet(devices):
    sem = pltpu.get_barrier_semaphore()
    for device in devices:
        pl.semaphore_signal(sem, inc=1, device_id=device, device_id_type=pl.DeviceIdType.MESH)
    pl.semaphore_wait(sem, len(devices))


def mod4(v):
    return lax.rem(v + 4, 4)


class Gather4:
    def __init__(self, views, axis, me, send, recv):
        one, two = me + 1 - 2 * lax.rem(me, 2), 3 - me
        far = two + 1 - 2 * lax.rem(two, 2)
        self.moves = [
            (me, one, 0, one),
            (me, two, 1, two),
            (me, two, 0, two),
            (me, one, 1, one),
            (one, far, 0, two),
            (two, far, 1, one),
        ]
        self.views, self.axis, self.send, self.recv = views, axis, send, recv

    def each(self, move, got):
        sent, received, half, partner = self.moves[move]
        for n, view in enumerate(self.views):
            ref = view(received if got else sent, half)
            at = n * 6 + move
            yield copy_to(ref, ref, self.send.at[at], self.recv.at[at], {self.axis: partner})

    def go(self, *moves):
        for move in moves:
            for copy in self.each(move, False):
                copy.start()

    def got(self, *moves):
        for move in moves:
            for copy in self.each(move, True):
                copy.wait_recv()

    def sent(self):
        for move in range(6):
            for copy in self.each(move, False):
                copy.wait_send()


def rows(ref, start, size, unit=16):
    return ref.at[pl.ds(pl.multiple_of(start, unit), size)]


def lanes(start, size):
    return pl.ds(pl.multiple_of(start, 128), size)


def columns(dst, table, chunk_of, count):
    lane = lax.broadcasted_iota(jnp.int32, (32, 128), 1)

    def body(n, _):
        feature = chunk_of(lax.div(n, 9)) * 288 + lax.rem(n, 9) * 32
        part = table[pl.ds(pl.multiple_of(lax.rem(feature, 128), 32), 32), :]
        value = jnp.sum(jnp.where(lane == lax.div(feature, 128), part, 0.0), axis=1, keepdims=True)
        dst[pl.ds(pl.multiple_of(n * 32, 32), 32), :] = jnp.broadcast_to(value, (32, 128))
        return 0

    lax.fori_loop(0, count * 9, body, 0)


def stage_in(
    old_ref, order_ref, xt, pre_ref, post_ref, wq_in, wk_in, wv_in, wo_in,
    q_out, kv_out, xs, wo, gain_out,
    wq, wk, wv, gain, table, cos, sin, slots, landed_0, landed_1, normed, squares, near, other, to_y, from_y, mine,
    s_w, s_one, r_one, s_two, r_two, s_three, r_three, s_wg, r_wg, s_og, r_og, s_z, r_z, s_q, r_q, s_c, r_c, s_y, r_y,
    send_kv,
):
    x, yl, c, z, yh = coords()
    landed = (landed_0, landed_1)
    at = pl.ds(pl.multiple_of(x * 288, 16), 288)
    owns = [
        pltpu.make_async_copy(src, dst.at[at], s_w.at[n])
        for n, (src, dst) in enumerate(((wq_in, wq), (wk_in, wk), (wv_in, wv), (wo_in, wo)))
    ]
    for copy in owns:
        copy.start()
    starts, total = [], 0
    for m in range(16):
        starts.append(total)
        total = total + old_ref[m]
    k = order_ref[x * 4 + yl * 2 + c]
    first = sum([jnp.where(k > m, old_ref[m], 0) for m in range(15)])
    for r in range(4):
        b = lax.rem(r - first + 64, 4)
        for h in range(2):
            for half in range(2):
                at_rows = slice(h * 288 + half * 144, h * 288 + half * 144 + 144)
                part = [xt[at_rows, n * 128:(n + 1) * 128] for n in range(4)]
                low = jnp.where(b == 0, part[0], part[1])
                slots[half, r * 2 + h] = jnp.where(b < 2, low, jnp.where(b == 2, part[2], part[3]))
    here = x * 2 + c
    for half in range(2):
        landed[half][here] = slots[half, here]
    ring_peers = [
        {"x": lax.rem(x + dx, 4), "c": c + dc - 2 * c * dc} for dx in range(4) for dc in range(2)
    ][1:]
    y_one = {"yl": 1 - yl}
    y_two = {"yl": 1 - yl, "yh": 1 - yh}
    group = [
        {"z": lax.rem(z + dz, 4), "yl": yl + dy - 2 * yl * dy, "c": c + dc - 2 * c * dc}
        for dz in range(4) for dy in range(2) for dc in range(2)
    ][1:]
    greet(ring_peers + [y_two] + group)
    one, two, three = [], [], []
    for half in range(2):
        for d, peer in enumerate(ring_peers, 1):
            n = half * 8 + d
            copy = copy_to(
                slots.at[half, peer["x"] * 2 + peer["c"]], landed[half].at[here], s_one.at[n], r_one.at[n], peer
            )
            copy.start()
            one.append(copy)
    for copy in owns:
        copy.wait()

    def half_rows(ref):
        return lambda chunk, half: rows(ref, chunk * 288 + half * 144, 144)

    weights = Gather4([half_rows(r) for r in (wq, wk, wv)], "x", x, s_wg, r_wg)
    weights.go(0, 1, 2, 3)
    straight = yl == yh
    for half in range(2):
        for d in range(8):
            n = half * 8 + d
            dx, dc = d // 2, d % 2
            slot = mod4(x - dx) * 2 + c + dc - 2 * c * dc
            if d > 0:
                copy_to(slots.at[half, slot], landed[half].at[slot], s_one.at[n], r_one.at[n], y_one).wait_recv()
            copy = copy_to(landed[half].at[slot], landed[half].at[8 + slot], s_two.at[n], r_two.at[n], y_two)
            copy.start()
            two.append(copy)
            copy = copy_to(landed[half].at[slot], landed[half].at[16 + slot], s_three.at[n], r_three.at[n], y_one)
            relay = copy_to(landed[half].at[8 + slot], landed[half].at[16 + slot], s_three.at[n], r_three.at[n], y_one)
            three.append((copy, relay))
            pl.when(jnp.logical_not(straight))(copy.start)
            if half == 1:
                two[d].wait_recv()
                pl.when(straight)(three[d][1].start)
    for n in range(8, 16):
        two[n].wait_recv()
        pl.when(straight)(three[n][1].start)
    weights.got(0, 1)
    weights.go(4, 5)
    wo_all = Gather4([half_rows(wo)], "x", x, s_og, r_og)
    wo_all.go(0, 1, 2, 3)
    me = z * 4 + yl * 2 + c
    first_buffer = jnp.where(straight, 0, 1)
    gather = Gather4([half_rows(xs)], "z", z, s_z, r_z)
    sources = []
    for place in range(8):
        g = x + 4 * kept(place % 4, place // 4)
        shard = sum([jnp.where(starts[m] <= g, 1, 0) for m in range(16)]) - 1
        holder = sum([jnp.where(order_ref[p] == shard, p, 0) for p in range(16)])
        y_source = lax.rem(lax.div(holder, 2), 2)
        sources.append(jnp.where(y_source == yh, first_buffer, 2) * 8 + lax.div(holder, 4) * 2 + lax.rem(holder, 2))
    for half in range(2):
        for n in range(half * 8, half * 8 + 8):
            three[n][0].wait_recv()
        for place in range(8):
            block = landed[half][sources[place]]
            xs[pl.ds(pl.multiple_of(z * 288 + half * 144, 16), 144), place * 128:(place + 1) * 128] = block
            wide = block.astype(F32)
            square = jnp.sum(wide * wide, axis=0, keepdims=True)
            if half == 1:
                square = square + squares[me, place:place + 1, :]
            squares[me, place:place + 1, :] = square
        if half == 0:
            gather.go(0, 2)
        else:
            gather.go(1, 3)
    sums = []
    for e, peer in enumerate(group, 1):
        copy = copy_to(squares.at[me], squares.at[me], s_q.at[e], r_q.at[e], peer)
        copy.start()
        sums.append(copy)
    table[...] = jnp.zeros_like(table)
    table[0:36, :] = pre_ref[...]
    table[...] = table[...].T
    columns(gain, table, lambda n: n * 4 + yl * 2 + c, 4)
    table[...] = jnp.zeros_like(table)
    table[0:36, :] = post_ref[...]
    table[...] = table[...].T
    columns(gain_out, table, lambda n: z * 4 + yl * 2 + c, 1)
    half_head = HEAD // 2
    inverse = jnp.exp(
        lax.broadcasted_iota(jnp.int32, (half_head, 128), 0).astype(F32) * (-2.0 * math.log(10000.0) / HEAD)
    )
    for p in range(4):
        place_of = (x + 4 * kept(p, c)) * BLOCK + lax.broadcasted_iota(jnp.int32, (half_head, 128), 1)
        angle = inverse * place_of.astype(F32)
        cos[:, p * 128:(p + 1) * 128] = jnp.cos(angle)
        sin[:, p * 128:(p + 1) * 128] = jnp.sin(angle)
    gather.got(0)
    gather.go(4)
    gather.got(1)
    gather.go(5)
    for copy in sums:
        copy.wait_recv()
    factor = lax.rsqrt(jnp.sum(squares[...], axis=0) * (1.0 / D) + EPS)

    def norm(chunk):
        for place in range(8):
            scale = factor[place:place + 1, :]

            def norm_rows(n, _, place=place, scale=scale):
                part = pl.ds(pl.multiple_of(chunk * 288 + n * 144, 16), 144)
                at = (part, slice(place * 128, (place + 1) * 128))
                normed[at] = (xs[at].astype(F32) * scale * gain[part, :]).astype(BF)
                return 0

            lax.fori_loop(0, 2, norm_rows, 0)

    def quarter(dst, y, core, late):
        low = lax.div(z, 2)
        part = pl.ds(pl.multiple_of((1 - low if late else low) * 576, 16), 576)
        right = normed[part, lanes(core * 512, 512)]

        def dot(left):
            return lax.dot_general(left, right, (((0,), (0,)), ((), ())), preferred_element_type=F32)

        for to, left in (
            (slice(0, 256), wq[part, lanes(y * 256, 256)]),
            (slice(256, 384), wk[part, lanes(y * 128, 128)]),
            (slice(384, 512), wv[part, lanes(y * 128, 128)]),
        ):
            if late:
                dst[to, :] += dot(left)
            else:
                dst[to, :] = dot(left)

    norm(z)
    gather.got(3)
    norm(z + 1 - 2 * lax.rem(z, 2))
    weights.got(2, 3, 4, 5)
    corners = [
        (near.at[0], 1 - yl, 1 - c), (mine.at[0], 1 - yl, c), (near.at[1], yl, 1 - c), (mine.at[1], yl, c),
    ]
    for dst, y, core in corners:
        quarter(dst, y, core, False)
    gather.got(2)
    norm(3 - z)
    wo_all.got(0, 1)
    wo_all.go(4, 5)
    gather.got(4, 5)
    far = 3 - z
    norm(far + 1 - 2 * lax.rem(far, 2))
    core = {"c": 1 - c}
    to_core = [copy_to(near.at[n], other.at[n], s_c.at[n], r_c.at[n], core) for n in range(2)]
    quarter(*corners[0], True)
    to_core[0].start()
    quarter(*corners[1], True)
    to_core[0].wait_recv()
    to_partner = {}
    for n in (2, 3, 0, 1):
        part = slice(n * 128, (n + 1) * 128)
        to_y[part, :] = (mine[0, part, :] + other[0, part, :]).astype(BF)
        copy = copy_to(to_y.at[part], from_y.at[part], s_y.at[n], r_y.at[n], y_one)
        to_partner[n] = copy
        copy.start()
    quarter(*corners[2], True)
    to_core[1].start()
    quarter(*corners[3], True)
    to_core[1].wait_recv()
    scale_q = (D // HEADS) ** (-0.5)
    for n in (2, 3, 0, 1):
        part = slice(n * 128, (n + 1) * 128)
        to_partner[n].wait_recv()
        value = mine[1, part, :] + other[1, part, :] + from_y[part, :].astype(F32)
        if n < 3:
            a, b = value[:64], value[64:]
            value = jnp.concatenate([a * cos[...] - b * sin[...], b * cos[...] + a * sin[...]], axis=0)
        if n < 2:
            q_out[part, :] = (value * scale_q).astype(BF)
        else:
            for p in range(4):
                kv_out[p, (n - 2) * 128:(n - 1) * 128, :] = value[:, p * 128:(p + 1) * 128].astype(BF)
        if n == 3:
            send_kv()

    def finish():
        wo_all.got(2, 3, 4, 5)
        for copy in one + two + sums + to_core + list(to_partner.values()):
            copy.wait_send()
        for copy, _ in three:
            copy.wait_send()
        weights.sent()
        wo_all.sent()
        gather.sent()

    return finish


class KeysValues:
    def __init__(self, kv_ref, kvs, s_x, r_x, s_c, r_c):
        x, _, c, _, _ = coords()

        def block(n):
            return lambda chunk, half: kvs.at[kept(half * 2 + n, c), :, lanes(chunk * 128, 128)]

        self.gather = Gather4([block(n) for n in range(2)], "x", x, s_x, r_x)
        self.kv_ref, self.kvs, self.s_c, self.r_c = kv_ref, kvs, s_c, r_c
        self.across = []

    def send(self):
        x, _, c, _, _ = coords()
        for p in range(4):
            self.kvs[kept(p, c), :, lanes(x * 128, 128)] = self.kv_ref[p]
        self.gather.go(0, 1, 2, 3)

    def core_copies(self, late, mine):
        x, _, c, _, _ = coords()
        low = lax.div(x, 2)
        cols = lanes((1 - low if late else low) * 256, 256)
        for p in range(4):
            ref = self.kvs.at[kept(p, c if mine else 1 - c), :, cols]
            n = p + 4 * late
            yield copy_to(ref, ref, self.s_c.at[n], self.r_c.at[n], {"c": 1 - c})

    def to_core(self, late):
        for copy in self.core_copies(late, True):
            copy.start()
            self.across.append(copy)

    def from_core(self):
        for late in (0, 1):
            for copy in self.core_copies(late, False):
                copy.wait_recv()


def stage_attend(q_ref, ctx, keys_values, kvs, qs, acc, den, s_y, r_y, s_o, r_o):
    x, yl, c, z, yh = coords()
    core, y_one = {"c": 1 - c}, {"yl": 1 - yl}
    gather = keys_values.gather
    for p in range(4):
        for h in range(2):
            part = q_ref[h * 128:(h + 1) * 128, p * 128:(p + 1) * 128].astype(F32)
            qs[p, h * 128:(h + 1) * 128, :] = part.T.astype(BF)
    acc[...] = jnp.zeros_like(acc)
    den[...] = jnp.zeros_like(den)
    gather.got(0)
    gather.go(4)
    gather.got(1)
    gather.go(5)
    gather.got(3)
    keys_values.to_core(0)

    def tile(p, group, masked, start, width):
        cols = lanes(start, width)
        for h in range(2):
            part = slice(h * 128, (h + 1) * 128)
            score = jnp.dot(qs[p, part, :], kvs[group, :128, cols], preferred_element_type=F32)
            weight = jnp.exp(50.0 * jnp.tanh(score * (1.0 / 50.0)))
            if masked:
                row = lax.broadcasted_iota(jnp.int32, (128, width), 0) + x * 128
                col = lax.broadcasted_iota(jnp.int32, (128, width), 1) + start
                weight = jnp.where(col <= row, weight, 0.0)
            den[p, part, :] += sum([weight[:, n:n + 128] for n in range(0, width, 128)])
            acc[p, part, :] += lax.dot_general(
                weight.astype(BF), kvs[group, 128:, cols], (((1,), (1,)), ((), ())), preferred_element_type=F32
            )

    def same_core(start):
        def place(p, _):
            def earlier(e, _):
                tile(p, kept(e, c), False, start, 256)
                return 0

            lax.fori_loop(0, p, earlier, 0)
            tile(p, kept(p, c), True, start, 256)
            return 0

        lax.fori_loop(0, 4, place, 0)

    low = lax.div(x, 2)
    same_core(low * 256)
    gather.got(2, 4, 5)
    keys_values.to_core(1)
    same_core(256 - low * 256)
    keys_values.from_core()
    def region(core_at, y_at, at, size):
        return ctx.at[pl.ds(at + core_at * 4, size), :, lanes(y_at * 256, 256)]

    to_y, to_core = [], []
    for p in range(4):

        def earlier(e, _, p=p):
            tile(p, kept(e, 1 - c), False, 0, 512)
            return 0

        lax.fori_loop(0, p + lax.rem(p + c, 2), earlier, 0)
        for h in range(2):
            part = slice(h * 128, (h + 1) * 128)
            total = jnp.sum(den[p, part, :], axis=1, keepdims=True)
            value = (acc[p, part, :] / total).astype(BF)
            cols = lanes(yl * 256 + h * 128, 128)
            ctx[c * 4 + p, :, cols] = value[:64]
            ctx[8 + c * 4 + p, :, cols] = value[64:]
        for half in range(2):
            ref = region(c, yl, half * 8 + p, 1)
            copy = copy_to(ref, ref, s_y.at[half * 4 + p], r_y.at[half * 4 + p], y_one)
            copy.start()
            to_y.append(copy)
    for half in range(2):
        ref = region(c, yl, half * 8, 4)
        copy = copy_to(ref, ref, s_o.at[half], r_o.at[half], core)
        copy.start()
        to_core.append(copy)
    for half in range(2):
        for p in range(4):
            ref = region(c, 1 - yl, half * 8 + p, 1)
            copy_to(ref, ref, s_y.at[half * 4 + p], r_y.at[half * 4 + p], y_one).wait_recv()
        ref = region(c, 1 - yl, half * 8, 4)
        copy = copy_to(ref, ref, s_o.at[2 + half], r_o.at[2 + half], core)
        copy.start()
        to_core.append(copy)
    for n in range(4):
        ref = region(1 - c, yl if n < 2 else 1 - yl, (n % 2) * 8, 4)
        copy_to(ref, ref, s_o.at[n], r_o.at[n], core).wait_recv()

    def finish():
        for copy in keys_values.across + to_y + to_core:
            copy.wait_send()
        gather.sent()

    return finish


class Reduce4:
    def __init__(self, z, send, got, more, more_got, s_1, r_1, s_2, r_2):
        self.one, self.two = z + 1 - 2 * lax.rem(z, 2), 3 - z
        self.far = self.two + 1 - 2 * lax.rem(self.two, 2)
        self.send, self.got, self.more, self.more_got = send, got, more, more_got
        self.sems = (s_1, r_1, s_2, r_2)
        self.first, self.second = {}, []

    def partner(self, part, step):
        return {"z": self.one if part == step else self.two}

    def chunk(self, part, slot):
        return self.far if slot == 1 else (self.two if part else self.one)

    def give(self, part, slot, value):
        self.send[part, slot] = value
        n = part * 2 + slot
        copy = copy_to(
            self.send.at[part, slot], self.got.at[part, slot], self.sems[0].at[n], self.sems[1].at[n], self.partner(part, 0)
        )
        copy.start()
        self.first[part, slot] = copy

    def pass_on(self, part, value):
        self.first[part, 1].wait_recv()
        self.more[part] = (value + self.got[part, 1].astype(F32)).astype(BF)
        copy = copy_to(
            self.more.at[part], self.more_got.at[part], self.sems[2].at[part], self.sems[3].at[part], self.partner(part, 1)
        )
        copy.start()
        self.second.append(copy)

    def own(self, part, value):
        self.first[part, 0].wait_recv()
        value = value + self.got[part, 0].astype(F32)
        self.second[part].wait_recv()
        return value + self.more_got[part].astype(F32)

    def sent(self):
        for copy in list(self.first.values()) + self.second:
            copy.wait_send()


def stage_out(
    new_ref, ctx, xs, wo, gain, fin,
    a_send, a_got, a_more, a_more_got, b_send, b_got, b_more, b_more_got,
    y_send, y_relay, y_got, h_send, h_relay, h_got, own_a, own_b, total,
    squares, fresh, f1, f2, f1_got_0, f1_got_1,
    a_s1, a_r1, a_s2, a_r2, b_s1, b_r1, b_s2, b_r2, s_y, r_y, s_h, r_h, s_q, r_q, s_f, r_f, s_g, r_g, s_c, r_c,
):
    x, yl, c, z, yh = coords()
    core = {"c": 1 - c}
    y_one, y_two = {"yl": 1 - yl}, {"yl": 1 - yl, "yh": 1 - yh}
    group = [
        {"z": lax.rem(z + dz, 4), "yl": yl + dy - 2 * yl * dy, "c": c + dc - 2 * c * dc}
        for dz in range(4) for dy in range(2) for dc in range(2)
    ][1:]
    others = [{"x": lax.rem(x + dx, 4)} for dx in range(1, 4)]
    f1_got = (f1_got_0, f1_got_1)

    def piece(chunk, half, part):
        left = wo[pl.ds(pl.multiple_of(chunk * 288 + part * 144, 16), 144), :]
        right = ctx[pl.ds(half * 8, 8)].reshape(512, 512)
        return lax.dot_general(left, right, (((1,), (1,)), ((), ())), preferred_element_type=F32)

    hop, pass_hop = {}, {}
    for n in range(4):
        y_send[n] = piece(n, 1 - yh, 1).astype(BF)
        hop[n] = copy_to(y_send.at[n], y_relay.at[n], s_y.at[n], r_y.at[n], y_two if n % 2 else y_one)
        hop[n].start()
    first = Reduce4(z, a_send, a_got, a_more, a_more_got, a_s1, a_r1, a_s2, a_r2)
    for slot in (1, 0):
        for part in range(2):
            first.give(part, slot, piece(first.chunk(part, slot), part, 0).astype(BF))
    own_a[0] = piece(first.two, 0, 0)
    own_a[1] = piece(first.one, 1, 0)

    def forward(n):
        hop[n].wait_recv()
        pass_hop[n] = copy_to(y_relay.at[n], y_got.at[n], s_y.at[4 + n], r_y.at[4 + n], y_one if n % 2 else y_two)
        pass_hop[n].start()

    forward(0)
    forward(1)
    for part in range(2):
        first.pass_on(part, own_a[part])
    own_a[0] = piece(z, 0, 0)
    own_a[1] = piece(z, 1, 0)
    forward(2)
    forward(3)
    for n in range(4):
        own_b[n] = piece(n, yh, 1)
    for part in range(2):
        own_a[part] = first.own(part, own_a[part])
    h_send[...] = own_a[1 - yh].astype(BF)
    spans = (slice(0, 80), slice(80, 144))
    last = []
    for n, peer in enumerate((y_one, y_two)):
        last.append(copy_to(h_send.at[spans[n]], h_relay.at[spans[n]], s_h.at[n], r_h.at[n], peer))
        last[-1].start()
    second = Reduce4(z, b_send, b_got, b_more, b_more_got, b_s1, b_r1, b_s2, b_r2)
    for n in range(4):
        pass_hop[n].wait_recv()
        own_b[n] = own_b[n] + y_got[n].astype(F32)
    cols = (slice(0, 256), slice(256, 512))
    for slot in (1, 0):
        for part in range(2):
            second.give(part, slot, own_b[second.chunk(part, slot), :, cols[part]].astype(BF))
    for n, peer in enumerate((y_two, y_one)):
        last[n].wait_recv()
        last.append(copy_to(h_relay.at[spans[n]], h_got.at[spans[n]], s_h.at[2 + n], r_h.at[2 + n], peer))
        last[-1].start()
    second.pass_on(0, own_b[second.two, :, cols[0]])
    second.pass_on(1, own_b[second.one, :, cols[1]])
    for part in range(2):
        total[144:, cols[part]] = second.own(part, own_b[z, :, cols[part]])
    last[2].wait_recv()
    last[3].wait_recv()
    total[:144, :] = own_a[yh] + h_got[...].astype(F32)
    me = z * 4 + yl * 2 + c
    for m in range(4):
        value = total[:, m * 128:(m + 1) * 128]
        squares[me, m:m + 1, :] = jnp.sum(value * value, axis=0, keepdims=True)
    sums = []
    for e, peer in enumerate(group, 1):
        copy = copy_to(squares.at[me], squares.at[me], s_q.at[e], r_q.at[e], peer)
        copy.start()
        sums.append(copy)
    low = lax.broadcasted_iota(jnp.int32, (144, 128), 1) < 64

    def pair(m, part):
        at = pl.ds(pl.multiple_of(z * 288 + part * 144, 16), 144)
        a = xs[at, m * 256:m * 256 + 128].astype(F32)
        b = xs[at, m * 256 + 128:m * 256 + 256].astype(F32)
        upper, lower = pltpu.roll(a, 64, 1), pltpu.roll(b, 64, 1)
        return jnp.where(low, jnp.where(yh == 0, a, upper), jnp.where(yh == 0, lower, b))

    for part in range(2):
        for m in range(4):
            fresh[part, m] = pair(m, part)
    for copy in sums:
        copy.wait_recv()
    factor = lax.rsqrt(jnp.sum(squares[...], axis=0) * (1.0 / D) + EPS)
    starts, so_far = [], 0
    for j in range(16):
        starts.append(so_far)
        so_far = so_far + new_ref[j]
    here = pl.ds(x * 2, 2)
    over_x = []
    for part in range(2):
        rows_of = slice(part * 144, part * 144 + 144)
        for m in range(4):
            value = total[rows_of, m * 128:(m + 1) * 128] * factor[m:m + 1, :] * gain[rows_of, :]
            fresh[part, m] = fresh[part, m] + value
        for n in range(8):
            sides = []
            for side in range(2):
                j = 2 * n + side
                within = lax.rem(x - starts[j] + 64, 4)
                i = jnp.minimum(lax.div(starts[j] + within - x, 4), 7)
                at = lax.div(i, 2)
                place = lax.rem(i + at, 2) * 4 + at
                value = fresh[part, lax.div(place, 2)]
                value = jnp.where(lax.rem(place, 2) == side, value, pltpu.roll(value, 64, 1))
                sides.append(jnp.where(within < new_ref[j], value, 0.0))
            f1[part, n] = jnp.where(low, sides[0], sides[1]).astype(BF)
        f1_got[part][here] = f1[part, here]
        for d, peer in enumerate(others):
            n = part * 3 + d
            copy = copy_to(f1.at[part, pl.ds(peer["x"] * 2, 2)], f1_got[part].at[here], s_f.at[n], r_f.at[n], peer)
            copy.start()
            over_x.append(copy)
    mine = [sum([jnp.where(x * 4 + n > m, new_ref[m], 0) for m in range(15)]) for n in range(4)]
    out, swap = [], []
    for part in range(2):
        rows_of = slice(part * 144, part * 144 + 144)
        for copy in over_x[part * 3:part * 3 + 3]:
            copy.wait_recv()
        for e in range(8):
            n = part * 8 + e
            dz, dy = e // 2, e % 2
            tz, ty = lax.rem(z + dz, 4), yl + dy - 2 * yl * dy
            sides = []
            for side in range(2):
                start = jnp.where(ty == 0, mine[side], mine[2 + side])
                sides.append(f1_got[part][lax.rem(start + tz, 4) * 2 + ty].astype(F32))
            value = jnp.where(low, sides[0], sides[1]).astype(BF)
            at = (z * 2 + yl) * 2 + c
            if e == 0:
                fin[at, rows_of, :] = value
            else:
                f2[part, e] = value
                copy = copy_to(f2.at[part, e], fin.at[at, rows_of], s_g.at[n], r_g.at[n], {"z": tz, "yl": ty})
                copy.start()
                out.append(copy)
    for part in range(2):
        rows_of = slice(part * 144, part * 144 + 144)
        for e in range(8):
            n = part * 8 + e
            dz, dy = e // 2, e % 2
            at = (mod4(z - dz) * 2 + yl + dy - 2 * yl * dy) * 2 + c
            ref = fin.at[at, rows_of]
            if e > 0:
                copy_to(ref, ref, s_g.at[n], r_g.at[n], core).wait_recv()
            copy = copy_to(ref, ref, s_c.at[n], r_c.at[n], core)
            copy.start()
            swap.append(copy)
    for copy in swap:
        copy.wait_recv()
    first.sent()
    second.sent()
    for copy in list(hop.values()) + list(pass_hop.values()) + last + sums + over_x + out + swap:
        copy.wait_send()


STAGE_IN = [
    VM((1152, 512), BF), VM((1152, 256), BF), VM((1152, 256), BF),
    VM((1152, 128), F32), VM((128, 128), F32), VM((64, 512), F32), VM((64, 512), F32),
    VM((2, 8, 144, 128), BF), VM((24, 144, 128), BF), VM((24, 144, 128), BF), VM((1152, 1024), BF), VM((16, 8, 128), F32),
    VM((2, 512, 512), F32), VM((2, 512, 512), F32), VM((512, 512), BF), VM((512, 512), BF), VM((2, 512, 512), F32),
    DMA((4,)), DMA((16,)), DMA((16,)), DMA((16,)), DMA((16,)), DMA((16,)), DMA((16,)),
    DMA((18,)), DMA((18,)), DMA((6,)), DMA((6,)), DMA((6,)), DMA((6,)), DMA((16,)), DMA((16,)),
    DMA((2,)), DMA((2,)), DMA((4,)), DMA((4,)),
]
STAGE_ATTEND = [
    VM((4, 256, 128), BF), VM((4, 256, 128), F32), VM((4, 256, 128), F32),
    DMA((8,)), DMA((8,)), DMA((4,)), DMA((4,)),
]
STAGE_OUT = (
    [VM((2, 2, 144, 512), BF), VM((2, 2, 144, 512), BF), VM((2, 144, 512), BF), VM((2, 144, 512), BF)]
    + [VM((2, 2, 144, 256), BF), VM((2, 2, 144, 256), BF), VM((2, 144, 256), BF), VM((2, 144, 256), BF)]
    + [VM((4, 144, 512), BF)] * 3
    + [VM((144, 512), BF)] * 3
    + [VM((2, 144, 512), F32), VM((4, 144, 512), F32), VM((288, 512), F32)]
    + [VM((16, 4, 128), F32), VM((2, 4, 144, 128), F32)]
    + [VM((2, 8, 144, 128), BF)] * 2
    + [VM((8, 144, 128), BF)] * 2
    + [DMA((4,)), DMA((4,)), DMA((2,)), DMA((2,))] * 2
    + [DMA((8,)), DMA((8,)), DMA((4,)), DMA((4,)), DMA((16,)), DMA((16,)), DMA((6,)), DMA((6,))]
    + [DMA((16,)), DMA((16,)), DMA((16,)), DMA((16,))]
)
SHARED = [
    VM((256, 512), BF), VM((4, 256, 128), BF), VM((1152, 1024), BF), VM((1152, 512), BF), VM((16, 64, 512), BF),
    VM((288, 128), F32), VM((8, 256, 512), BF), DMA((12,)), DMA((12,)), DMA((8,)), DMA((8,)),
]


def kernel(old_ref, new_ref, order_ref, xt, pre_ref, post_ref, wq_in, wk_in, wv_in, wo_in, fin, *scratch):
    q, kv, xs, wo, ctx, gain_out, kvs, s_x, r_x, s_c, r_c = scratch[:11]
    scratch = scratch[11:]
    keys_values = KeysValues(kv, kvs, s_x, r_x, s_c, r_c)
    own_in, scratch = scratch[:len(STAGE_IN)], scratch[len(STAGE_IN):]
    own_attend, own_out = scratch[:len(STAGE_ATTEND)], scratch[len(STAGE_ATTEND):]
    end_in = stage_in(
        old_ref, order_ref, xt, pre_ref, post_ref, wq_in, wk_in, wv_in, wo_in, q, kv, xs, wo, gain_out, *own_in,
        keys_values.send,
    )
    end_attend = stage_attend(q, ctx, keys_values, kvs, *own_attend)
    end_in()
    stage_out(new_ref, ctx, xs, wo, gain_out, fin, *own_out)
    end_attend()


def run(old_blocks, new_blocks, order, xt, pre_gain, post_gain, w_query, w_key, w_value, w_out_t):
    smem = pl.BlockSpec(memory_space=pltpu.SMEM)
    vmem = pl.BlockSpec(memory_space=pltpu.VMEM)
    hbm = pl.BlockSpec(memory_space=pltpu.HBM)
    return pl.pallas_call(
        kernel,
        name="sublayer",
        out_shape=jax.ShapeDtypeStruct((16, 288, 128), BF),
        in_specs=[smem, smem, smem, vmem, vmem, vmem, hbm, hbm, hbm, hbm],
        out_specs=vmem,
        scratch_shapes=SHARED + STAGE_IN + STAGE_ATTEND + STAGE_OUT,
        compiler_params=pltpu.CompilerParams(collective_id=0, has_side_effects=True, vmem_limit_bytes=62 * 2**20),
    )(old_blocks, new_blocks, order, xt, pre_gain, post_gain, w_query, w_key, w_value, w_out_t)


def per_device(
    x_old, old_blocks, new_blocks, order, pre_gain, post_gain, w_query, w_key, w_value, w_out_t
):
    c = lax.axis_index("c")
    fin = run(
        old_blocks, new_blocks, order, x_old.T, pre_gain.reshape(36, 128), post_gain.reshape(36, 128),
        w_query, w_key, w_value, w_out_t,
    )
    return lax.dynamic_slice(fin, (0, 0, c * 64), (16, 288, 64)).reshape(4608, 64).T


def solution(mesh):
    torus = Mesh(mesh.devices.reshape(4, 2, 2, 4, 2), ("x", "yl", "c", "z", "yh"))
    seq, tp = ("x", "yl", "c"), ("z", "yh")
    both = P(seq, tp)
    in_specs = (both, P(), P(), P(), P(), P(), both, both, both, both)
    return jax.shard_map(
        per_device, mesh=torus, in_specs=in_specs, out_specs=P(seq + tp, None), check_vma=False
    )
```

```python
import functools
import math

import jax
import jax.numpy as jnp
from jax import lax
from jax.experimental import pallas as pl
from jax.experimental.pallas import tpu as pltpu
from jax.sharding import Mesh
from jax.sharding import PartitionSpec as P

D = 4608
HEADS = 32
HEAD = 128
BLOCK = 128
EPS = 1e-06
BF = jnp.bfloat16
F32 = jnp.float32
VM = pltpu.VMEM
OUT = (160, 128)
PARTS = 3
WIDE = 288 // PARTS
DMA = pltpu.SemaphoreType.DMA


def kept(at, c):
    return 2 * at + lax.rem(at + c, 2)


def coords():
    return tuple(lax.axis_index(name) for name in ("x", "yl", "c", "z", "yh"))


def copy_to(src, dst, send_sem, recv_sem, device):
    return pltpu.make_async_remote_copy(
        src_ref=src,
        dst_ref=dst,
        send_sem=send_sem,
        recv_sem=recv_sem,
        device_id=device,
        device_id_type=pl.DeviceIdType.MESH,
    )


def greet(devices):
    sem = pltpu.get_barrier_semaphore()
    for device in devices:
        pl.semaphore_signal(sem, inc=1, device_id=device, device_id_type=pl.DeviceIdType.MESH)


def greeted(devices):
    pl.semaphore_wait(pltpu.get_barrier_semaphore(), len(devices))


def mod4(v):
    return lax.rem(v + 4, 4)


class Gather4:
    def __init__(self, views, axis, me, send, recv):
        one, two = me + 1 - 2 * lax.rem(me, 2), 3 - me
        far = two + 1 - 2 * lax.rem(two, 2)
        self.moves = [
            (me, one, 0, one),
            (me, two, 1, two),
            (me, two, 0, two),
            (me, one, 1, one),
            (one, far, 0, two),
            (two, far, 1, one),
        ]
        self.views, self.axis, self.send, self.recv = views, axis, send, recv

    def each(self, move, got):
        sent, received, half, partner = self.moves[move]
        for n, view in enumerate(self.views):
            ref = view(received if got else sent, half)
            at = n * 6 + move
            yield copy_to(ref, ref, self.send.at[at], self.recv.at[at], {self.axis: partner})

    def go(self, *moves):
        for move in moves:
            for copy in self.each(move, False):
                copy.start()

    def got(self, *moves):
        for move in moves:
            for copy in self.each(move, True):
                copy.wait_recv()

    def sent(self):
        for move in range(6):
            for copy in self.each(move, False):
                copy.wait_send()


def rows(ref, start, size, unit=16):
    return ref.at[pl.ds(pl.multiple_of(start, unit), size)]


def lanes(start, size):
    return pl.ds(pl.multiple_of(start, 128), size)


def columns(dst, table, chunk_of, count):
    lane = lax.broadcasted_iota(jnp.int32, (32, 128), 1)

    def body(n, _):
        feature = chunk_of(lax.div(n, 9)) * 288 + lax.rem(n, 9) * 32
        part = table[pl.ds(pl.multiple_of(lax.rem(feature, 128), 32), 32), :]
        value = jnp.sum(jnp.where(lane == lax.div(feature, 128), part, 0.0), axis=1, keepdims=True)
        dst[pl.ds(pl.multiple_of(n * 32, 32), 32), :] = jnp.broadcast_to(value, (32, 128))
        return 0

    lax.fori_loop(0, count * 9, body, 0)


def stage_in(
    old_ref, order_ref, xt_in, pre_ref, post_ref, wq_in, wk_in, wv_in, wo_in,
    q_out, kv_out, xs, wo, gain_out,
    wq, wk, wv, gain, table, cos, sin, xt, slots, landed_0, landed_1, landed_2, normed, squares, near, other, to_y, from_y, mine,
    s_w, s_one, r_one, s_two, r_two, s_three, r_three, s_wg, r_wg, s_og, r_og, s_z, r_z, s_q, r_q, s_c, r_c, s_y, r_y,
    keys_values,
):
    x, yl, c, z, yh = coords()
    landed = (landed_0, landed_1, landed_2)
    ring_peers = [
        {"x": lax.rem(x + dx, 4), "c": c + dc - 2 * c * dc} for dx in range(4) for dc in range(2)
    ][1:]
    y_one = {"yl": 1 - yl}
    y_two = {"yl": 1 - yl, "yh": 1 - yh}
    group = [
        {"z": lax.rem(z + dz, 4), "yl": yl + dy - 2 * yl * dy, "c": c + dc - 2 * c * dc}
        for dz in range(4) for dy in range(2) for dc in range(2)
    ][1:]
    greet(ring_peers + [y_two] + group)
    into = pltpu.make_async_copy(xt_in, xt, s_w.at[5])
    into.start()
    at = pl.ds(pl.multiple_of(x * 288, 16), 288)
    owns = [
        pltpu.make_async_copy(src, dst.at[at], s_w.at[n])
        for n, (src, dst) in enumerate(((wq_in, wq), (wk_in, wk), (wv_in, wv)))
    ]

    def out_rows(chunk, half):
        return rows(wo, half * 4 * OUT[0] + chunk * OUT[half], OUT[half])

    for half in range(2):
        part = wo_in.at[pl.ds(half * OUT[0], OUT[half])]
        owns.append(pltpu.make_async_copy(part, out_rows(x, half), s_w.at[3 + half]))
    for copy in owns:
        copy.start()
    starts, total = [], 0
    for m in range(16):
        starts.append(total)
        total = total + old_ref[m]
    k = order_ref[x * 4 + yl * 2 + c]
    first = sum([jnp.where(k > m, old_ref[m], 0) for m in range(15)])
    into.wait()
    for r in range(4):
        b = lax.rem(r - first + 64, 4)
        for h in range(2):
            for half in range(PARTS):
                at_rows = slice(h * 288 + half * WIDE, h * 288 + half * WIDE + WIDE)
                part = [xt[at_rows, n * 128:(n + 1) * 128] for n in range(4)]
                low = jnp.where(b == 0, part[0], part[1])
                slots[half, r * 2 + h] = jnp.where(b < 2, low, jnp.where(b == 2, part[2], part[3]))
    here = x * 2 + c
    for half in range(PARTS):
        landed[half][here] = slots[half, here]
    greeted(ring_peers + [y_two] + group)
    one, two, three = [], [], []
    for half in range(PARTS):
        for d, peer in enumerate(ring_peers, 1):
            n = half * 8 + d
            copy = copy_to(
                slots.at[half, peer["x"] * 2 + peer["c"]], landed[half].at[here], s_one.at[n], r_one.at[n], peer
            )
            copy.start()
            one.append(copy)
    for copy in owns:
        copy.wait()

    def half_rows(ref):
        return lambda chunk, half: rows(ref, chunk * 288 + half * 144, 144)

    weights = Gather4([half_rows(r) for r in (wq, wk, wv)], "x", x, s_wg, r_wg)
    weights.go(0, 1, 2, 3)
    straight = yl == yh
    for half in range(PARTS):
        for d in range(8):
            n = half * 8 + d
            dx, dc = d // 2, d % 2
            slot = mod4(x - dx) * 2 + c + dc - 2 * c * dc
            if d > 0:
                copy_to(slots.at[half, slot], landed[half].at[slot], s_one.at[n], r_one.at[n], y_one).wait_recv()
            copy = copy_to(landed[half].at[slot], landed[half].at[8 + slot], s_two.at[n], r_two.at[n], y_two)
            copy.start()
            two.append(copy)
            copy = copy_to(landed[half].at[slot], landed[half].at[16 + slot], s_three.at[n], r_three.at[n], y_one)
            relay = copy_to(landed[half].at[8 + slot], landed[half].at[16 + slot], s_three.at[n], r_three.at[n], y_one)
            three.append((copy, relay))
            pl.when(jnp.logical_not(straight))(copy.start)
            if half == 2:
                two[d].wait_recv()
                pl.when(straight)(three[d][1].start)
    me = z * 4 + yl * 2 + c
    first_buffer = jnp.where(straight, 0, 1)

    def part_rows(part):
        return lambda chunk, half: rows(xs, chunk * 288 + part * WIDE + half * (WIDE // 2), WIDE // 2)

    gathers = [
        Gather4([part_rows(part)], "z", z, s_z.at[pl.ds(6 * part, 6)], r_z.at[pl.ds(6 * part, 6)])
        for part in range(PARTS)
    ]
    sources = []
    for place in range(8):
        g = x + 4 * kept(place % 4, place // 4)
        shard = sum([jnp.where(starts[m] <= g, 1, 0) for m in range(16)]) - 1
        holder = sum([jnp.where(order_ref[p] == shard, p, 0) for p in range(16)])
        y_source = lax.rem(lax.div(holder, 2), 2)
        sources.append(jnp.where(y_source == yh, first_buffer, 2) * 8 + lax.div(holder, 4) * 2 + lax.rem(holder, 2))

    def pick(half):
        for n in range(half * 8, half * 8 + 8):
            three[n][0].wait_recv()
        for place in range(8):
            block = landed[half][sources[place]]
            xs[pl.ds(pl.multiple_of(z * 288 + half * WIDE, 32), WIDE), place * 128:(place + 1) * 128] = block
            wide = block.astype(F32)
            square = jnp.sum(wide * wide, axis=0, keepdims=True)
            if half > 0:
                square = square + squares[me, place:place + 1, :]
            squares[me, place:place + 1, :] = square
        gathers[half].go(0, 1, 2, 3)

    for n in range(8, 24):
        if n in (13, 21):
            pick((n - 13) // 8)
        two[n].wait_recv()
        pl.when(straight)(three[n][1].start)
    pick(2)
    weights.got(0, 1)
    weights.go(4, 5)
    wo_all = Gather4([out_rows], "x", x, s_og, r_og)
    wo_all.go(0, 1, 2, 3)
    sums = []
    for e, peer in enumerate(group, 1):
        copy = copy_to(squares.at[me], squares.at[me], s_q.at[e], r_q.at[e], peer)
        copy.start()
        sums.append(copy)
    table[...] = jnp.zeros_like(table)
    table[0:36, :] = pre_ref[...]
    table[...] = table[...].T
    columns(gain, table, lambda n: n * 4 + yl * 2 + c, 4)
    table[...] = jnp.zeros_like(table)
    table[0:36, :] = post_ref[...]
    table[...] = table[...].T
    columns(gain_out, table, lambda n: z * 4 + yl * 2 + c, 1)
    gathers[0].got(0, 1)
    gathers[0].go(4, 5)
    half_head = HEAD // 2
    inverse = jnp.exp(
        lax.broadcasted_iota(jnp.int32, (half_head, 128), 0).astype(F32) * (-2.0 * math.log(10000.0) / HEAD)
    )
    for p in range(4):
        place_of = (x + 4 * kept(p, c)) * BLOCK + lax.broadcasted_iota(jnp.int32, (half_head, 128), 1)
        angle = inverse * place_of.astype(F32)
        cos[:, p * 128:(p + 1) * 128] = jnp.cos(angle)
        sin[:, p * 128:(p + 1) * 128] = jnp.sin(angle)
    for part in (1, 2):
        gathers[part].got(0, 1)
        gathers[part].go(4, 5)
    for copy in sums:
        copy.wait_recv()
    factor = lax.rsqrt(jnp.sum(squares[...], axis=0) * (1.0 / D) + EPS)

    def norm(chunk):
        for place in range(8):
            scale = factor[place:place + 1, :]

            def norm_rows(n, _, place=place, scale=scale):
                part = pl.ds(pl.multiple_of(chunk * 288 + n * 144, 16), 144)
                at = (part, slice(place * 128, (place + 1) * 128))
                normed[at] = (xs[at].astype(F32) * scale * gain[part, :]).astype(BF)
                return 0

            lax.fori_loop(0, 2, norm_rows, 0)

    pieces = {"q": (slice(0, 256), wq, 256), "k": (slice(256, 384), wk, 128), "v": (slice(384, 512), wv, 128)}

    def corner(dst, y, core, late, names="qkv"):
        low = lax.div(z, 2)
        part = pl.ds(pl.multiple_of((1 - low if late else low) * 576, 16), 576)
        right = normed[part, lanes(core * 512, 512)]
        for name in names:
            to, table_of, width = pieces[name]
            left = table_of[part, lanes(y * width, width)]
            value = lax.dot_general(left, right, (((0,), (0,)), ((), ())), preferred_element_type=F32)
            if late:
                dst[to, :] += value
            else:
                dst[to, :] = value

    norm(z)
    for one_part in gathers:
        one_part.got(3)
    norm(z + 1 - 2 * lax.rem(z, 2))
    weights.got(2, 3, 4, 5)
    corners = [
        (near.at[0], 1 - yl, 1 - c), (mine.at[0], 1 - yl, c), (near.at[1], yl, 1 - c), (mine.at[1], yl, c),
    ]
    for dst, y, core in corners:
        corner(dst, y, core, False)
    for one_part in gathers:
        one_part.got(2)
    norm(3 - z)
    wo_all.got(0, 1)
    wo_all.go(4, 5)
    for one_part in gathers:
        one_part.got(4, 5)
    far = 3 - z
    norm(far + 1 - 2 * lax.rem(far, 2))
    core = {"c": 1 - c}
    to_core = {}

    def over_core(n, name):
        to = pieces[name][0]
        at = n * 3 + "kvq".index(name)
        copy = copy_to(near.at[n, to], other.at[n, to], s_c.at[at], r_c.at[at], core)
        copy.start()
        to_core[n, name] = copy

    to_partner = {}
    first_rows, last_rows = slice(0, 256), slice(256, 512)
    k_part, v_part = slice(256, 384), slice(384, 512)
    spans = (
        (0, k_part, first_rows), (1, v_part, first_rows), (2, k_part, last_rows), (3, v_part, last_rows),
        (4, slice(0, 256), first_rows), (5, slice(0, 256), last_rows),
    )

    def over_y(name):
        to_core[0, name].wait_recv()
        to = pieces[name][0]
        to_y[to, :] = (mine[0, to, :] + other[0, to, :]).astype(BF)
        for at, part, cols in {"k": spans[:1], "v": spans[1:4], "q": spans[4:]}[name]:
            copy = copy_to(to_y.at[part, cols], from_y.at[part, cols], s_y.at[at], r_y.at[at], y_one)
            to_partner[at] = copy
            copy.start()

    for name in "kv":
        corner(*corners[0], True, name)
        over_core(0, name)
    corner(*corners[1], True, "kv")
    over_y("k")
    corner(*corners[0], True, "q")
    over_core(0, "q")
    over_y("v")
    corner(*corners[1], True, "q")
    over_y("q")
    corner(*corners[2], True)
    for name in "kvq":
        over_core(1, name)
    corner(*corners[3], True)
    for name in "kvq":
        to_core[1, name].wait_recv()
    scale_q = (D // HEADS) ** (-0.5)

    def summed(part, cols):
        return mine[1, part, cols] + other[1, part, cols] + from_y[part, cols].astype(F32)

    def turned(value, cols):
        a, b = value[:64], value[64:]
        return jnp.concatenate(
            [a * cos[:, cols] - b * sin[:, cols], b * cos[:, cols] + a * sin[:, cols]], axis=0
        ).astype(BF)

    for late, cols in enumerate((first_rows, last_rows)):
        to_partner[2 * late].wait_recv()
        key = turned(summed(k_part, cols), cols)
        to_partner[2 * late + 1].wait_recv()
        value = summed(v_part, cols).astype(BF)
        for p in range(2):
            kv_out[2 * late + p, :128, :] = key[:, p * 128:(p + 1) * 128]
            kv_out[2 * late + p, 128:, :] = value[:, p * 128:(p + 1) * 128]
        keys_values.send(late)
    for late in range(2):
        keys_values.gathers[late].got(0, 1)
        keys_values.gathers[late].go(4, 5)
    for late, cols in enumerate((first_rows, last_rows)):
        to_partner[4 + late].wait_recv()
        for h in range(2):
            part = slice(h * 128, (h + 1) * 128)
            a, b = summed(slice(h * 128, h * 128 + 64), cols), summed(slice(h * 128 + 64, h * 128 + 128), cols)
            turn_a = a * cos[:, cols] - b * sin[:, cols]
            turn_b = b * cos[:, cols] + a * sin[:, cols]
            q_out[part, cols] = (jnp.concatenate([turn_a, turn_b], axis=0) * scale_q).astype(BF)

    def finish():
        wo_all.got(2, 3, 4, 5)
        for copy in one + two + sums + list(to_core.values()) + list(to_partner.values()):
            copy.wait_send()
        for copy, _ in three:
            copy.wait_send()
        weights.sent()
        wo_all.sent()
        for one_part in gathers:
            one_part.sent()

    return finish


class KeysValues:
    def __init__(self, kv_ref, kvs, s_x, r_x, s_c, r_c):
        x, _, c, _, _ = coords()

        def block(late):
            return lambda chunk, half: kvs.at[kept(2 * late + half, c), :, lanes(chunk * 128, 128)]

        self.gathers = [
            Gather4([block(late)], "x", x, s_x.at[pl.ds(6 * late, 6)], r_x.at[pl.ds(6 * late, 6)]) for late in range(2)
        ]
        self.kv_ref, self.kvs, self.s_c, self.r_c = kv_ref, kvs, s_c, r_c
        self.across = []

    def send(self, late):
        x, _, c, _, _ = coords()
        for p in (2 * late, 2 * late + 1):
            self.kvs[kept(p, c), :, lanes(x * 128, 128)] = self.kv_ref[p]
        self.gathers[late].go(0, 1, 2, 3)

    def core_copies(self, late, mine):
        _, _, c, _, _ = coords()
        for p in (2 * late, 2 * late + 1):
            ref = self.kvs.at[kept(p, c if mine else 1 - c)]
            yield copy_to(ref, ref, self.s_c.at[p], self.r_c.at[p], {"c": 1 - c})

    def to_core(self, late):
        self.gathers[late].got(2, 3, 4, 5)
        for copy in self.core_copies(late, True):
            copy.start()
            self.across.append(copy)

    def from_core(self, late):
        for copy in self.core_copies(late, False):
            copy.wait_recv()


def stage_attend(q_ref, ctx, keys_values, kvs, qs, acc, den, s_y, r_y, s_o, r_o):
    x, yl, c, z, yh = coords()
    core, y_one = {"c": 1 - c}, {"yl": 1 - yl}
    for p in range(4):
        for h in range(2):
            part = q_ref[h * 128:(h + 1) * 128, p * 128:(p + 1) * 128].astype(F32)
            qs[p, h * 128:(h + 1) * 128, :] = part.T.astype(BF)
    acc[...] = jnp.zeros_like(acc)
    den[...] = jnp.zeros_like(den)
    keys_values.to_core(0)

    def tiles(pairs, core_at, diagonal=()):
        pairs = [(p, kept(e, core_at), n in diagonal) for n, (p, e) in enumerate(pairs)]
        scores = [jnp.dot(qs[p], kvs[group, :128, :], preferred_element_type=F32) for p, group, _ in pairs]
        for (p, group, masked), score in zip(pairs, scores):
            weight = jnp.exp2((50.0 * math.log2(math.e)) * jnp.tanh(score * (1.0 / 50.0)))
            if masked:
                row = lax.rem(lax.broadcasted_iota(jnp.int32, (256, 512), 0), 128)
                col = lax.broadcasted_iota(jnp.int32, (256, 512), 1)
                weight = jnp.where(col - row <= x * 128, weight, 0.0)
            den[p] += sum([weight[:, n:n + 128] for n in range(0, 512, 128)])
            acc[p] += lax.dot_general(
                weight.astype(BF), kvs[group, 128:, :], (((1,), (1,)), ((), ())), preferred_element_type=F32
            )

    def region(core_at, y_at, at, size):
        return ctx.at[pl.ds(at + core_at * 4, size), :, lanes(y_at * 256, 256)]

    to_y, to_core = [], []

    def put(step):
        for p in (2 * step, 2 * step + 1):
            for h in range(2):
                part = slice(h * 128, (h + 1) * 128)
                total = jnp.sum(den[p, part, :], axis=1, keepdims=True)
                value = (acc[p, part, :] / total).astype(BF)
                cols = lanes(yl * 256 + h * 128, 128)
                ctx[c * 4 + p, :, cols] = value[:64]
                ctx[8 + c * 4 + p, :, cols] = value[64:]
        for peer, send, recv, at in ((y_one, s_y, r_y, to_y), (core, s_o, r_o, to_core)):
            for half in range(2):
                n = half * 2 + step
                ref = region(c, yl, half * 8 + 2 * step, 2)
                copy = copy_to(ref, ref, send.at[n], recv.at[n], peer)
                copy.start()
                at.append(copy)

    def pass_on(step):
        for half in range(2):
            n = half * 2 + step
            ref = region(c, 1 - yl, half * 8 + 2 * step, 2)
            copy_to(ref, ref, s_y.at[n], r_y.at[n], y_one).wait_recv()
            copy = copy_to(ref, ref, s_o.at[4 + n], r_o.at[4 + n], core)
            copy.start()
            to_core.append(copy)

    tiles([(0, 0), (1, 0), (1, 1)], c, (0, 2))
    keys_values.from_core(0)
    tiles([(1 - c, 0), (1, 1 - c)], 1 - c)
    put(0)
    tiles([(2, 0), (2, 1), (3, 0), (3, 1)], c)
    keys_values.to_core(1)
    tiles([(2, 0), (2, 1), (3, 0), (3, 1)], 1 - c)
    tiles([(2, 2), (3, 2), (3, 3)], c, (0, 2))
    keys_values.from_core(1)
    tiles([(3 - c, 2), (3, 3 - c)], 1 - c)
    put(1)
    pass_on(0)
    pass_on(1)
    for n in range(8):
        half, step = (n % 4) // 2, n % 2
        ref = region(1 - c, yl if n < 4 else 1 - yl, half * 8 + 2 * step, 2)
        copy_to(ref, ref, s_o.at[n], r_o.at[n], core).wait_recv()

    def finish():
        for copy in keys_values.across + to_y + to_core:
            copy.wait_send()
        for one_part in keys_values.gathers:
            one_part.sent()

    return finish


class Reduce4:
    def __init__(self, z, send, got, more, more_got, s_1, r_1, s_2, r_2):
        self.one, self.two = z + 1 - 2 * lax.rem(z, 2), 3 - z
        self.far = self.two + 1 - 2 * lax.rem(self.two, 2)
        self.send, self.got, self.more, self.more_got = send, got, more, more_got
        self.sems = (s_1, r_1, s_2, r_2)
        self.first, self.second = {}, []

    def partner(self, part, step):
        return {"z": self.one if part == step else self.two}

    def chunk(self, part, slot):
        return self.far if slot == 1 else (self.two if part else self.one)

    def give(self, part, slot, value):
        self.send[part, slot] = value
        n = part * 2 + slot
        copy = copy_to(
            self.send.at[part, slot], self.got.at[part, slot], self.sems[0].at[n], self.sems[1].at[n], self.partner(part, 0)
        )
        copy.start()
        self.first[part, slot] = copy

    def pass_on(self, part, value):
        self.first[part, 1].wait_recv()
        self.more[part] = (value + self.got[part, 1].astype(F32)).astype(BF)
        copy = copy_to(
            self.more.at[part], self.more_got.at[part], self.sems[2].at[part], self.sems[3].at[part], self.partner(part, 1)
        )
        copy.start()
        self.second.append(copy)

    def own(self, part, value):
        self.first[part, 0].wait_recv()
        value = value + self.got[part, 0].astype(F32)
        self.second[part].wait_recv()
        return value + self.more_got[part].astype(F32)

    def sent(self):
        for copy in list(self.first.values()) + self.second:
            copy.wait_send()


def stage_out(
    new_ref, ctx, xs, wo, gain, fin,
    a_send, a_got, a_more, a_more_got, b_send, b_got, b_more, b_more_got,
    y_send, y_relay, y_got, h_send, h_relay, h_got, own_a, own_b, total,
    squares, fresh, f1, f2, f1_got_0, f1_got_1, f1_got_2,
    a_s1, a_r1, a_s2, a_r2, b_s1, b_r1, b_s2, b_r2, s_y, r_y, s_h, r_h, s_q, r_q, s_f, r_f, s_g, r_g, s_c, r_c,
):
    x, yl, c, z, yh = coords()
    core = {"c": 1 - c}
    y_one, y_two = {"yl": 1 - yl}, {"yl": 1 - yl, "yh": 1 - yh}
    group = [
        {"z": lax.rem(z + dz, 4), "yl": yl + dy - 2 * yl * dy, "c": c + dc - 2 * c * dc}
        for dz in range(4) for dy in range(2) for dc in range(2)
    ][1:]
    others = [{"x": lax.rem(x + dx, 4)} for dx in range(1, 4)]
    f1_got = (f1_got_0, f1_got_1, f1_got_2)

    def sums_of(half, part):
        left = wo[part * 4 * OUT[0]:part * 4 * OUT[0] + 4 * OUT[part], :]
        right = ctx[pl.ds(half * 8, 8)].reshape(512, 512)
        value = lax.dot_general(left, right, (((1,), (1,)), ((), ())), preferred_element_type=F32)
        return value.reshape(4, OUT[part], 512)

    hop, pass_hop = {}, {}
    y_send[...] = sums_of(1 - yh, 1).astype(BF)
    for n in range(4):
        hop[n] = copy_to(y_send.at[n], y_relay.at[n], s_y.at[n], r_y.at[n], y_two if n % 2 else y_one)
        hop[n].start()
    first = Reduce4(z, a_send, a_got, a_more, a_more_got, a_s1, a_r1, a_s2, a_r2)
    for part in range(2):
        own_a[part] = sums_of(part, 0)
        first.give(part, 1, own_a[part, first.chunk(part, 1)].astype(BF))
    for part in range(2):
        first.give(part, 0, own_a[part, first.chunk(part, 0)].astype(BF))
    own_b[...] = sums_of(yh, 1)

    def forward(n):
        hop[n].wait_recv()
        pass_hop[n] = copy_to(y_relay.at[n], y_got.at[n], s_y.at[4 + n], r_y.at[4 + n], y_one if n % 2 else y_two)
        pass_hop[n].start()

    forward(0)
    forward(1)
    for part in range(2):
        first.pass_on(part, own_a[part, first.one if part else first.two])
    forward(2)
    forward(3)
    for part in range(2):
        own_a[part, z] = first.own(part, own_a[part, z])
    h_send[...] = own_a[1 - yh, z].astype(BF)
    spans = (slice(0, 80), slice(80, OUT[0]))
    last = []
    for n, peer in enumerate((y_one, y_two)):
        last.append(copy_to(h_send.at[spans[n]], h_relay.at[spans[n]], s_h.at[n], r_h.at[n], peer))
        last[-1].start()
    second = Reduce4(z, b_send, b_got, b_more, b_more_got, b_s1, b_r1, b_s2, b_r2)
    for n in range(4):
        pass_hop[n].wait_recv()
        own_b[n] = own_b[n] + y_got[n].astype(F32)
    cols = (slice(0, 256), slice(256, 512))
    for slot in (1, 0):
        for part in range(2):
            second.give(part, slot, own_b[second.chunk(part, slot), :, cols[part]].astype(BF))
    for n, peer in enumerate((y_two, y_one)):
        last[n].wait_recv()
        last.append(copy_to(h_relay.at[spans[n]], h_got.at[spans[n]], s_h.at[2 + n], r_h.at[2 + n], peer))
        last[-1].start()
    second.pass_on(0, own_b[second.two, :, cols[0]])
    second.pass_on(1, own_b[second.one, :, cols[1]])
    for part in range(2):
        total[OUT[0]:, cols[part]] = second.own(part, own_b[z, :, cols[part]])
    last[2].wait_recv()
    last[3].wait_recv()
    total[:OUT[0], :] = own_a[yh, z] + h_got[...].astype(F32)
    me = z * 4 + yl * 2 + c
    for m in range(4):
        value = total[:, m * 128:(m + 1) * 128]
        squares[me, m:m + 1, :] = jnp.sum(value * value, axis=0, keepdims=True)
    sums = []
    for e, peer in enumerate(group, 1):
        copy = copy_to(squares.at[me], squares.at[me], s_q.at[e], r_q.at[e], peer)
        copy.start()
        sums.append(copy)
    low = lax.broadcasted_iota(jnp.int32, (WIDE, 128), 1) < 64

    def pair(m, part):
        at = pl.ds(pl.multiple_of(z * 288 + part * WIDE, 32), WIDE)
        a = xs[at, m * 256:m * 256 + 128].astype(F32)
        b = xs[at, m * 256 + 128:m * 256 + 256].astype(F32)
        upper, lower = pltpu.roll(a, 64, 1), pltpu.roll(b, 64, 1)
        return jnp.where(low, jnp.where(yh == 0, a, upper), jnp.where(yh == 0, lower, b))

    for part in range(PARTS):
        for m in range(4):
            fresh[part, m] = pair(m, part)
    for copy in sums:
        copy.wait_recv()
    factor = lax.rsqrt(jnp.sum(squares[...], axis=0) * (1.0 / D) + EPS)
    starts, so_far = [], 0
    for j in range(16):
        starts.append(so_far)
        so_far = so_far + new_ref[j]
    here = pl.ds(x * 2, 2)
    over_x = []
    for part in range(PARTS):
        rows_of = slice(part * WIDE, part * WIDE + WIDE)
        for m in range(4):
            value = total[rows_of, m * 128:(m + 1) * 128] * factor[m:m + 1, :] * gain[rows_of, :]
            fresh[part, m] = fresh[part, m] + value
        for n in range(8):
            sides = []
            for side in range(2):
                j = 2 * n + side
                within = lax.rem(x - starts[j] + 64, 4)
                i = jnp.minimum(lax.div(starts[j] + within - x, 4), 7)
                at = lax.div(i, 2)
                place = lax.rem(i + at, 2) * 4 + at
                value = fresh[part, lax.div(place, 2)]
                value = jnp.where(lax.rem(place, 2) == side, value, pltpu.roll(value, 64, 1))
                sides.append(jnp.where(within < new_ref[j], value, 0.0))
            f1[part, n] = jnp.where(low, sides[0], sides[1]).astype(BF)
        f1_got[part][here] = f1[part, here]
        for d, peer in enumerate(others):
            n = part * 3 + d
            copy = copy_to(f1.at[part, pl.ds(peer["x"] * 2, 2)], f1_got[part].at[here], s_f.at[n], r_f.at[n], peer)
            copy.start()
            over_x.append(copy)
    mine = [sum([jnp.where(x * 4 + n > m, new_ref[m], 0) for m in range(15)]) for n in range(4)]
    out, swap = [], []
    for part in range(PARTS):
        rows_of = slice(part * WIDE, part * WIDE + WIDE)
        for copy in over_x[part * 3:part * 3 + 3]:
            copy.wait_recv()
        for e in range(8):
            n = part * 8 + e
            dz, dy = e // 2, e % 2
            tz, ty = lax.rem(z + dz, 4), yl + dy - 2 * yl * dy
            sides = []
            for side in range(2):
                start = jnp.where(ty == 0, mine[side], mine[2 + side])
                sides.append(f1_got[part][lax.rem(start + tz, 4) * 2 + ty].astype(F32))
            value = jnp.where(low, sides[0], sides[1]).astype(BF)
            at = (z * 2 + yl) * 2 + c
            if e == 0:
                fin[at, rows_of, :] = value
            else:
                f2[part, e] = value
                copy = copy_to(f2.at[part, e], fin.at[at, rows_of], s_g.at[n], r_g.at[n], {"z": tz, "yl": ty})
                copy.start()
                out.append(copy)
    for part in range(PARTS):
        rows_of = slice(part * WIDE, part * WIDE + WIDE)
        for e in range(8):
            n = part * 8 + e
            dz, dy = e // 2, e % 2
            at = (mod4(z - dz) * 2 + yl + dy - 2 * yl * dy) * 2 + c
            ref = fin.at[at, rows_of]
            if e > 0:
                copy_to(ref, ref, s_g.at[n], r_g.at[n], core).wait_recv()
            copy = copy_to(ref, ref, s_c.at[n], r_c.at[n], core)
            copy.start()
            swap.append(copy)
    for copy in swap:
        copy.wait_recv()
    first.sent()
    second.sent()
    for copy in list(hop.values()) + list(pass_hop.values()) + last + sums + over_x + out + swap:
        copy.wait_send()


STAGE_IN = [
    VM((1152, 512), BF), VM((1152, 256), BF), VM((1152, 256), BF),
    VM((1152, 128), F32), VM((128, 128), F32), VM((64, 512), F32), VM((64, 512), F32),
    VM((576, 512), BF), VM((PARTS, 8, WIDE, 128), BF), VM((24, WIDE, 128), BF), VM((24, WIDE, 128), BF), VM((24, WIDE, 128), BF), VM((1152, 1024), BF), VM((16, 8, 128), F32),
    VM((2, 512, 512), F32), VM((2, 512, 512), F32), VM((512, 512), BF), VM((512, 512), BF), VM((2, 512, 512), F32),
    DMA((6,)), DMA((8 * PARTS,)), DMA((8 * PARTS,)), DMA((8 * PARTS,)), DMA((8 * PARTS,)), DMA((8 * PARTS,)), DMA((8 * PARTS,)),
    DMA((18,)), DMA((18,)), DMA((6,)), DMA((6,)), DMA((6 * PARTS,)), DMA((6 * PARTS,)), DMA((16,)), DMA((16,)),
    DMA((6,)), DMA((6,)), DMA((6,)), DMA((6,)),
]
STAGE_ATTEND = [
    VM((4, 256, 128), BF), VM((4, 256, 128), F32), VM((4, 256, 128), F32),
    DMA((4,)), DMA((4,)), DMA((8,)), DMA((8,)),
]
STAGE_OUT = (
    [VM((2, 2, OUT[0], 512), BF), VM((2, 2, OUT[0], 512), BF), VM((2, OUT[0], 512), BF), VM((2, OUT[0], 512), BF)]
    + [VM((2, 2, OUT[1], 256), BF), VM((2, 2, OUT[1], 256), BF), VM((2, OUT[1], 256), BF), VM((2, OUT[1], 256), BF)]
    + [VM((4, OUT[1], 512), BF)] * 3
    + [VM((OUT[0], 512), BF)] * 3
    + [VM((2, 4, OUT[0], 512), F32), VM((4, OUT[1], 512), F32), VM((288, 512), F32)]
    + [VM((16, 4, 128), F32), VM((PARTS, 4, WIDE, 128), F32)]
    + [VM((PARTS, 8, WIDE, 128), BF)] * 2
    + [VM((8, WIDE, 128), BF)] * PARTS
    + [DMA((4,)), DMA((4,)), DMA((2,)), DMA((2,))] * 2
    + [DMA((8,)), DMA((8,)), DMA((4,)), DMA((4,)), DMA((16,)), DMA((16,)), DMA((3 * PARTS,)), DMA((3 * PARTS,))]
    + [DMA((8 * PARTS,))] * 4
)
SHARED = [
    VM((256, 512), BF), VM((4, 256, 128), BF), VM((1152, 1024), BF), VM((1152, 512), BF), VM((16, 64, 512), BF),
    VM((288, 128), F32), VM((8, 256, 512), BF), DMA((12,)), DMA((12,)), DMA((4,)), DMA((4,)),
]


def kernel(old_ref, new_ref, order_ref, xt_in, pre_ref, post_ref, wq_in, wk_in, wv_in, wo_in, fin, *scratch):
    q, kv, xs, wo, ctx, gain_out, kvs, s_x, r_x, s_c, r_c = scratch[:11]
    scratch = scratch[11:]
    keys_values = KeysValues(kv, kvs, s_x, r_x, s_c, r_c)
    own_in, scratch = scratch[:len(STAGE_IN)], scratch[len(STAGE_IN):]
    own_attend, own_out = scratch[:len(STAGE_ATTEND)], scratch[len(STAGE_ATTEND):]
    end_in = stage_in(
        old_ref, order_ref, xt_in, pre_ref, post_ref, wq_in, wk_in, wv_in, wo_in, q, kv, xs, wo, gain_out, *own_in,
        keys_values,
    )
    end_attend = stage_attend(q, ctx, keys_values, kvs, *own_attend)
    end_in()
    stage_out(new_ref, ctx, xs, wo, gain_out, fin, *own_out)
    end_attend()


def run(old_blocks, new_blocks, order, xt, pre_gain, post_gain, w_query, w_key, w_value, w_out_t):
    smem = pl.BlockSpec(memory_space=pltpu.SMEM)
    vmem = pl.BlockSpec(memory_space=pltpu.VMEM)
    hbm = pl.BlockSpec(memory_space=pltpu.HBM)
    return pl.pallas_call(
        kernel,
        name="sublayer",
        out_shape=jax.ShapeDtypeStruct((16, 288, 128), BF),
        in_specs=[smem, smem, smem, hbm, vmem, vmem, hbm, hbm, hbm, hbm],
        out_specs=vmem,
        scratch_shapes=SHARED + STAGE_IN + STAGE_ATTEND + STAGE_OUT,
        compiler_params=pltpu.CompilerParams(collective_id=0, has_side_effects=True, vmem_limit_bytes=62 * 2**20),
    )(old_blocks, new_blocks, order, xt, pre_gain, post_gain, w_query, w_key, w_value, w_out_t)


def per_device(
    x_old, old_blocks, new_blocks, order, pre_gain, post_gain, w_query, w_key, w_value, w_out_t
):
    c = lax.axis_index("c")
    fin = run(
        old_blocks, new_blocks, order, x_old.T, pre_gain.reshape(36, 128), post_gain.reshape(36, 128),
        w_query, w_key, w_value, w_out_t,
    )
    return lax.dynamic_slice(fin, (0, 0, c * 64), (16, 288, 64)).reshape(4608, 64).T


def solution(mesh):
    torus = Mesh(mesh.devices.reshape(4, 2, 2, 4, 2), ("x", "yl", "c", "z", "yh"))
    seq, tp = ("x", "yl", "c"), ("z", "yh")
    both = P(seq, tp)
    in_specs = (both, P(), P(), P(), P(), P(), both, both, both, both)
    return jax.shard_map(
        per_device, mesh=torus, in_specs=in_specs, out_specs=P(seq + tp, None), check_vma=False
    )
```

```python
import functools
import math

import jax
import jax.numpy as jnp
from jax import lax
from jax.experimental import pallas as pl
from jax.experimental.pallas import tpu as pltpu
from jax.sharding import Mesh
from jax.sharding import PartitionSpec as P

D = 4608
HEADS = 32
HEAD = 128
BLOCK = 128
EPS = 1e-06
BF = jnp.bfloat16
F32 = jnp.float32
VM = pltpu.VMEM
OUT = (160, 128)
PARTS = 3
WIDE = 288 // PARTS
DMA = pltpu.SemaphoreType.DMA


def kept(at, c):
    return 2 * at + lax.rem(at + c, 2)


def coords():
    return tuple(lax.axis_index(name) for name in ("x", "yl", "c", "z", "yh"))


def copy_to(src, dst, send_sem, recv_sem, device):
    return pltpu.make_async_remote_copy(
        src_ref=src,
        dst_ref=dst,
        send_sem=send_sem,
        recv_sem=recv_sem,
        device_id=device,
        device_id_type=pl.DeviceIdType.MESH,
    )


def greet(devices):
    sem = pltpu.get_barrier_semaphore()
    for device in devices:
        pl.semaphore_signal(sem, inc=1, device_id=device, device_id_type=pl.DeviceIdType.MESH)


def greeted(devices):
    pl.semaphore_wait(pltpu.get_barrier_semaphore(), len(devices))


def mod4(v):
    return lax.rem(v + 4, 4)


def arrived(ref, sem):
    copy_to(ref, ref, sem, sem, {"c": 1 - lax.axis_index("c")}).wait_recv()


def gone(ref, sem):
    copy_to(ref, ref, sem, sem, {"c": 1 - lax.axis_index("c")}).wait_send()


class Gather4:
    def __init__(self, views, axis, me, send, recv, size):
        one, two = me + 1 - 2 * lax.rem(me, 2), 3 - me
        far = two + 1 - 2 * lax.rem(two, 2)
        self.moves = [
            (me, one, 0, one),
            (me, two, 1, two),
            (me, two, 0, two),
            (me, one, 1, one),
            (one, far, 0, two),
            (two, far, 1, one),
        ]
        self.views, self.axis, self.send, self.recv, self.size = views, axis, send, recv, size

    def go(self, *moves):
        for move in moves:
            sent, _, half, partner = self.moves[move]
            for view in self.views:
                ref = view(sent, half)
                copy_to(ref, ref, self.send(move // 4), self.recv(move // 2), {self.axis: partner}).start()

    def start(self):
        self.go(0, 1, 2, 3)

    def relay(self):
        arrived(self.size(2), self.recv(0))
        self.go(4, 5)

    def near(self):
        arrived(self.size(2), self.recv(1))

    def far(self):
        arrived(self.size(2), self.recv(2))

    def sent(self):
        gone(self.size(4), self.send(0))
        gone(self.size(2), self.send(1))


def some(sems, start):
    return lambda n: sems.at[start + n]


def rows(ref, start, size, unit=16):
    return ref.at[pl.ds(pl.multiple_of(start, unit), size)]


def lanes(start, size):
    return pl.ds(pl.multiple_of(start, 128), size)


def columns(dst, table, chunk_of, count):
    lane = lax.broadcasted_iota(jnp.int32, (32, 128), 1)

    def body(n, _):
        feature = chunk_of(lax.div(n, 9)) * 288 + lax.rem(n, 9) * 32
        part = table[pl.ds(pl.multiple_of(lax.rem(feature, 128), 32), 32), :]
        value = jnp.sum(jnp.where(lane == lax.div(feature, 128), part, 0.0), axis=1, keepdims=True)
        dst[pl.ds(pl.multiple_of(n * 32, 32), 32), :] = jnp.broadcast_to(value, (32, 128))
        return 0

    lax.fori_loop(0, count * 9, body, 0)


def stage_in(
    old_ref, order_ref, xt_in, pre_ref, post_ref, wq_in, wk_in, wv_in, wo_in,
    q_out, kv_out, xs, wo, gain_out,
    wq, wk, wv, gain, table, cos, sin, xt, slots, landed_0, landed_1, landed_2, normed, squares, near, other, to_y, from_y, mine,
    s_w, s_one, r_one, s_two, r_two, s_three, r_three, s_wg, r_wg, s_og, r_og, s_z, r_z, s_q, r_q, s_c, r_c, s_y, r_y,
    keys_values,
):
    x, yl, c, z, yh = coords()
    landed = (landed_0, landed_1, landed_2)
    ring_peers = [
        {"x": lax.rem(x + dx, 4), "c": c + dc - 2 * c * dc} for dx in range(4) for dc in range(2)
    ][1:]
    y_one = {"yl": 1 - yl}
    y_two = {"yl": 1 - yl, "yh": 1 - yh}
    group = [
        {"z": lax.rem(z + dz, 4), "yl": yl + dy - 2 * yl * dy, "c": c + dc - 2 * c * dc}
        for dz in range(4) for dy in range(2) for dc in range(2)
    ][1:]
    greet(ring_peers + [y_two] + group)
    into = pltpu.make_async_copy(xt_in, xt, s_w.at[1])
    into.start()
    at = pl.ds(pl.multiple_of(x * 288, 16), 288)
    owns = [
        pltpu.make_async_copy(src, dst.at[at], s_w.at[0]) for src, dst in ((wq_in, wq), (wk_in, wk), (wv_in, wv))
    ]

    def out_rows(chunk, half):
        return rows(wo, half * 4 * OUT[0] + chunk * OUT[half], OUT[half])

    for half in range(2):
        part = wo_in.at[pl.ds(half * OUT[0], OUT[half])]
        owns.append(pltpu.make_async_copy(part, out_rows(x, half), s_w.at[0]))
    for copy in owns:
        copy.start()
    starts, total = [], 0
    for m in range(16):
        starts.append(total)
        total = total + old_ref[m]
    k = order_ref[x * 4 + yl * 2 + c]
    first = sum([jnp.where(k > m, old_ref[m], 0) for m in range(15)])
    into.wait()
    for r in range(4):
        b = lax.rem(r - first + 64, 4)
        for h in range(2):
            for half in range(PARTS):
                at_rows = slice(h * 288 + half * WIDE, h * 288 + half * WIDE + WIDE)
                part = [xt[at_rows, n * 128:(n + 1) * 128] for n in range(4)]
                low = jnp.where(b == 0, part[0], part[1])
                slots[half, r * 2 + h] = jnp.where(b < 2, low, jnp.where(b == 2, part[2], part[3]))
    here = x * 2 + c
    for half in range(PARTS):
        landed[half][here] = slots[half, here]
    greeted(ring_peers + [y_two] + group)
    for half in range(PARTS):
        for d, peer in enumerate(ring_peers, 1):
            copy_to(
                slots.at[half, peer["x"] * 2 + peer["c"]], landed[half].at[here],
                s_one.at[half], r_one.at[half * 4 + d // 2], peer,
            ).start()
    everything = wo.at[pl.ds(0, 864)]
    pltpu.make_async_copy(everything, everything, s_w.at[0]).wait()

    def half_rows(ref):
        return lambda chunk, half: rows(ref, chunk * 288 + half * 144, 144)

    weights = Gather4(
        [half_rows(r) for r in (wq, wk, wv)], "x", x, some(s_wg, 0), some(r_wg, 0), lambda n: wq.at[pl.ds(0, 288 * n)]
    )
    weights.start()
    straight = yl == yh

    def slot_pair(half, dx, where):
        return landed[half].at[pl.ds(where * 8 + mod4(x - dx) * 2, 2)]

    def relay_y(n):
        half, dx = n // 4, n % 4
        arrived(slot_pair(half, dx, 1), r_two.at[n])
        copy = copy_to(slot_pair(half, dx, 1), slot_pair(half, dx, 2), s_three.at[half], r_three.at[half], y_one)
        pl.when(straight)(copy.start)

    for half in range(PARTS):
        for dx in range(4):
            n = half * 4 + dx
            from_x = slot_pair(half, dx, 0) if dx > 0 else landed[half].at[x * 2 + 1 - c]
            arrived(from_x, r_one.at[n])
            copy_to(slot_pair(half, dx, 0), slot_pair(half, dx, 1), s_two.at[half], r_two.at[n], y_two).start()
            copy = copy_to(slot_pair(half, dx, 0), slot_pair(half, dx, 2), s_three.at[half], r_three.at[half], y_one)
            pl.when(jnp.logical_not(straight))(copy.start)
            if half == 2:
                relay_y(dx)
    me = z * 4 + yl * 2 + c
    first_buffer = jnp.where(straight, 0, 1)

    def part_rows(part):
        return lambda chunk, half: rows(xs, chunk * 288 + part * WIDE + half * (WIDE // 2), WIDE // 2)

    gathers = [
        Gather4(
            [part_rows(part)], "z", z, some(s_z, 2 * part), some(r_z, 3 * part),
            lambda n: xs.at[pl.ds(0, (WIDE // 2) * n)],
        )
        for part in range(PARTS)
    ]
    sources = []
    for place in range(8):
        g = x + 4 * kept(place % 4, place // 4)
        shard = sum([jnp.where(starts[m] <= g, 1, 0) for m in range(16)]) - 1
        holder = sum([jnp.where(order_ref[p] == shard, p, 0) for p in range(16)])
        y_source = lax.rem(lax.div(holder, 2), 2)
        sources.append(jnp.where(y_source == yh, first_buffer, 2) * 8 + lax.div(holder, 4) * 2 + lax.rem(holder, 2))

    def pick(half):
        arrived(landed[half].at[pl.ds(16, 8)], r_three.at[half])
        for place in range(8):
            block = landed[half][sources[place]]
            xs[pl.ds(pl.multiple_of(z * 288 + half * WIDE, 32), WIDE), place * 128:(place + 1) * 128] = block
            wide = block.astype(F32)
            square = jnp.sum(wide * wide, axis=0, keepdims=True)
            if half > 0:
                square = square + squares[me, place:place + 1, :]
            squares[me, place:place + 1, :] = square
        gathers[half].start()

    for n in range(4, 12):
        if n in (6, 10):
            pick((n - 6) // 4)
        relay_y(n)
    pick(2)
    weights.relay()
    wo_all = Gather4(
        [out_rows], "x", x, some(s_og, 0), some(r_og, 0), lambda n: wo.at[pl.ds(0, 144 * n)]
    )
    wo_all.start()
    for peer in group:
        copy_to(squares.at[me], squares.at[me], s_q.at[0], r_q.at[0], peer).start()
    table[...] = jnp.zeros_like(table)
    table[0:36, :] = pre_ref[...]
    table[...] = table[...].T
    columns(gain, table, lambda n: n * 4 + yl * 2 + c, 4)
    table[...] = jnp.zeros_like(table)
    table[0:36, :] = post_ref[...]
    table[...] = table[...].T
    columns(gain_out, table, lambda n: z * 4 + yl * 2 + c, 1)
    gathers[0].relay()
    half_head = HEAD // 2
    inverse = jnp.exp(
        lax.broadcasted_iota(jnp.int32, (half_head, 128), 0).astype(F32) * (-2.0 * math.log(10000.0) / HEAD)
    )
    for p in range(4):
        place_of = (x + 4 * kept(p, c)) * BLOCK + lax.broadcasted_iota(jnp.int32, (half_head, 128), 1)
        angle = inverse * place_of.astype(F32)
        cos[:, p * 128:(p + 1) * 128] = jnp.cos(angle)
        sin[:, p * 128:(p + 1) * 128] = jnp.sin(angle)
    for part in (1, 2):
        gathers[part].relay()
    arrived(squares.at[pl.ds(0, 15)], r_q.at[0])
    factor = lax.rsqrt(jnp.sum(squares[...], axis=0) * (1.0 / D) + EPS)

    def norm(chunk):
        for place in range(8):
            scale = factor[place:place + 1, :]

            def norm_rows(n, _, place=place, scale=scale):
                part = pl.ds(pl.multiple_of(chunk * 288 + n * 144, 16), 144)
                at = (part, slice(place * 128, (place + 1) * 128))
                normed[at] = (xs[at].astype(F32) * scale * gain[part, :]).astype(BF)
                return 0

            lax.fori_loop(0, 2, norm_rows, 0)

    pieces = {"q": (slice(0, 256), wq, 256), "k": (slice(256, 384), wk, 128), "v": (slice(384, 512), wv, 128)}

    def corner(dst, y, core, late, names="qkv"):
        low = lax.div(z, 2)
        part = pl.ds(pl.multiple_of((1 - low if late else low) * 576, 16), 576)
        right = normed[part, lanes(core * 512, 512)]
        for name in names:
            to, table_of, width = pieces[name]
            left = table_of[part, lanes(y * width, width)]
            value = lax.dot_general(left, right, (((0,), (0,)), ((), ())), preferred_element_type=F32)
            if late:
                dst[to, :] += value
            else:
                dst[to, :] = value

    norm(z)
    for one_part in gathers:
        one_part.near()
    norm(z + 1 - 2 * lax.rem(z, 2))
    weights.near()
    weights.far()
    corners = [
        (near.at[0], 1 - yl, 1 - c), (mine.at[0], 1 - yl, c), (near.at[1], yl, 1 - c), (mine.at[1], yl, c),
    ]
    for dst, y, core in corners:
        corner(dst, y, core, False)
    norm(3 - z)
    wo_all.relay()
    for one_part in gathers:
        one_part.far()
    far = 3 - z
    norm(far + 1 - 2 * lax.rem(far, 2))
    core = {"c": 1 - c}

    def over_core(n, name):
        to = pieces[name][0]
        recv = r_c.at["kvq".index(name) if n == 0 else 3]
        copy_to(near.at[n, to], other.at[n, to], s_c.at[0], recv, core).start()

    first_rows, last_rows = slice(0, 256), slice(256, 512)
    k_part, v_part = slice(256, 384), slice(384, 512)
    spans = (
        (0, k_part, first_rows), (1, v_part, first_rows), (2, k_part, last_rows), (3, v_part, last_rows),
        (4, slice(0, 256), first_rows), (5, slice(0, 256), last_rows),
    )

    def over_y(name):
        to = pieces[name][0]
        arrived(other.at[0, to], r_c.at["kvq".index(name)])
        to_y[to, :] = (mine[0, to, :] + other[0, to, :]).astype(BF)
        for at, part, cols in {"k": spans[:1], "v": spans[1:4], "q": spans[4:]}[name]:
            copy_to(to_y.at[part, cols], from_y.at[part, cols], s_y.at[0], r_y.at[at // 2 if at < 4 else at - 2], y_one).start()

    for name in "kv":
        corner(*corners[0], True, name)
        over_core(0, name)
    corner(*corners[1], True, "kv")
    over_y("k")
    corner(*corners[0], True, "q")
    over_core(0, "q")
    over_y("v")
    corner(*corners[1], True, "q")
    over_y("q")
    corner(*corners[2], True)
    for name in "kvq":
        over_core(1, name)
    corner(*corners[3], True)
    arrived(other.at[1], r_c.at[3])
    scale_q = (D // HEADS) ** (-0.5)

    def summed(part, cols):
        return mine[1, part, cols] + other[1, part, cols] + from_y[part, cols].astype(F32)

    def turned(value, cols):
        a, b = value[:64], value[64:]
        return jnp.concatenate(
            [a * cos[:, cols] - b * sin[:, cols], b * cos[:, cols] + a * sin[:, cols]], axis=0
        ).astype(BF)

    for late, cols in enumerate((first_rows, last_rows)):
        arrived(from_y.at[pl.ds(256, 256), cols], r_y.at[late])
        key = turned(summed(k_part, cols), cols)
        value = summed(v_part, cols).astype(BF)
        for p in range(2):
            kv_out[2 * late + p, :128, :] = key[:, p * 128:(p + 1) * 128]
            kv_out[2 * late + p, 128:, :] = value[:, p * 128:(p + 1) * 128]
        keys_values.send(late)
    for late in range(2):
        keys_values.gathers[late].relay()
    for late, cols in enumerate((first_rows, last_rows)):
        arrived(from_y.at[pl.ds(0, 256), cols], r_y.at[2 + late])
        for h in range(2):
            part = slice(h * 128, (h + 1) * 128)
            a, b = summed(slice(h * 128, h * 128 + 64), cols), summed(slice(h * 128 + 64, h * 128 + 128), cols)
            turn_a = a * cos[:, cols] - b * sin[:, cols]
            turn_b = b * cos[:, cols] + a * sin[:, cols]
            q_out[part, cols] = (jnp.concatenate([turn_a, turn_b], axis=0) * scale_q).astype(BF)

    def finish():
        wo_all.near()
        wo_all.far()
        for half in range(PARTS):
            gone(slots.at[half, pl.ds(0, 7)], s_one.at[half])
            gone(landed[half].at[pl.ds(0, 8)], s_two.at[half])
            gone(landed[half].at[pl.ds(0, 8)], s_three.at[half])
        gone(squares.at[pl.ds(0, 15)], s_q.at[0])
        gone(near, s_c.at[0])
        gone(to_y, s_y.at[0])
        weights.sent()
        wo_all.sent()
        for one_part in gathers:
            one_part.sent()

    return finish


class KeysValues:
    def __init__(self, kv_ref, kvs, s_x, r_x, s_c, r_c):
        x, _, c, _, _ = coords()

        def block(late):
            return lambda chunk, half: kvs.at[kept(2 * late + half, c), :, lanes(chunk * 128, 128)]

        self.gathers = [
            Gather4(
                [block(late)], "x", x, some(s_x, 2 * late), some(r_x, 3 * late),
                lambda n: kvs.at[0, :, pl.ds(0, 128 * n)],
            )
            for late in range(2)
        ]
        self.kv_ref, self.kvs, self.s_c, self.r_c = kv_ref, kvs, s_c, r_c

    def send(self, late):
        x, _, c, _, _ = coords()
        for p in (2 * late, 2 * late + 1):
            self.kvs[kept(p, c), :, lanes(x * 128, 128)] = self.kv_ref[p]
        self.gathers[late].start()

    def to_core(self, late):
        _, _, c, _, _ = coords()
        self.gathers[late].near()
        self.gathers[late].far()
        for p in (2 * late, 2 * late + 1):
            ref = self.kvs.at[kept(p, c)]
            copy_to(ref, ref, self.s_c.at[0], self.r_c.at[late], {"c": 1 - c}).start()

    def from_core(self, late):
        arrived(self.kvs.at[pl.ds(0, 2)], self.r_c.at[late])

    def sent(self):
        gone(self.kvs.at[pl.ds(0, 4)], self.s_c.at[0])
        for gather in self.gathers:
            gather.sent()


def stage_attend(q_ref, ctx, keys_values, kvs, qs, acc, den, s_y, r_y, s_o, r_o):
    x, yl, c, z, yh = coords()
    core, y_one = {"c": 1 - c}, {"yl": 1 - yl}
    for p in range(4):
        for h in range(2):
            part = q_ref[h * 128:(h + 1) * 128, p * 128:(p + 1) * 128].astype(F32)
            qs[p, h * 128:(h + 1) * 128, :] = part.T.astype(BF)
    acc[...] = jnp.zeros_like(acc)
    den[...] = jnp.zeros_like(den)
    keys_values.to_core(0)

    def tiles(pairs, core_at, diagonal=()):
        pairs = [(p, kept(e, core_at), n in diagonal) for n, (p, e) in enumerate(pairs)]
        scores = [jnp.dot(qs[p], kvs[group, :128, :], preferred_element_type=F32) for p, group, _ in pairs]
        for (p, group, masked), score in zip(pairs, scores):
            weight = jnp.exp2((50.0 * math.log2(math.e)) * jnp.tanh(score * (1.0 / 50.0)))
            if masked:
                row = lax.rem(lax.broadcasted_iota(jnp.int32, (256, 512), 0), 128)
                col = lax.broadcasted_iota(jnp.int32, (256, 512), 1)
                weight = jnp.where(col - row <= x * 128, weight, 0.0)
            den[p] += sum([weight[:, n:n + 128] for n in range(0, 512, 128)])
            acc[p] += lax.dot_general(
                weight.astype(BF), kvs[group, 128:, :], (((1,), (1,)), ((), ())), preferred_element_type=F32
            )

    def region(core_at, y_at, at, size):
        return ctx.at[pl.ds(at + core_at * 4, size), :, lanes(y_at * 256, 256)]

    def put(step):
        for p in (2 * step, 2 * step + 1):
            for h in range(2):
                part = slice(h * 128, (h + 1) * 128)
                total = jnp.sum(den[p, part, :], axis=1, keepdims=True)
                value = (acc[p, part, :] / total).astype(BF)
                cols = lanes(yl * 256 + h * 128, 128)
                ctx[c * 4 + p, :, cols] = value[:64]
                ctx[8 + c * 4 + p, :, cols] = value[64:]
        for half in range(2):
            ref = region(c, yl, half * 8 + 2 * step, 2)
            copy_to(ref, ref, s_y.at[0], r_y.at[step], y_one).start()
            copy_to(ref, ref, s_o.at[0], r_o.at[0], core).start()

    def pass_on(step):
        arrived(ctx.at[pl.ds(0, 4), :, pl.ds(0, 256)], r_y.at[step])
        for half in range(2):
            ref = region(c, 1 - yl, half * 8 + 2 * step, 2)
            copy_to(ref, ref, s_o.at[0], r_o.at[0], core).start()

    tiles([(0, 0), (1, 0), (1, 1)], c, (0, 2))
    keys_values.from_core(0)
    tiles([(1 - c, 0), (1, 1 - c)], 1 - c)
    put(0)
    tiles([(2, 0), (2, 1), (3, 0), (3, 1)], c)
    keys_values.to_core(1)
    tiles([(2, 0), (2, 1), (3, 0), (3, 1)], 1 - c)
    tiles([(2, 2), (3, 2), (3, 3)], c, (0, 2))
    keys_values.from_core(1)
    tiles([(3 - c, 2), (3, 3 - c)], 1 - c)
    put(1)
    pass_on(0)
    pass_on(1)
    arrived(ctx.at[:, :, pl.ds(0, 256)], r_o.at[0])

    def finish():
        gone(ctx.at[pl.ds(0, 8), :, pl.ds(0, 256)], s_y.at[0])
        gone(ctx.at[:, :, pl.ds(0, 256)], s_o.at[0])
        keys_values.sent()

    return finish


class Reduce4:
    def __init__(self, z, send, got, more, more_got, s, r):
        self.one, self.two = z + 1 - 2 * lax.rem(z, 2), 3 - z
        self.far = self.two + 1 - 2 * lax.rem(self.two, 2)
        self.send, self.got, self.more, self.more_got, self.s, self.r = send, got, more, more_got, s, r

    def partner(self, part, step):
        return {"z": self.one if part == step else self.two}

    def chunk(self, part, slot):
        return self.far if slot == 1 else (self.two if part else self.one)

    def give(self, part, slot, value):
        self.send[part, slot] = value
        copy_to(
            self.send.at[part, slot], self.got.at[part, slot], self.s.at[0], self.r.at[slot], self.partner(part, 0)
        ).start()

    def pass_on(self, values):
        arrived(self.got.at[0], self.r.at[1])
        for part, value in enumerate(values):
            self.more[part] = (value + self.got[part, 1].astype(F32)).astype(BF)
            copy_to(
                self.more.at[part], self.more_got.at[part], self.s.at[1], self.r.at[2], self.partner(part, 1)
            ).start()

    def own(self, values):
        arrived(self.got.at[0], self.r.at[0])
        arrived(self.more_got, self.r.at[2])
        return [
            value + self.got[part, 0].astype(F32) + self.more_got[part].astype(F32) for part, value in enumerate(values)
        ]

    def sent(self):
        gone(self.send, self.s.at[0])
        gone(self.more, self.s.at[1])


def stage_out(
    new_ref, ctx, xs, wo, gain, fin,
    a_send, a_got, a_more, a_more_got, b_send, b_got, b_more, b_more_got,
    y_send, y_relay, y_got, h_send, h_relay, h_got, own_a, own_b, total,
    squares, fresh, f1, f2, f1_got_0, f1_got_1, f1_got_2,
    a_s, a_r, b_s, b_r, s_y, r_y, s_h, r_h, s_q, r_q, s_f, r_f, s_g, r_g, s_c, r_c,
):
    x, yl, c, z, yh = coords()
    core = {"c": 1 - c}
    y_one, y_two = {"yl": 1 - yl}, {"yl": 1 - yl, "yh": 1 - yh}
    group = [
        {"z": lax.rem(z + dz, 4), "yl": yl + dy - 2 * yl * dy, "c": c + dc - 2 * c * dc}
        for dz in range(4) for dy in range(2) for dc in range(2)
    ][1:]
    others = [{"x": lax.rem(x + dx, 4)} for dx in range(1, 4)]
    f1_got = (f1_got_0, f1_got_1, f1_got_2)

    def sums_of(half, part):
        left = wo[part * 4 * OUT[0]:part * 4 * OUT[0] + 4 * OUT[part], :]
        right = ctx[pl.ds(half * 8, 8)].reshape(512, 512)
        value = lax.dot_general(left, right, (((1,), (1,)), ((), ())), preferred_element_type=F32)
        return value.reshape(4, OUT[part], 512)

    y_send[...] = sums_of(1 - yh, 1).astype(BF)
    for n in range(4):
        copy_to(y_send.at[n], y_relay.at[n], s_y.at[0], r_y.at[n // 2], y_two if n % 2 else y_one).start()
    first = Reduce4(z, a_send, a_got, a_more, a_more_got, a_s, a_r)
    for part in range(2):
        own_a[part] = sums_of(part, 0)
        first.give(part, 1, own_a[part, first.chunk(part, 1)].astype(BF))
    for part in range(2):
        first.give(part, 0, own_a[part, first.chunk(part, 0)].astype(BF))
    own_b[...] = sums_of(yh, 1)

    def forward(step):
        arrived(y_relay.at[pl.ds(0, 2)], r_y.at[step])
        for n in (2 * step, 2 * step + 1):
            copy_to(y_relay.at[n], y_got.at[n], s_y.at[1], r_y.at[2], y_one if n % 2 else y_two).start()

    forward(0)
    first.pass_on([own_a[0, first.two], own_a[1, first.one]])
    forward(1)
    for part, value in enumerate(first.own([own_a[0, z], own_a[1, z]])):
        own_a[part, z] = value
    h_send[...] = own_a[1 - yh, z].astype(BF)
    spans = (slice(0, 80), slice(80, OUT[0]))
    for n, peer in enumerate((y_one, y_two)):
        copy_to(h_send.at[spans[n]], h_relay.at[spans[n]], s_h.at[0], r_h.at[0], peer).start()
    second = Reduce4(z, b_send, b_got, b_more, b_more_got, b_s, b_r)
    arrived(y_got, r_y.at[2])
    own_b[...] = own_b[...] + y_got[...].astype(F32)
    cols = (slice(0, 256), slice(256, 512))
    for slot in (1, 0):
        for part in range(2):
            second.give(part, slot, own_b[second.chunk(part, slot), :, cols[part]].astype(BF))
    arrived(h_relay, r_h.at[0])
    for n, peer in enumerate((y_two, y_one)):
        copy_to(h_relay.at[spans[n]], h_got.at[spans[n]], s_h.at[1], r_h.at[1], peer).start()
    second.pass_on([own_b[second.two, :, cols[0]], own_b[second.one, :, cols[1]]])
    for part, value in enumerate(second.own([own_b[z, :, cols[0]], own_b[z, :, cols[1]]])):
        total[OUT[0]:, cols[part]] = value
    arrived(h_got, r_h.at[1])
    total[:OUT[0], :] = own_a[yh, z] + h_got[...].astype(F32)
    me = z * 4 + yl * 2 + c
    for m in range(4):
        value = total[:, m * 128:(m + 1) * 128]
        squares[me, m:m + 1, :] = jnp.sum(value * value, axis=0, keepdims=True)
    for peer in group:
        copy_to(squares.at[me], squares.at[me], s_q.at[0], r_q.at[0], peer).start()
    low = lax.broadcasted_iota(jnp.int32, (WIDE, 128), 1) < 64

    def pair(m, part):
        at = pl.ds(pl.multiple_of(z * 288 + part * WIDE, 32), WIDE)
        a = xs[at, m * 256:m * 256 + 128].astype(F32)
        b = xs[at, m * 256 + 128:m * 256 + 256].astype(F32)
        upper, lower = pltpu.roll(a, 64, 1), pltpu.roll(b, 64, 1)
        return jnp.where(low, jnp.where(yh == 0, a, upper), jnp.where(yh == 0, lower, b))

    for part in range(PARTS):
        for m in range(4):
            fresh[part, m] = pair(m, part)
    arrived(squares.at[pl.ds(0, 15)], r_q.at[0])
    factor = lax.rsqrt(jnp.sum(squares[...], axis=0) * (1.0 / D) + EPS)
    starts, so_far = [], 0
    for j in range(16):
        starts.append(so_far)
        so_far = so_far + new_ref[j]
    here = pl.ds(x * 2, 2)
    for part in range(PARTS):
        rows_of = slice(part * WIDE, part * WIDE + WIDE)
        for m in range(4):
            value = total[rows_of, m * 128:(m + 1) * 128] * factor[m:m + 1, :] * gain[rows_of, :]
            fresh[part, m] = fresh[part, m] + value
        for n in range(8):
            sides = []
            for side in range(2):
                j = 2 * n + side
                within = lax.rem(x - starts[j] + 64, 4)
                i = jnp.minimum(lax.div(starts[j] + within - x, 4), 7)
                at = lax.div(i, 2)
                place = lax.rem(i + at, 2) * 4 + at
                value = fresh[part, lax.div(place, 2)]
                value = jnp.where(lax.rem(place, 2) == side, value, pltpu.roll(value, 64, 1))
                sides.append(jnp.where(within < new_ref[j], value, 0.0))
            f1[part, n] = jnp.where(low, sides[0], sides[1]).astype(BF)
        f1_got[part][here] = f1[part, here]
        for peer in others:
            copy_to(
                f1.at[part, pl.ds(peer["x"] * 2, 2)], f1_got[part].at[here], s_f.at[0], r_f.at[part], peer
            ).start()
    mine = [sum([jnp.where(x * 4 + n > m, new_ref[m], 0) for m in range(15)]) for n in range(4)]
    for part in range(PARTS):
        rows_of = slice(part * WIDE, part * WIDE + WIDE)
        arrived(f1_got[part].at[pl.ds(0, 6)], r_f.at[part])
        for e in range(8):
            dz, dy = e // 2, e % 2
            tz, ty = lax.rem(z + dz, 4), yl + dy - 2 * yl * dy
            sides = []
            for side in range(2):
                start = jnp.where(ty == 0, mine[side], mine[2 + side])
                sides.append(f1_got[part][lax.rem(start + tz, 4) * 2 + ty].astype(F32))
            value = jnp.where(low, sides[0], sides[1]).astype(BF)
            at = z * 2 + yl
            if e == 0:
                fin[at, c, rows_of, :] = value
            else:
                f2[part, e] = value
                copy_to(
                    f2.at[part, e], fin.at[at, c, rows_of], s_g.at[0], r_g.at[part], {"z": tz, "yl": ty}
                ).start()
    for part in range(PARTS):
        rows_of = slice(part * WIDE, part * WIDE + WIDE)
        arrived(fin.at[pl.ds(0, 7), c, rows_of], r_g.at[part])
        ref = fin.at[:, c, rows_of]
        copy_to(ref, ref, s_c.at[0], r_c.at[0], core).start()
    arrived(fin.at[:, c], r_c.at[0])
    first.sent()
    second.sent()
    gone(y_send, s_y.at[0])
    gone(y_relay, s_y.at[1])
    gone(h_send, s_h.at[0])
    gone(h_relay, s_h.at[1])
    gone(squares.at[pl.ds(0, 15)], s_q.at[0])
    gone(f1.at[:, pl.ds(0, 6)], s_f.at[0])
    gone(f2.at[:, pl.ds(0, 7)], s_g.at[0])
    gone(fin.at[:, c], s_c.at[0])


STAGE_IN = [
    VM((1152, 512), BF), VM((1152, 256), BF), VM((1152, 256), BF),
    VM((1152, 128), F32), VM((128, 128), F32), VM((64, 512), F32), VM((64, 512), F32),
    VM((576, 512), BF), VM((PARTS, 8, WIDE, 128), BF), VM((24, WIDE, 128), BF), VM((24, WIDE, 128), BF), VM((24, WIDE, 128), BF), VM((1152, 1024), BF), VM((16, 8, 128), F32),
    VM((2, 512, 512), F32), VM((2, 512, 512), F32), VM((512, 512), BF), VM((512, 512), BF), VM((2, 512, 512), F32),
    DMA((2,)), DMA((PARTS,)), DMA((4 * PARTS,)), DMA((PARTS,)), DMA((4 * PARTS,)), DMA((PARTS,)), DMA((PARTS,)),
    DMA((2,)), DMA((3,)), DMA((2,)), DMA((3,)), DMA((2 * PARTS,)), DMA((3 * PARTS,)), DMA((1,)), DMA((1,)),
    DMA((1,)), DMA((4,)), DMA((1,)), DMA((4,)),
]
STAGE_ATTEND = [
    VM((4, 256, 128), BF), VM((4, 256, 128), F32), VM((4, 256, 128), F32),
    DMA((1,)), DMA((2,)), DMA((1,)), DMA((1,)),
]
STAGE_OUT = (
    [VM((2, 2, OUT[0], 512), BF), VM((2, 2, OUT[0], 512), BF), VM((2, OUT[0], 512), BF), VM((2, OUT[0], 512), BF)]
    + [VM((2, 2, OUT[1], 256), BF), VM((2, 2, OUT[1], 256), BF), VM((2, OUT[1], 256), BF), VM((2, OUT[1], 256), BF)]
    + [VM((4, OUT[1], 512), BF)] * 3
    + [VM((OUT[0], 512), BF)] * 3
    + [VM((2, 4, OUT[0], 512), F32), VM((4, OUT[1], 512), F32), VM((288, 512), F32)]
    + [VM((16, 4, 128), F32), VM((PARTS, 4, WIDE, 128), F32)]
    + [VM((PARTS, 8, WIDE, 128), BF)] * 2
    + [VM((8, WIDE, 128), BF)] * PARTS
    + [DMA((2,)), DMA((3,)), DMA((2,)), DMA((3,))]
    + [DMA((2,)), DMA((3,)), DMA((2,)), DMA((2,)), DMA((1,)), DMA((1,)), DMA((1,)), DMA((PARTS,))]
    + [DMA((1,)), DMA((PARTS,)), DMA((1,)), DMA((1,))]
)
SHARED = [
    VM((256, 512), BF), VM((4, 256, 128), BF), VM((1152, 1024), BF), VM((1152, 512), BF), VM((16, 64, 512), BF),
    VM((288, 128), F32), VM((8, 256, 512), BF), DMA((4,)), DMA((6,)), DMA((1,)), DMA((2,)),
]


def kernel(old_ref, new_ref, order_ref, xt_in, pre_ref, post_ref, wq_in, wk_in, wv_in, wo_in, fin, *scratch):
    q, kv, xs, wo, ctx, gain_out, kvs, s_x, r_x, s_c, r_c = scratch[:11]
    scratch = scratch[11:]
    keys_values = KeysValues(kv, kvs, s_x, r_x, s_c, r_c)
    own_in, scratch = scratch[:len(STAGE_IN)], scratch[len(STAGE_IN):]
    own_attend, own_out = scratch[:len(STAGE_ATTEND)], scratch[len(STAGE_ATTEND):]
    end_in = stage_in(
        old_ref, order_ref, xt_in, pre_ref, post_ref, wq_in, wk_in, wv_in, wo_in, q, kv, xs, wo, gain_out, *own_in,
        keys_values,
    )
    end_attend = stage_attend(q, ctx, keys_values, kvs, *own_attend)
    end_in()
    stage_out(new_ref, ctx, xs, wo, gain_out, fin, *own_out)
    end_attend()


def run(old_blocks, new_blocks, order, xt, pre_gain, post_gain, w_query, w_key, w_value, w_out_t):
    smem = pl.BlockSpec(memory_space=pltpu.SMEM)
    vmem = pl.BlockSpec(memory_space=pltpu.VMEM)
    hbm = pl.BlockSpec(memory_space=pltpu.HBM)
    return pl.pallas_call(
        kernel,
        name="sublayer",
        out_shape=jax.ShapeDtypeStruct((8, 2, 288, 128), BF),
        in_specs=[smem, smem, smem, hbm, vmem, vmem, hbm, hbm, hbm, hbm],
        out_specs=vmem,
        scratch_shapes=SHARED + STAGE_IN + STAGE_ATTEND + STAGE_OUT,
        compiler_params=pltpu.CompilerParams(collective_id=0, has_side_effects=True, vmem_limit_bytes=62 * 2**20),
    )(old_blocks, new_blocks, order, xt, pre_gain, post_gain, w_query, w_key, w_value, w_out_t)


def per_device(
    x_old, old_blocks, new_blocks, order, pre_gain, post_gain, w_query, w_key, w_value, w_out_t
):
    c = lax.axis_index("c")
    fin = run(
        old_blocks, new_blocks, order, x_old.T, pre_gain.reshape(36, 128), post_gain.reshape(36, 128),
        w_query, w_key, w_value, w_out_t,
    )
    return lax.dynamic_slice(fin.reshape(16, 288, 128), (0, 0, c * 64), (16, 288, 64)).reshape(4608, 64).T


def solution(mesh):
    torus = Mesh(mesh.devices.reshape(4, 2, 2, 4, 2), ("x", "yl", "c", "z", "yh"))
    seq, tp = ("x", "yl", "c"), ("z", "yh")
    both = P(seq, tp)
    in_specs = (both, P(), P(), P(), P(), P(), both, both, both, both)
    return jax.shard_map(
        per_device, mesh=torus, in_specs=in_specs, out_specs=P(seq + tp, None), check_vma=False
    )
```

```python
import functools
import math

import jax
import jax.numpy as jnp
from jax import lax
from jax.experimental import pallas as pl
from jax.experimental.pallas import tpu as pltpu
from jax.sharding import Mesh
from jax.sharding import PartitionSpec as P

D = 4608
HEADS = 32
HEAD = 128
BLOCK = 128
EPS = 1e-06
BF = jnp.bfloat16
F32 = jnp.float32
VM = pltpu.VMEM
OUT = (160, 128)
IN = ((0, 32), (32, 64), (96, 96), (192, 96))
BACK = ((0, 96), (96, 96), (192, 64), (256, 32))
PARTS = 4
DMA = pltpu.SemaphoreType.DMA


def kept(at, c):
    return 2 * at + lax.rem(at + c, 2)


def coords():
    return tuple(lax.axis_index(name) for name in ("x", "yl", "c", "z", "yh"))


def copy_to(src, dst, send_sem, recv_sem, device):
    return pltpu.make_async_remote_copy(
        src_ref=src,
        dst_ref=dst,
        send_sem=send_sem,
        recv_sem=recv_sem,
        device_id=device,
        device_id_type=pl.DeviceIdType.MESH,
    )


def greet(devices):
    sem = pltpu.get_barrier_semaphore()
    for device in devices:
        pl.semaphore_signal(sem, inc=1, device_id=device, device_id_type=pl.DeviceIdType.MESH)


def greeted(devices):
    pl.semaphore_wait(pltpu.get_barrier_semaphore(), len(devices))


def mod4(v):
    return lax.rem(v + 4, 4)


def arrived(ref, sem):
    copy_to(ref, ref, sem, sem, {"c": 1 - lax.axis_index("c")}).wait_recv()


def gone(ref, sem):
    copy_to(ref, ref, sem, sem, {"c": 1 - lax.axis_index("c")}).wait_send()


class Gather4:
    def __init__(self, views, axis, me, send, recv, size):
        one, two = me + 1 - 2 * lax.rem(me, 2), 3 - me
        far = two + 1 - 2 * lax.rem(two, 2)
        self.moves = [
            (me, one, 0, one),
            (me, two, 1, two),
            (me, two, 0, two),
            (me, one, 1, one),
            (one, far, 0, two),
            (two, far, 1, one),
        ]
        self.views, self.axis, self.send, self.recv, self.size = views, axis, send, recv, size

    def go(self, *moves):
        for move in moves:
            sent, _, half, partner = self.moves[move]
            for view in self.views:
                ref = view(sent, half)
                copy_to(ref, ref, self.send(move // 4), self.recv(move // 2), {self.axis: partner}).start()

    def start(self):
        self.go(0, 1, 2, 3)

    def relay(self):
        arrived(self.size(2), self.recv(0))
        self.go(4, 5)

    def near(self):
        arrived(self.size(2), self.recv(1))

    def far(self):
        arrived(self.size(2), self.recv(2))

    def sent(self):
        gone(self.size(4), self.send(0))
        gone(self.size(2), self.send(1))


def some(sems, start):
    return lambda n: sems.at[start + n]


def rows(ref, start, size, unit=16):
    return ref.at[pl.ds(pl.multiple_of(start, unit), size)]


def lanes(start, size):
    return pl.ds(pl.multiple_of(start, 128), size)


def columns(dst, table, chunk_of, count):
    lane = lax.broadcasted_iota(jnp.int32, (32, 128), 1)

    def body(n, _):
        feature = chunk_of(lax.div(n, 9)) * 288 + lax.rem(n, 9) * 32
        part = table[pl.ds(pl.multiple_of(lax.rem(feature, 128), 32), 32), :]
        value = jnp.sum(jnp.where(lane == lax.div(feature, 128), part, 0.0), axis=1, keepdims=True)
        dst[pl.ds(pl.multiple_of(n * 32, 32), 32), :] = jnp.broadcast_to(value, (32, 128))
        return 0

    lax.fori_loop(0, count * 9, body, 0)


def stage_in(
    old_ref, order_ref, xt_in, pre_ref, post_ref, wq_in, wk_in, wv_in, wo_in,
    q_out, kv_out, xs, wo, gain_out,
    wq, wk, wv, gain, table, cos, sin, xt, slots, landed, normed, squares, near, other, to_y, from_y, mine,
    s_w, s_one, r_one, s_two, r_two, s_three, r_three, s_wg, r_wg, s_og, r_og, s_z, r_z, s_q, r_q, s_c, r_c, s_y, r_y,
    keys_values,
):
    x, yl, c, z, yh = coords()
    ring_peers = [
        {"x": lax.rem(x + dx, 4), "c": c + dc - 2 * c * dc} for dx in range(4) for dc in range(2)
    ][1:]
    y_one = {"yl": 1 - yl}
    y_two = {"yl": 1 - yl, "yh": 1 - yh}
    group = [
        {"z": lax.rem(z + dz, 4), "yl": yl + dy - 2 * yl * dy, "c": c + dc - 2 * c * dc}
        for dz in (0, 2, 1, 3) for dy in range(2) for dc in range(2)
    ][1:]
    greet(ring_peers + [y_two] + group)
    into = pltpu.make_async_copy(xt_in, xt, s_w.at[1])
    into.start()
    at = pl.ds(pl.multiple_of(x * 288, 16), 288)
    owns = [
        pltpu.make_async_copy(src, dst.at[at], s_w.at[0]) for src, dst in ((wq_in, wq), (wk_in, wk), (wv_in, wv))
    ]

    def out_rows(chunk, half):
        return rows(wo, half * 4 * OUT[0] + chunk * OUT[half], OUT[half])

    for half in range(2):
        part = wo_in.at[pl.ds(half * OUT[0], OUT[half])]
        owns.append(pltpu.make_async_copy(part, out_rows(x, half), s_w.at[0]))
    for copy in owns:
        copy.start()
    starts, total = [], 0
    for m in range(16):
        starts.append(total)
        total = total + old_ref[m]
    k = order_ref[x * 4 + yl * 2 + c]
    first = sum([jnp.where(k > m, old_ref[m], 0) for m in range(15)])
    into.wait()
    for r in range(4):
        b = lax.rem(r - first + 64, 4)
        for h in range(2):
            for half, (begin, count) in enumerate(IN):
                at_rows = slice(h * 288 + begin, h * 288 + begin + count)
                part = [xt[at_rows, n * 128:(n + 1) * 128] for n in range(4)]
                low = jnp.where(b == 0, part[0], part[1])
                slots[half][r * 2 + h] = jnp.where(b < 2, low, jnp.where(b == 2, part[2], part[3]))
    here = x * 2 + c
    for half in range(PARTS):
        landed[half][here] = slots[half][here]
    greeted(ring_peers + [y_two] + group)
    for half in range(PARTS):
        for d, peer in enumerate(ring_peers, 1):
            copy_to(
                slots[half].at[peer["x"] * 2 + peer["c"]], landed[half].at[here],
                s_one.at[half], r_one.at[half * 4 + d // 2], peer,
            ).start()
    everything = wo.at[pl.ds(0, 864)]
    pltpu.make_async_copy(everything, everything, s_w.at[0]).wait()

    def half_rows(ref):
        return lambda chunk, half: rows(ref, chunk * 288 + half * 144, 144)

    weights = Gather4(
        [half_rows(r) for r in (wq, wk, wv)], "x", x, some(s_wg, 0), some(r_wg, 0), lambda n: wq.at[pl.ds(0, 288 * n)]
    )
    weights.start()
    straight = yl == yh

    def slot_pair(half, dx, where):
        return landed[half].at[pl.ds(where * 8 + mod4(x - dx) * 2, 2)]

    def relay_y(n):
        half, dx = n // 4, n % 4
        arrived(slot_pair(half, dx, 1), r_two.at[n])
        copy = copy_to(slot_pair(half, dx, 1), slot_pair(half, dx, 2), s_three.at[half], r_three.at[half], y_one)
        pl.when(straight)(copy.start)

    for half in range(PARTS):
        for dx in range(4):
            n = half * 4 + dx
            from_x = slot_pair(half, dx, 0) if dx > 0 else landed[half].at[x * 2 + 1 - c]
            arrived(from_x, r_one.at[n])
            copy_to(slot_pair(half, dx, 0), slot_pair(half, dx, 1), s_two.at[half], r_two.at[n], y_two).start()
            copy = copy_to(slot_pair(half, dx, 0), slot_pair(half, dx, 2), s_three.at[half], r_three.at[half], y_one)
            pl.when(jnp.logical_not(straight))(copy.start)
            if half >= 2:
                relay_y(half * 4 - 8 + dx)
    me = z * 4 + yl * 2 + c
    first_buffer = jnp.where(straight, 0, 1)

    def part_rows(part):
        begin, count = IN[part]
        return lambda chunk, half: rows(xs, chunk * 288 + begin + half * (count // 2), count // 2)

    def some_rows(part):
        return lambda n: xs.at[pl.ds(0, IN[part][1] // 2 * n)]

    gathers = [
        Gather4(
            [part_rows(part)], "z", z, some(s_z, 2 * part), some(r_z, 3 * part),
            some_rows(part),
        )
        for part in range(PARTS)
    ]
    sources = []
    for place in range(8):
        g = x + 4 * kept(place % 4, place // 4)
        shard = sum([jnp.where(starts[m] <= g, 1, 0) for m in range(16)]) - 1
        holder = sum([jnp.where(order_ref[p] == shard, p, 0) for p in range(16)])
        y_source = lax.rem(lax.div(holder, 2), 2)
        sources.append(jnp.where(y_source == yh, first_buffer, 2) * 8 + lax.div(holder, 4) * 2 + lax.rem(holder, 2))

    def pick(half):
        arrived(landed[half].at[pl.ds(16, 8)], r_three.at[half])
        for place in range(8):
            block = landed[half][sources[place]]
            begin, count = IN[half]
            xs[pl.ds(pl.multiple_of(z * 288 + begin, 32), count), place * 128:(place + 1) * 128] = block
            wide = block.astype(F32)
            square = jnp.sum(wide * wide, axis=0, keepdims=True)
            if half > 0:
                square = square + squares[me, place:place + 1, :]
            squares[me, place:place + 1, :] = square
        if half == PARTS - 1:
            for peer in group:
                copy_to(squares.at[me], squares.at[me], s_q.at[0], r_q.at[0], peer).start()
        gathers[half].start()

    pick(0)
    for n in range(8, 16):
        if n in (10, 14):
            pick(1 + (n - 10) // 4)
            if n == 10:
                gathers[0].relay()
        relay_y(n)
    pick(3)
    gathers[1].relay()
    weights.relay()
    wo_all = Gather4(
        [out_rows], "x", x, some(s_og, 0), some(r_og, 0), lambda n: wo.at[pl.ds(0, 144 * n)]
    )
    wo_all.start()
    table[...] = jnp.zeros_like(table)
    table[0:36, :] = pre_ref[...]
    table[...] = table[...].T
    columns(gain, table, lambda n: n * 4 + yl * 2 + c, 4)
    table[...] = jnp.zeros_like(table)
    table[0:36, :] = post_ref[...]
    table[...] = table[...].T
    columns(gain_out, table, lambda n: z * 4 + yl * 2 + c, 1)
    gathers[2].relay()
    half_head = HEAD // 2
    inverse = jnp.exp(
        lax.broadcasted_iota(jnp.int32, (half_head, 128), 0).astype(F32) * (-2.0 * math.log(10000.0) / HEAD)
    )
    for p in range(4):
        place_of = (x + 4 * kept(p, c)) * BLOCK + lax.broadcasted_iota(jnp.int32, (half_head, 128), 1)
        angle = inverse * place_of.astype(F32)
        cos[:, p * 128:(p + 1) * 128] = jnp.cos(angle)
        sin[:, p * 128:(p + 1) * 128] = jnp.sin(angle)
    gathers[3].relay()
    arrived(squares.at[pl.ds(0, 15)], r_q.at[0])
    factor = lax.rsqrt(jnp.sum(squares[...], axis=0) * (1.0 / D) + EPS)

    def norm(chunk):
        for place in range(8):
            scale = factor[place:place + 1, :]

            def norm_rows(n, _, place=place, scale=scale):
                part = pl.ds(pl.multiple_of(chunk * 288 + n * 144, 16), 144)
                at = (part, slice(place * 128, (place + 1) * 128))
                normed[at] = (xs[at].astype(F32) * scale * gain[part, :]).astype(BF)
                return 0

            lax.fori_loop(0, 2, norm_rows, 0)

    pieces = {"q": (slice(0, 256), wq, 256), "k": (slice(256, 384), wk, 128), "v": (slice(384, 512), wv, 128)}

    def corner(dst, y, core, late, names="qkv", part=None):
        if not late:
            part = pl.ds(pl.multiple_of(lax.div(z, 2) * 576, 16), 576)
        elif part is None:
            part = pl.ds(pl.multiple_of(far * 288, 16), 288)
        right = normed[part, lanes(core * 512, 512)]
        for name in names:
            to, table_of, width = pieces[name]
            left = table_of[part, lanes(y * width, width)]
            value = lax.dot_general(left, right, (((0,), (0,)), ((), ())), preferred_element_type=F32)
            if late:
                dst[to, :] += value
            else:
                dst[to, :] = value

    norm(z)
    for one_part in gathers:
        one_part.near()
    norm(z + 1 - 2 * lax.rem(z, 2))
    weights.near()
    weights.far()
    corners = [
        (near.at[0], 1 - yl, 1 - c), (mine.at[0], 1 - yl, c), (near.at[1], yl, 1 - c), (mine.at[1], yl, c),
    ]
    for dst, y, core in corners:
        corner(dst, y, core, False)
    far = (3 - z) + 1 - 2 * lax.rem(3 - z, 2)
    norm(3 - z)
    for dst, y, core in corners:
        corner(dst, y, core, True, part=pl.ds(pl.multiple_of((3 - z) * 288, 16), 288))
    wo_all.relay()
    for one_part in gathers:
        one_part.far()
    norm(far)
    core = {"c": 1 - c}

    def over_core(n, name):
        to = pieces[name][0]
        recv = r_c.at["kvq".index(name) if n == 0 else 3]
        copy_to(near.at[n, to], other.at[n, to], s_c.at[0], recv, core).start()

    first_rows, last_rows = slice(0, 256), slice(256, 512)
    k_part, v_part = slice(256, 384), slice(384, 512)
    spans = (
        (0, k_part, first_rows), (1, v_part, first_rows), (2, k_part, last_rows), (3, v_part, last_rows),
        (4, slice(0, 256), first_rows), (5, slice(0, 256), last_rows),
    )

    def over_y(name):
        to = pieces[name][0]
        arrived(other.at[0, to], r_c.at["kvq".index(name)])
        to_y[to, :] = (mine[0, to, :] + other[0, to, :]).astype(BF)
        for at, part, cols in {"k": spans[:1], "v": spans[1:4], "q": spans[4:]}[name]:
            copy_to(to_y.at[part, cols], from_y.at[part, cols], s_y.at[0], r_y.at[at // 2 if at < 4 else at - 2], y_one).start()

    for name in "kv":
        corner(*corners[0], True, name)
        over_core(0, name)
    corner(*corners[1], True, "kv")
    over_y("k")
    corner(*corners[0], True, "q")
    over_core(0, "q")
    over_y("v")
    corner(*corners[1], True, "q")
    over_y("q")
    corner(*corners[2], True)
    for name in "kvq":
        over_core(1, name)
    corner(*corners[3], True)
    arrived(other.at[1], r_c.at[3])
    scale_q = (D // HEADS) ** (-0.5)

    def summed(part, cols):
        return mine[1, part, cols] + other[1, part, cols] + from_y[part, cols].astype(F32)

    def turned(value, cols):
        a, b = value[:64], value[64:]
        return jnp.concatenate(
            [a * cos[:, cols] - b * sin[:, cols], b * cos[:, cols] + a * sin[:, cols]], axis=0
        ).astype(BF)

    for late, cols in enumerate((first_rows, last_rows)):
        arrived(from_y.at[pl.ds(256, 256), cols], r_y.at[late])
        key = turned(summed(k_part, cols), cols)
        value = summed(v_part, cols).astype(BF)
        for p in range(2):
            kv_out[2 * late + p, :128, :] = key[:, p * 128:(p + 1) * 128]
            kv_out[2 * late + p, 128:, :] = value[:, p * 128:(p + 1) * 128]
        keys_values.send(late)
    for late in range(2):
        keys_values.gathers[late].relay()
    for late, cols in enumerate((first_rows, last_rows)):
        arrived(from_y.at[pl.ds(0, 256), cols], r_y.at[2 + late])
        for h in range(2):
            part = slice(h * 128, (h + 1) * 128)
            a, b = summed(slice(h * 128, h * 128 + 64), cols), summed(slice(h * 128 + 64, h * 128 + 128), cols)
            turn_a = a * cos[:, cols] - b * sin[:, cols]
            turn_b = b * cos[:, cols] + a * sin[:, cols]
            q_out[part, cols] = (jnp.concatenate([turn_a, turn_b], axis=0) * scale_q).astype(BF)

    def out_weights():
        wo_all.near()
        wo_all.far()

    def finish():
        for half in range(PARTS):
            gone(slots[half].at[pl.ds(0, 7)], s_one.at[half])
            gone(landed[half].at[pl.ds(0, 8)], s_two.at[half])
            gone(landed[half].at[pl.ds(0, 8)], s_three.at[half])
        gone(squares.at[pl.ds(0, 15)], s_q.at[0])
        gone(near, s_c.at[0])
        gone(to_y, s_y.at[0])
        weights.sent()
        wo_all.sent()
        for one_part in gathers:
            one_part.sent()

    return out_weights, finish


class KeysValues:
    def __init__(self, kv_ref, kvs, s_x, r_x, s_c, r_c):
        x, _, c, _, _ = coords()

        def block(late):
            return lambda chunk, half: kvs.at[kept(2 * late + half, c), :, lanes(chunk * 128, 128)]

        self.gathers = [
            Gather4(
                [block(late)], "x", x, some(s_x, 2 * late), some(r_x, 3 * late),
                lambda n: kvs.at[0, :, pl.ds(0, 128 * n)],
            )
            for late in range(2)
        ]
        self.kv_ref, self.kvs, self.s_c, self.r_c = kv_ref, kvs, s_c, r_c

    def send(self, late):
        x, _, c, _, _ = coords()
        for p in (2 * late, 2 * late + 1):
            self.kvs[kept(p, c), :, lanes(x * 128, 128)] = self.kv_ref[p]
        self.gathers[late].start()

    def to_core(self, late):
        _, _, c, _, _ = coords()
        self.gathers[late].near()
        self.gathers[late].far()
        for p in (2 * late, 2 * late + 1):
            ref = self.kvs.at[kept(p, c)]
            copy_to(ref, ref, self.s_c.at[0], self.r_c.at[late], {"c": 1 - c}).start()

    def from_core(self, late):
        arrived(self.kvs.at[pl.ds(0, 2)], self.r_c.at[late])

    def sent(self):
        gone(self.kvs.at[pl.ds(0, 4)], self.s_c.at[0])
        for gather in self.gathers:
            gather.sent()


def stage_attend(q_ref, ctx, keys_values, kvs, early_sums, qs, acc, den, s_y, r_y, s_o, r_o):
    x, yl, c, z, yh = coords()
    core, y_one = {"c": 1 - c}, {"yl": 1 - yl}
    for p in range(4):
        for h in range(2):
            part = q_ref[h * 128:(h + 1) * 128, p * 128:(p + 1) * 128].astype(F32)
            qs[p, h * 128:(h + 1) * 128, :] = part.T.astype(BF)
    acc[...] = jnp.zeros_like(acc)
    den[...] = jnp.zeros_like(den)
    keys_values.to_core(0)

    def tiles(pairs, core_at, diagonal=()):
        pairs = [(p, kept(e, core_at), n in diagonal) for n, (p, e) in enumerate(pairs)]
        scores = [jnp.dot(qs[p], kvs[group, :128, :], preferred_element_type=F32) for p, group, _ in pairs]
        for (p, group, masked), score in zip(pairs, scores):
            weight = jnp.exp2((50.0 * math.log2(math.e)) * jnp.tanh(score * (1.0 / 50.0)))
            if masked:
                row = lax.rem(lax.broadcasted_iota(jnp.int32, (256, 512), 0), 128)
                col = lax.broadcasted_iota(jnp.int32, (256, 512), 1)
                weight = jnp.where(col - row <= x * 128, weight, 0.0)
            den[p] += sum([weight[:, n:n + 128] for n in range(0, 512, 128)])
            acc[p] += lax.dot_general(
                weight.astype(BF), kvs[group, 128:, :], (((1,), (1,)), ((), ())), preferred_element_type=F32
            )

    def region(core_at, y_at, at, size):
        return ctx.at[pl.ds(at + core_at * 4, size), :, lanes(y_at * 256, 256)]

    def put(step):
        for p in (2 * step, 2 * step + 1):
            for h in range(2):
                part = slice(h * 128, (h + 1) * 128)
                total = jnp.sum(den[p, part, :], axis=1, keepdims=True)
                value = (acc[p, part, :] / total).astype(BF)
                cols = lanes(yl * 256 + h * 128, 128)
                ctx[c * 4 + p, :, cols] = value[:64]
                ctx[8 + c * 4 + p, :, cols] = value[64:]
        for half in range(2):
            ref = region(c, yl, half * 8 + 2 * step, 2)
            copy_to(ref, ref, s_y.at[0], r_y.at[step], y_one).start()
            copy_to(ref, ref, s_o.at[0], r_o.at[0], core).start()

    def pass_on(step):
        arrived(ctx.at[pl.ds(0, 4), :, pl.ds(0, 256)], r_y.at[step])
        for half in range(2):
            ref = region(c, 1 - yl, half * 8 + 2 * step, 2)
            copy_to(ref, ref, s_o.at[0], r_o.at[1], core).start()

    tiles([(0, 0), (1, 0), (1, 1)], c, (0, 2))
    keys_values.from_core(0)
    tiles([(1 - c, 0), (1, 1 - c)], 1 - c)
    put(0)
    tiles([(2, 0), (2, 1), (3, 0), (3, 1)], c)
    keys_values.to_core(1)
    tiles([(2, 0), (2, 1), (3, 0), (3, 1)], 1 - c)
    tiles([(2, 2), (3, 2), (3, 3)], c, (0, 2))
    keys_values.from_core(1)
    tiles([(3 - c, 2), (3, 3 - c)], 1 - c)
    put(1)
    pass_on(0)
    arrived(ctx.at[pl.ds(0, 8), :, pl.ds(0, 256)], r_o.at[0])
    early_sums()
    pass_on(1)
    arrived(ctx.at[pl.ds(0, 8), :, pl.ds(0, 256)], r_o.at[1])

    def finish():
        gone(ctx.at[pl.ds(0, 8), :, pl.ds(0, 256)], s_y.at[0])
        gone(ctx.at[:, :, pl.ds(0, 256)], s_o.at[0])
        keys_values.sent()

    return finish


class Reduce4:
    def __init__(self, z, send, got, more, more_got, s, r):
        self.one, self.two = z + 1 - 2 * lax.rem(z, 2), 3 - z
        self.far = self.two + 1 - 2 * lax.rem(self.two, 2)
        self.send, self.got, self.more, self.more_got, self.s, self.r = send, got, more, more_got, s, r

    def partner(self, part, step):
        return {"z": self.one if part == step else self.two}

    def chunk(self, part, slot):
        return self.far if slot == 1 else (self.two if part else self.one)

    def give(self, part, slot, value):
        self.send[part, slot] = value
        copy_to(
            self.send.at[part, slot], self.got.at[part, slot], self.s.at[0], self.r.at[slot], self.partner(part, 0)
        ).start()

    def pass_on(self, values):
        arrived(self.got.at[0], self.r.at[1])
        for part, value in enumerate(values):
            self.more[part] = (value + self.got[part, 1].astype(F32)).astype(BF)
            copy_to(
                self.more.at[part], self.more_got.at[part], self.s.at[1], self.r.at[2], self.partner(part, 1)
            ).start()

    def own(self, values):
        arrived(self.got.at[0], self.r.at[0])
        arrived(self.more_got, self.r.at[2])
        return [
            value + self.got[part, 0].astype(F32) + self.more_got[part].astype(F32) for part, value in enumerate(values)
        ]

    def sent(self):
        gone(self.send, self.s.at[0])
        gone(self.more, self.s.at[1])


class OutSums:
    def __init__(self, ctx, wo, own_y, own_a, own_b):
        _, yl, _, _, yh = coords()
        self.ctx, self.wo, self.yl = ctx, wo, yl
        self.all = [(own_y, 1 - yh, 1), (own_a.at[0], 0, 0), (own_a.at[1], 1, 0), (own_b, yh, 1)]

    def product(self, n, y):
        _, half, part = self.all[n]
        left = self.wo[part * 4 * OUT[0]:part * 4 * OUT[0] + 4 * OUT[part], lanes(y * 256, 256)]
        right = self.ctx[pl.ds(half * 8, 8), :, lanes(y * 256, 256)].reshape(512, 256)
        value = lax.dot_general(left, right, (((1,), (1,)), ((), ())), preferred_element_type=F32)
        return value.reshape(4, OUT[part], 512)

    def early(self):
        for n, (dst, _, _) in enumerate(self.all):
            dst[...] = self.product(n, self.yl)

    def late(self, n):
        dst = self.all[n][0]
        dst[...] = dst[...] + self.product(n, 1 - self.yl)


def stage_out(
    new_ref, ctx, xs, wo, gain, out_ref, out_sums, own_y, own_a, own_b,
    a_send, a_got, a_more, a_more_got, b_send, b_got, b_more, b_more_got,
    y_send, y_relay, y_got, h_send, h_relay, h_got, total,
    squares, fresh, f1, f2, f1_got, fin,
    a_s, a_r, b_s, b_r, s_y, r_y, s_h, r_h, s_q, r_q, s_f, r_f, s_g, r_g, s_c, r_c,
):
    x, yl, c, z, yh = coords()
    core = {"c": 1 - c}
    y_one, y_two = {"yl": 1 - yl}, {"yl": 1 - yl, "yh": 1 - yh}
    group = [
        {"z": lax.rem(z + dz, 4), "yl": yl + dy - 2 * yl * dy, "c": c + dc - 2 * c * dc}
        for dz in (0, 2, 1, 3) for dy in (0, 1) for dc in (0, 1)
    ]
    group = group[4:] + group[1:4]
    others = [{"x": lax.rem(x + dx, 4)} for dx in (2, 1, 3)]

    out_sums.late(0)
    y_send[...] = own_y[...].astype(BF)
    for n in range(4):
        copy_to(y_send.at[n], y_relay.at[n], s_y.at[0], r_y.at[n // 2], y_two if n % 2 else y_one).start()
    first = Reduce4(z, a_send, a_got, a_more, a_more_got, a_s, a_r)
    for part in range(2):
        out_sums.late(1 + part)
        first.give(part, 1, own_a[part, first.chunk(part, 1)].astype(BF))
    for part in range(2):
        first.give(part, 0, own_a[part, first.chunk(part, 0)].astype(BF))
    out_sums.late(3)

    def forward(step):
        arrived(y_relay.at[pl.ds(0, 2)], r_y.at[step])
        for n in (2 * step, 2 * step + 1):
            copy_to(y_relay.at[n], y_got.at[n], s_y.at[1], r_y.at[2], y_one if n % 2 else y_two).start()

    forward(0)
    first.pass_on([own_a[0, first.two], own_a[1, first.one]])
    forward(1)
    for part, value in enumerate(first.own([own_a[0, z], own_a[1, z]])):
        own_a[part, z] = value
    h_send[...] = own_a[1 - yh, z].astype(BF)
    spans = (slice(0, 80), slice(80, OUT[0]))
    for n, peer in enumerate((y_one, y_two)):
        copy_to(h_send.at[spans[n]], h_relay.at[spans[n]], s_h.at[0], r_h.at[0], peer).start()
    second = Reduce4(z, b_send, b_got, b_more, b_more_got, b_s, b_r)
    arrived(y_got, r_y.at[2])
    own_b[...] = own_b[...] + y_got[...].astype(F32)
    cols = (slice(0, 256), slice(256, 512))
    for slot in (1, 0):
        for part in range(2):
            second.give(part, slot, own_b[second.chunk(part, slot), :, cols[part]].astype(BF))
    arrived(h_relay, r_h.at[0])
    for n, peer in enumerate((y_two, y_one)):
        copy_to(h_relay.at[spans[n]], h_got.at[spans[n]], s_h.at[1], r_h.at[1], peer).start()
    second.pass_on([own_b[second.two, :, cols[0]], own_b[second.one, :, cols[1]]])
    for part, value in enumerate(second.own([own_b[z, :, cols[0]], own_b[z, :, cols[1]]])):
        total[OUT[0]:, cols[part]] = value
    arrived(h_got, r_h.at[1])
    total[:OUT[0], :] = own_a[yh, z] + h_got[...].astype(F32)
    me = z * 4 + yl * 2 + c
    for m in range(4):
        value = total[:, m * 128:(m + 1) * 128]
        squares[me, m:m + 1, :] = jnp.sum(value * value, axis=0, keepdims=True)
    for peer in group:
        copy_to(squares.at[me], squares.at[me], s_q.at[0], r_q.at[0], peer).start()
    lane = lax.broadcasted_iota(jnp.int32, (96, 128), 1)

    def pair(m, part):
        begin, count = BACK[part]
        low = lane[:count] < 64
        at = pl.ds(pl.multiple_of(z * 288 + begin, 32), count)
        a = xs[at, m * 256:m * 256 + 128].astype(F32)
        b = xs[at, m * 256 + 128:m * 256 + 256].astype(F32)
        upper, lower = pltpu.roll(a, 64, 1), pltpu.roll(b, 64, 1)
        return jnp.where(low, jnp.where(yh == 0, a, upper), jnp.where(yh == 0, lower, b))

    for part in range(PARTS):
        for m in range(4):
            fresh[part][m] = pair(m, part)
    arrived(squares.at[pl.ds(0, 15)], r_q.at[0])
    factor = lax.rsqrt(jnp.sum(squares[...], axis=0) * (1.0 / D) + EPS)
    starts, so_far = [], 0
    for j in range(16):
        starts.append(so_far)
        so_far = so_far + new_ref[j]
    here = pl.ds(x * 2, 2)
    for part, (begin, count) in enumerate(BACK):
        rows_of = slice(begin, begin + count)
        low = lane[:count] < 64
        for m in range(4):
            value = total[rows_of, m * 128:(m + 1) * 128] * factor[m:m + 1, :] * gain[rows_of, :]
            fresh[part][m] = fresh[part][m] + value
        for n in range(8):
            sides = []
            for side in range(2):
                j = 2 * n + side
                within = lax.rem(x - starts[j] + 64, 4)
                i = jnp.minimum(lax.div(starts[j] + within - x, 4), 7)
                at = lax.div(i, 2)
                place = lax.rem(i + at, 2) * 4 + at
                value = fresh[part][lax.div(place, 2)]
                value = jnp.where(lax.rem(place, 2) == side, value, pltpu.roll(value, 64, 1))
                sides.append(jnp.where(within < new_ref[j], value, 0.0))
            f1[part][n] = jnp.where(low, sides[0], sides[1]).astype(BF)
        f1_got[part][here] = f1[part][here]
        for peer in others:
            copy_to(
                f1[part].at[pl.ds(peer["x"] * 2, 2)], f1_got[part].at[here], s_f.at[part], r_f.at[part], peer
            ).start()
    mine = [sum([jnp.where(x * 4 + n > m, new_ref[m], 0) for m in range(15)]) for n in range(4)]
    for part, (begin, count) in enumerate(BACK):
        rows_of = slice(begin, begin + count)
        low = lane[:count] < 64
        arrived(f1_got[part].at[pl.ds(0, 6)], r_f.at[part])
        for e in (5, 4, 3, 7, 2, 6, 1, 0):
            dz, dy = e // 2, e % 2
            tz, ty = lax.rem(z + dz, 4), yl + dy - 2 * yl * dy
            sides = []
            for side in range(2):
                start = jnp.where(ty == 0, mine[side], mine[2 + side])
                sides.append(f1_got[part][lax.rem(start + tz, 4) * 2 + ty].astype(F32))
            value = jnp.where(low, sides[0], sides[1]).astype(BF)
            at = z * 2 + yl
            if e == 0:
                fin[at, c, rows_of, :] = value
            else:
                f2[part][e] = value
                copy_to(
                    f2[part].at[e], fin.at[at, c, rows_of], s_g.at[part], r_g.at[part], {"z": tz, "yl": ty}
                ).start()
    for part, (begin, count) in enumerate(BACK):
        rows_of = slice(begin, begin + count)
        arrived(fin.at[pl.ds(0, 7), c, rows_of], r_g.at[part])
        ref = fin.at[:, c, rows_of]
        copy_to(ref, ref, s_c.at[0], r_c.at[0], core).start()
    arrived(fin.at[:, c], r_c.at[0])
    mine_of = lax.broadcasted_iota(jnp.int32, (64, 128), 0) + c * 64
    pick = jnp.where(lane[:64] == mine_of, 1.0, 0.0).astype(BF)
    for n in range(4):
        block = fin[2 * n:2 * n + 2].reshape(1152, 128)
        value = lax.dot_general(pick, block, (((1,), (1,)), ((), ())), preferred_element_type=F32)
        out_ref[:, n * 1152:(n + 1) * 1152] = value.astype(BF)
    first.sent()
    second.sent()
    gone(y_send, s_y.at[0])
    gone(y_relay, s_y.at[1])
    gone(h_send, s_h.at[0])
    gone(h_relay, s_h.at[1])
    gone(squares.at[pl.ds(0, 15)], s_q.at[0])
    for part in range(PARTS):
        gone(f1[part].at[pl.ds(0, 6)], s_f.at[part])
        gone(f2[part].at[pl.ds(0, 7)], s_g.at[part])
    gone(fin.at[:, c], s_c.at[0])


STAGE_IN = [
    VM((1152, 512), BF), VM((1152, 256), BF), VM((1152, 256), BF),
    VM((1152, 128), F32), VM((128, 128), F32), VM((64, 512), F32), VM((64, 512), F32),
    VM((576, 512), BF), [VM((8, count, 128), BF) for _, count in IN], [VM((24, count, 128), BF) for _, count in IN], VM((1152, 1024), BF), VM((16, 8, 128), F32),
    VM((2, 512, 512), F32), VM((2, 512, 512), F32), VM((512, 512), BF), VM((512, 512), BF), VM((2, 512, 512), F32),
    DMA((2,)), DMA((PARTS,)), DMA((4 * PARTS,)), DMA((PARTS,)), DMA((4 * PARTS,)), DMA((PARTS,)), DMA((PARTS,)),
    DMA((2,)), DMA((3,)), DMA((2,)), DMA((3,)), DMA((2 * PARTS,)), DMA((3 * PARTS,)), DMA((1,)), DMA((1,)),
    DMA((1,)), DMA((4,)), DMA((1,)), DMA((4,)),
]
STAGE_ATTEND = [
    VM((4, 256, 128), BF), VM((4, 256, 128), F32), VM((4, 256, 128), F32),
    DMA((1,)), DMA((2,)), DMA((1,)), DMA((2,)),
]
STAGE_OUT = (
    [VM((2, 2, OUT[0], 512), BF), VM((2, 2, OUT[0], 512), BF), VM((2, OUT[0], 512), BF), VM((2, OUT[0], 512), BF)]
    + [VM((2, 2, OUT[1], 256), BF), VM((2, 2, OUT[1], 256), BF), VM((2, OUT[1], 256), BF), VM((2, OUT[1], 256), BF)]
    + [VM((4, OUT[1], 512), BF)] * 3
    + [VM((OUT[0], 512), BF)] * 3
    + [VM((288, 512), F32), VM((16, 4, 128), F32), [VM((4, count, 128), F32) for _, count in BACK]]
    + [[VM((8, count, 128), BF) for _, count in BACK]] * 3
    + [VM((8, 2, 288, 128), BF)]
    + [DMA((2,)), DMA((3,)), DMA((2,)), DMA((3,))]
    + [DMA((2,)), DMA((3,)), DMA((2,)), DMA((2,)), DMA((1,)), DMA((1,)), DMA((PARTS,)), DMA((PARTS,))]
    + [DMA((PARTS,)), DMA((PARTS,)), DMA((1,)), DMA((1,))]
)
SHARED = [
    VM((256, 512), BF), VM((4, 256, 128), BF), VM((1152, 1024), BF), VM((1152, 512), BF), VM((16, 64, 512), BF),
    VM((288, 128), F32), VM((8, 256, 512), BF), DMA((4,)), DMA((6,)), DMA((1,)), DMA((2,)),
    VM((4, OUT[1], 512), F32), VM((2, 4, OUT[0], 512), F32), VM((4, OUT[1], 512), F32),
]


def kernel(old_ref, new_ref, order_ref, xt_in, pre_ref, post_ref, wq_in, wk_in, wv_in, wo_in, out_ref, *scratch):
    q, kv, xs, wo, ctx, gain_out, kvs, s_x, r_x, s_c, r_c, own_y, own_a, own_b = scratch[:14]
    scratch = scratch[14:]
    out_sums = OutSums(ctx, wo, own_y, own_a, own_b)
    keys_values = KeysValues(kv, kvs, s_x, r_x, s_c, r_c)
    own_in, scratch = scratch[:len(STAGE_IN)], scratch[len(STAGE_IN):]
    own_attend, own_out = scratch[:len(STAGE_ATTEND)], scratch[len(STAGE_ATTEND):]
    out_weights, end_in = stage_in(
        old_ref, order_ref, xt_in, pre_ref, post_ref, wq_in, wk_in, wv_in, wo_in, q, kv, xs, wo, gain_out, *own_in,
        keys_values,
    )

    def early_sums():
        out_weights()
        out_sums.early()

    end_attend = stage_attend(q, ctx, keys_values, kvs, early_sums, *own_attend)
    end_in()
    stage_out(new_ref, ctx, xs, wo, gain_out, out_ref, out_sums, own_y, own_a, own_b, *own_out)
    end_attend()


def run(old_blocks, new_blocks, order, xt, pre_gain, post_gain, w_query, w_key, w_value, w_out_t):
    smem = pl.BlockSpec(memory_space=pltpu.SMEM)
    vmem = pl.BlockSpec(memory_space=pltpu.VMEM)
    hbm = pl.BlockSpec(memory_space=pltpu.HBM)
    return pl.pallas_call(
        kernel,
        name="sublayer",
        out_shape=jax.ShapeDtypeStruct((64, D), BF),
        in_specs=[smem, smem, smem, hbm, vmem, vmem, hbm, hbm, hbm, hbm],
        out_specs=vmem,
        scratch_shapes=SHARED + STAGE_IN + STAGE_ATTEND + STAGE_OUT,
        compiler_params=pltpu.CompilerParams(collective_id=0, has_side_effects=True, vmem_limit_bytes=62 * 2**20),
    )(old_blocks, new_blocks, order, xt, pre_gain, post_gain, w_query, w_key, w_value, w_out_t)


def per_device(
    x_old, old_blocks, new_blocks, order, pre_gain, post_gain, w_query, w_key, w_value, w_out_t
):
    return run(
        old_blocks, new_blocks, order, x_old.T, pre_gain.reshape(36, 128), post_gain.reshape(36, 128),
        w_query, w_key, w_value, w_out_t,
    )


def solution(mesh):
    torus = Mesh(mesh.devices.reshape(4, 2, 2, 4, 2), ("x", "yl", "c", "z", "yh"))
    seq, tp = ("x", "yl", "c"), ("z", "yh")
    both = P(seq, tp)
    in_specs = (both, P(), P(), P(), P(), P(), both, both, both, both)
    return jax.shard_map(
        per_device, mesh=torus, in_specs=in_specs, out_specs=P(seq + tp, None), check_vma=False
    )
```

```python
import functools
import math

import jax
import jax.numpy as jnp
from jax import lax
from jax.experimental import pallas as pl
from jax.experimental.pallas import tpu as pltpu
from jax.sharding import Mesh
from jax.sharding import PartitionSpec as P

D = 4608
HEADS = 32
HEAD = 128
BLOCK = 128
EPS = 1e-06
BF = jnp.bfloat16
F32 = jnp.float32
VM = pltpu.VMEM
OUT = (144, 144)
IN = ((0, 32), (32, 64), (96, 96), (192, 96))
BACK = ((0, 96), (96, 96), (192, 64), (256, 32))
PARTS = 4
DMA = pltpu.SemaphoreType.DMA


def kept(at, c):
    return 2 * at + lax.rem(at + c, 2)


def coords():
    return tuple(lax.axis_index(name) for name in ("x", "yl", "c", "z", "yh"))


def copy_to(src, dst, send_sem, recv_sem, device):
    return pltpu.make_async_remote_copy(
        src_ref=src,
        dst_ref=dst,
        send_sem=send_sem,
        recv_sem=recv_sem,
        device_id=device,
        device_id_type=pl.DeviceIdType.MESH,
    )


def greet(devices):
    sem = pltpu.get_barrier_semaphore()
    for device in devices:
        pl.semaphore_signal(sem, inc=1, device_id=device, device_id_type=pl.DeviceIdType.MESH)


def greeted(devices):
    pl.semaphore_wait(pltpu.get_barrier_semaphore(), len(devices))


def mod4(v):
    return lax.rem(v + 4, 4)


def arrived(ref, sem):
    copy_to(ref, ref, sem, sem, {"c": 1 - lax.axis_index("c")}).wait_recv()


def gone(ref, sem):
    copy_to(ref, ref, sem, sem, {"c": 1 - lax.axis_index("c")}).wait_send()


class Gather4:
    def __init__(self, views, axis, me, send, recv, size):
        one, two = me + 1 - 2 * lax.rem(me, 2), 3 - me
        far = two + 1 - 2 * lax.rem(two, 2)
        self.moves = [
            (me, one, 0, one),
            (me, two, 1, two),
            (me, two, 0, two),
            (me, one, 1, one),
            (one, far, 0, two),
            (two, far, 1, one),
        ]
        self.views, self.axis, self.send, self.recv, self.size = views, axis, send, recv, size

    def go(self, *moves):
        for move in moves:
            sent, _, half, partner = self.moves[move]
            for view in self.views:
                ref = view(sent, half)
                copy_to(ref, ref, self.send(move // 4), self.recv(move // 2), {self.axis: partner}).start()

    def start(self):
        self.go(0, 1, 2, 3)

    def relay(self):
        arrived(self.size(2), self.recv(0))
        self.go(4, 5)

    def near(self):
        arrived(self.size(2), self.recv(1))

    def far(self):
        arrived(self.size(2), self.recv(2))

    def sent(self):
        gone(self.size(4), self.send(0))
        gone(self.size(2), self.send(1))


def some(sems, start):
    return lambda n: sems.at[start + n]


def rows(ref, start, size, unit=16):
    return ref.at[pl.ds(pl.multiple_of(start, unit), size)]


def lanes(start, size):
    return pl.ds(pl.multiple_of(start, 128), size)


def columns(dst, table, chunk_of, count):
    lane = lax.broadcasted_iota(jnp.int32, (32, 128), 1)

    def body(n, _):
        feature = chunk_of(lax.div(n, 9)) * 288 + lax.rem(n, 9) * 32
        part = table[pl.ds(pl.multiple_of(lax.rem(feature, 128), 32), 32), :]
        value = jnp.sum(jnp.where(lane == lax.div(feature, 128), part, 0.0), axis=1, keepdims=True)
        dst[pl.ds(pl.multiple_of(n * 32, 32), 32), :] = jnp.broadcast_to(value, (32, 128))
        return 0

    lax.fori_loop(0, count * 9, body, 0)


def stage_in(
    old_ref, order_ref, xt_in, pre_ref, post_ref, wq_in, wk_in, wv_in, wo_in,
    q_out, kv_out, xs, wo, gain_out,
    wq, wk, wv, gain, table, cos, sin, xt, slots, landed, normed, squares, near, other, to_y, from_y, mine,
    s_w, s_one, r_one, s_two, r_two, s_three, r_three, s_wg, r_wg, s_og, r_og, s_z, r_z, s_q, r_q, s_c, r_c, s_y, r_y,
    keys_values,
):
    x, yl, c, z, yh = coords()
    ring_peers = [
        {"x": lax.rem(x + dx, 4), "c": c + dc - 2 * c * dc} for dx in range(4) for dc in range(2)
    ][1:]
    y_one = {"yl": 1 - yl}
    y_two = {"yl": 1 - yl, "yh": 1 - yh}
    group = [
        {"z": lax.rem(z + dz, 4), "yl": yl + dy - 2 * yl * dy, "c": c + dc - 2 * c * dc}
        for dz in (0, 2, 1, 3) for dy in range(2) for dc in range(2)
    ][1:]
    greet(ring_peers + [y_two] + group)
    into = pltpu.make_async_copy(xt_in, xt, s_w.at[1])
    into.start()
    at = pl.ds(pl.multiple_of(x * 288, 16), 288)
    owns = [
        pltpu.make_async_copy(src, dst.at[at], s_w.at[0]) for src, dst in ((wq_in, wq), (wk_in, wk), (wv_in, wv))
    ]

    def out_rows(chunk, half):
        return rows(wo, half * 4 * OUT[0] + chunk * OUT[half], OUT[half])

    for half in range(2):
        part = wo_in.at[pl.ds(half * OUT[0], OUT[half])]
        owns.append(pltpu.make_async_copy(part, out_rows(x, half), s_w.at[0]))
    for copy in owns:
        copy.start()
    starts, total = [], 0
    for m in range(16):
        starts.append(total)
        total = total + old_ref[m]
    k = order_ref[x * 4 + yl * 2 + c]
    first = sum([jnp.where(k > m, old_ref[m], 0) for m in range(15)])
    into.wait()
    for r in range(4):
        b = lax.rem(r - first + 64, 4)
        for h in range(2):
            for half, (begin, count) in enumerate(IN):
                at_rows = slice(h * 288 + begin, h * 288 + begin + count)
                part = [xt[at_rows, n * 128:(n + 1) * 128] for n in range(4)]
                low = jnp.where(b == 0, part[0], part[1])
                slots[half][r * 2 + h] = jnp.where(b < 2, low, jnp.where(b == 2, part[2], part[3]))
    here = x * 2 + c
    for half in range(PARTS):
        landed[half][here] = slots[half][here]
    greeted(ring_peers + [y_two] + group)
    for half in range(PARTS):
        for d, peer in enumerate(ring_peers, 1):
            copy_to(
                slots[half].at[peer["x"] * 2 + peer["c"]], landed[half].at[here],
                s_one.at[half], r_one.at[half * 4 + d // 2], peer,
            ).start()
    everything = wo.at[pl.ds(0, 864)]
    pltpu.make_async_copy(everything, everything, s_w.at[0]).wait()

    def half_rows(ref):
        return lambda chunk, half: rows(ref, chunk * 288 + half * 144, 144)

    weights = Gather4(
        [half_rows(r) for r in (wq, wk, wv)], "x", x, some(s_wg, 0), some(r_wg, 0), lambda n: wq.at[pl.ds(0, 288 * n)]
    )
    weights.start()
    straight = yl == yh

    def slot_pair(half, dx, where):
        return landed[half].at[pl.ds(where * 8 + mod4(x - dx) * 2, 2)]

    def relay_y(n):
        half, dx = n // 4, n % 4
        arrived(slot_pair(half, dx, 1), r_two.at[n])
        copy = copy_to(slot_pair(half, dx, 1), slot_pair(half, dx, 2), s_three.at[half], r_three.at[half], y_one)
        pl.when(straight)(copy.start)

    for half in range(PARTS):
        for dx in range(4):
            n = half * 4 + dx
            from_x = slot_pair(half, dx, 0) if dx > 0 else landed[half].at[x * 2 + 1 - c]
            arrived(from_x, r_one.at[n])
            copy_to(slot_pair(half, dx, 0), slot_pair(half, dx, 1), s_two.at[half], r_two.at[n], y_two).start()
            copy = copy_to(slot_pair(half, dx, 0), slot_pair(half, dx, 2), s_three.at[half], r_three.at[half], y_one)
            pl.when(jnp.logical_not(straight))(copy.start)
            if half >= 2:
                relay_y(half * 4 - 8 + dx)
    me = z * 4 + yl * 2 + c
    first_buffer = jnp.where(straight, 0, 1)

    def part_rows(part):
        begin, count = IN[part]
        return lambda chunk, half: rows(xs, chunk * 288 + begin + half * (count // 2), count // 2)

    def some_rows(part):
        return lambda n: xs.at[pl.ds(0, IN[part][1] // 2 * n)]

    gathers = [
        Gather4(
            [part_rows(part)], "z", z, some(s_z, 2 * part), some(r_z, 3 * part),
            some_rows(part),
        )
        for part in range(PARTS)
    ]
    sources = []
    for place in range(8):
        g = x + 4 * kept(place % 4, place // 4)
        shard = sum([jnp.where(starts[m] <= g, 1, 0) for m in range(16)]) - 1
        holder = sum([jnp.where(order_ref[p] == shard, p, 0) for p in range(16)])
        y_source = lax.rem(lax.div(holder, 2), 2)
        sources.append(jnp.where(y_source == yh, first_buffer, 2) * 8 + lax.div(holder, 4) * 2 + lax.rem(holder, 2))

    def pick(half):
        arrived(landed[half].at[pl.ds(16, 8)], r_three.at[half])
        for place in range(8):
            block = landed[half][sources[place]]
            begin, count = IN[half]
            xs[pl.ds(pl.multiple_of(z * 288 + begin, 32), count), place * 128:(place + 1) * 128] = block
            wide = block.astype(F32)
            square = jnp.sum(wide * wide, axis=0, keepdims=True)
            if half > 0:
                square = square + squares[me, place:place + 1, :]
            squares[me, place:place + 1, :] = square
        if half == PARTS - 1:
            for peer in group:
                copy_to(squares.at[me], squares.at[me], s_q.at[0], r_q.at[0], peer).start()
        gathers[half].start()

    pick(0)
    for n in range(8, 16):
        if n in (10, 14):
            pick(1 + (n - 10) // 4)
            if n == 10:
                gathers[0].relay()
        relay_y(n)
    pick(3)
    gathers[1].relay()
    weights.relay()
    wo_all = Gather4(
        [out_rows], "x", x, some(s_og, 0), some(r_og, 0), lambda n: wo.at[pl.ds(0, 144 * n)]
    )
    wo_all.start()
    table[...] = jnp.zeros_like(table)
    table[0:36, :] = pre_ref[...]
    table[...] = table[...].T
    columns(gain, table, lambda n: n * 4 + yl * 2 + c, 4)
    table[...] = jnp.zeros_like(table)
    table[0:36, :] = post_ref[...]
    table[...] = table[...].T
    columns(gain_out, table, lambda n: z * 4 + yl * 2 + c, 1)
    gathers[2].relay()
    half_head = HEAD // 2
    inverse = jnp.exp(
        lax.broadcasted_iota(jnp.int32, (half_head, 128), 0).astype(F32) * (-2.0 * math.log(10000.0) / HEAD)
    )
    for p in range(4):
        place_of = (x + 4 * kept(p, c)) * BLOCK + lax.broadcasted_iota(jnp.int32, (half_head, 128), 1)
        angle = inverse * place_of.astype(F32)
        cos[:, p * 128:(p + 1) * 128] = jnp.cos(angle)
        sin[:, p * 128:(p + 1) * 128] = jnp.sin(angle)
    gathers[3].relay()
    arrived(squares.at[pl.ds(0, 15)], r_q.at[0])
    factor = lax.rsqrt(jnp.sum(squares[...], axis=0) * (1.0 / D) + EPS)

    def norm(chunk):
        for place in range(8):
            scale = factor[place:place + 1, :]

            def norm_rows(n, _, place=place, scale=scale):
                part = pl.ds(pl.multiple_of(chunk * 288 + n * 144, 16), 144)
                at = (part, slice(place * 128, (place + 1) * 128))
                normed[at] = (xs[at].astype(F32) * scale * gain[part, :]).astype(BF)
                return 0

            lax.fori_loop(0, 2, norm_rows, 0)

    pieces = {"q": (slice(0, 256), wq, 256), "k": (slice(256, 384), wk, 128), "v": (slice(384, 512), wv, 128)}

    def corner(dst, y, core, late, names="qkv", part=None):
        if not late:
            part = pl.ds(pl.multiple_of(lax.div(z, 2) * 576, 16), 576)
        elif part is None:
            part = pl.ds(pl.multiple_of(far * 288, 16), 288)
        right = normed[part, lanes(core * 512, 512)]
        for name in names:
            to, table_of, width = pieces[name]
            left = table_of[part, lanes(y * width, width)]
            value = lax.dot_general(left, right, (((0,), (0,)), ((), ())), preferred_element_type=F32)
            if late:
                dst[to, :] += value
            else:
                dst[to, :] = value

    norm(z)
    for one_part in gathers:
        one_part.near()
    norm(z + 1 - 2 * lax.rem(z, 2))
    weights.near()
    weights.far()
    corners = [
        (near.at[0], 1 - yl, 1 - c), (mine.at[0], 1 - yl, c), (near.at[1], yl, 1 - c), (mine.at[1], yl, c),
    ]
    for dst, y, core in corners:
        corner(dst, y, core, False)
    far = (3 - z) + 1 - 2 * lax.rem(3 - z, 2)
    norm(3 - z)
    for dst, y, core in corners:
        corner(dst, y, core, True, part=pl.ds(pl.multiple_of((3 - z) * 288, 16), 288))
    wo_all.relay()
    for one_part in gathers:
        one_part.far()
    norm(far)
    core = {"c": 1 - c}

    def over_core(n, name):
        to = pieces[name][0]
        recv = r_c.at["kvq".index(name) if n == 0 else 3]
        copy_to(near.at[n, to], other.at[n, to], s_c.at[0], recv, core).start()

    first_rows, last_rows = slice(0, 256), slice(256, 512)
    k_part, v_part = slice(256, 384), slice(384, 512)
    spans = (
        (0, k_part, first_rows), (1, v_part, first_rows), (2, k_part, last_rows), (3, v_part, last_rows),
        (4, slice(0, 256), first_rows), (5, slice(0, 256), last_rows),
    )

    def over_y(name):
        to = pieces[name][0]
        arrived(other.at[0, to], r_c.at["kvq".index(name)])
        to_y[to, :] = (mine[0, to, :] + other[0, to, :]).astype(BF)
        for at, part, cols in {"k": spans[:1], "v": spans[1:4], "q": spans[4:]}[name]:
            copy_to(to_y.at[part, cols], from_y.at[part, cols], s_y.at[0], r_y.at[at // 2 if at < 4 else at - 2], y_one).start()

    for name in "kv":
        corner(*corners[0], True, name)
        over_core(0, name)
    corner(*corners[1], True, "kv")
    over_y("k")
    corner(*corners[0], True, "q")
    over_core(0, "q")
    over_y("v")
    corner(*corners[1], True, "q")
    over_y("q")
    corner(*corners[2], True)
    for name in "kvq":
        over_core(1, name)
    corner(*corners[3], True)
    arrived(other.at[1], r_c.at[3])
    scale_q = (D // HEADS) ** (-0.5)

    def summed(part, cols):
        return mine[1, part, cols] + other[1, part, cols] + from_y[part, cols].astype(F32)

    def turned(value, cols):
        a, b = value[:64], value[64:]
        return jnp.concatenate(
            [a * cos[:, cols] - b * sin[:, cols], b * cos[:, cols] + a * sin[:, cols]], axis=0
        ).astype(BF)

    for late, cols in enumerate((first_rows, last_rows)):
        arrived(from_y.at[pl.ds(256, 256), cols], r_y.at[late])
        key = turned(summed(k_part, cols), cols)
        value = summed(v_part, cols).astype(BF)
        for p in range(2):
            kv_out[2 * late + p, :128, :] = key[:, p * 128:(p + 1) * 128]
            kv_out[2 * late + p, 128:, :] = value[:, p * 128:(p + 1) * 128]
        keys_values.send(late)
    for late in range(2):
        keys_values.gathers[late].relay()
    for late, cols in enumerate((first_rows, last_rows)):
        arrived(from_y.at[pl.ds(0, 256), cols], r_y.at[2 + late])
        for h in range(2):
            part = slice(h * 128, (h + 1) * 128)
            a, b = summed(slice(h * 128, h * 128 + 64), cols), summed(slice(h * 128 + 64, h * 128 + 128), cols)
            turn_a = a * cos[:, cols] - b * sin[:, cols]
            turn_b = b * cos[:, cols] + a * sin[:, cols]
            q_out[part, cols] = (jnp.concatenate([turn_a, turn_b], axis=0) * scale_q).astype(BF)

    def out_weights():
        wo_all.near()
        wo_all.far()

    def finish():
        for half in range(PARTS):
            gone(slots[half].at[pl.ds(0, 7)], s_one.at[half])
            gone(landed[half].at[pl.ds(0, 8)], s_two.at[half])
            gone(landed[half].at[pl.ds(0, 8)], s_three.at[half])
        gone(squares.at[pl.ds(0, 15)], s_q.at[0])
        gone(near, s_c.at[0])
        gone(to_y, s_y.at[0])
        weights.sent()
        wo_all.sent()
        for one_part in gathers:
            one_part.sent()

    return out_weights, finish


class KeysValues:
    def __init__(self, kv_ref, kvs, s_x, r_x, s_c, r_c):
        x, _, c, _, _ = coords()

        def block(late):
            return lambda chunk, half: kvs.at[kept(2 * late + half, c), :, lanes(chunk * 128, 128)]

        self.gathers = [
            Gather4(
                [block(late)], "x", x, some(s_x, 2 * late), some(r_x, 3 * late),
                lambda n: kvs.at[0, :, pl.ds(0, 128 * n)],
            )
            for late in range(2)
        ]
        self.kv_ref, self.kvs, self.s_c, self.r_c = kv_ref, kvs, s_c, r_c

    def send(self, late):
        x, _, c, _, _ = coords()
        for p in (2 * late, 2 * late + 1):
            self.kvs[kept(p, c), :, lanes(x * 128, 128)] = self.kv_ref[p]
        self.gathers[late].start()

    def to_core(self, late):
        _, _, c, _, _ = coords()
        self.gathers[late].near()
        self.gathers[late].far()
        for p in (2 * late, 2 * late + 1):
            ref = self.kvs.at[kept(p, c)]
            copy_to(ref, ref, self.s_c.at[0], self.r_c.at[late], {"c": 1 - c}).start()

    def from_core(self, late):
        arrived(self.kvs.at[pl.ds(0, 2)], self.r_c.at[late])

    def sent(self):
        gone(self.kvs.at[pl.ds(0, 4)], self.s_c.at[0])
        for gather in self.gathers:
            gather.sent()


def stage_attend(q_ref, ctx, keys_values, kvs, early_sums, qs, acc, den, s_y, r_y, s_o, r_o):
    x, yl, c, z, yh = coords()
    core, y_one = {"c": 1 - c}, {"yl": 1 - yl}
    for p in range(4):
        for h in range(2):
            part = q_ref[h * 128:(h + 1) * 128, p * 128:(p + 1) * 128].astype(F32)
            qs[p, h * 128:(h + 1) * 128, :] = part.T.astype(BF)
    acc[...] = jnp.zeros_like(acc)
    den[...] = jnp.zeros_like(den)
    keys_values.to_core(0)

    def tiles(pairs, core_at, diagonal=()):
        pairs = [(p, kept(e, core_at), n in diagonal) for n, (p, e) in enumerate(pairs)]
        scores = [jnp.dot(qs[p], kvs[group, :128, :], preferred_element_type=F32) for p, group, _ in pairs]
        for (p, group, masked), score in zip(pairs, scores):
            weight = jnp.exp2((50.0 * math.log2(math.e)) * jnp.tanh(score * (1.0 / 50.0)))
            if masked:
                row = lax.rem(lax.broadcasted_iota(jnp.int32, (256, 512), 0), 128)
                col = lax.broadcasted_iota(jnp.int32, (256, 512), 1)
                weight = jnp.where(col - row <= x * 128, weight, 0.0)
            den[p] += sum([weight[:, n:n + 128] for n in range(0, 512, 128)])
            acc[p] += lax.dot_general(
                weight.astype(BF), kvs[group, 128:, :], (((1,), (1,)), ((), ())), preferred_element_type=F32
            )

    def region(core_at, y_at, at, size):
        return ctx.at[pl.ds(at + core_at * 4, size), :, lanes(y_at * 256, 256)]

    def put(step):
        for p in (2 * step, 2 * step + 1):
            for h in range(2):
                part = slice(h * 128, (h + 1) * 128)
                total = jnp.sum(den[p, part, :], axis=1, keepdims=True)
                value = (acc[p, part, :] / total).astype(BF)
                cols = lanes(yl * 256 + h * 128, 128)
                ctx[c * 4 + p, :, cols] = value[:64]
                ctx[8 + c * 4 + p, :, cols] = value[64:]
        for half in range(2):
            ref = region(c, yl, half * 8 + 2 * step, 2)
            copy_to(ref, ref, s_y.at[0], r_y.at[step], y_one).start()
            copy_to(ref, ref, s_o.at[0], r_o.at[0], core).start()

    def pass_on(step):
        arrived(ctx.at[pl.ds(0, 4), :, pl.ds(0, 256)], r_y.at[step])
        for half in range(2):
            ref = region(c, 1 - yl, half * 8 + 2 * step, 2)
            copy_to(ref, ref, s_o.at[0], r_o.at[1], core).start()

    tiles([(0, 0), (1, 0), (1, 1)], c, (0, 2))
    keys_values.from_core(0)
    tiles([(1 - c, 0), (1, 1 - c)], 1 - c)
    put(0)
    tiles([(2, 0), (2, 1), (3, 0), (3, 1)], c)
    keys_values.to_core(1)
    tiles([(2, 0), (2, 1), (3, 0), (3, 1)], 1 - c)
    tiles([(2, 2), (3, 2), (3, 3)], c, (0, 2))
    keys_values.from_core(1)
    tiles([(3 - c, 2), (3, 3 - c)], 1 - c)
    put(1)
    pass_on(0)
    arrived(ctx.at[pl.ds(0, 8), :, pl.ds(0, 256)], r_o.at[0])
    early_sums()
    pass_on(1)
    arrived(ctx.at[pl.ds(0, 8), :, pl.ds(0, 256)], r_o.at[1])

    def finish():
        gone(ctx.at[pl.ds(0, 8), :, pl.ds(0, 256)], s_y.at[0])
        gone(ctx.at[:, :, pl.ds(0, 256)], s_o.at[0])
        keys_values.sent()

    return finish


class Reduce4:
    def __init__(self, z, send, got, more, more_got, s, r):
        self.one, self.two = z + 1 - 2 * lax.rem(z, 2), 3 - z
        self.far = self.two + 1 - 2 * lax.rem(self.two, 2)
        self.send, self.got, self.more, self.more_got, self.s, self.r = send, got, more, more_got, s, r

    def partner(self, part, step):
        return {"z": self.one if part == step else self.two}

    def chunk(self, part, slot):
        return self.far if slot == 1 else (self.two if part else self.one)

    def give(self, part, slot, value):
        self.send[part, slot] = value
        copy_to(
            self.send.at[part, slot], self.got.at[part, slot], self.s.at[0], self.r.at[slot], self.partner(part, 0)
        ).start()

    def pass_on(self, values):
        arrived(self.got.at[0], self.r.at[1])
        for part, value in enumerate(values):
            self.more[part] = (value + self.got[part, 1].astype(F32)).astype(BF)
            copy_to(
                self.more.at[part], self.more_got.at[part], self.s.at[1], self.r.at[2], self.partner(part, 1)
            ).start()

    def own(self, values):
        arrived(self.got.at[0], self.r.at[0])
        arrived(self.more_got, self.r.at[2])
        return [
            value + self.got[part, 0].astype(F32) + self.more_got[part].astype(F32) for part, value in enumerate(values)
        ]

    def sent(self):
        gone(self.send, self.s.at[0])
        gone(self.more, self.s.at[1])


class OutSums:
    def __init__(self, ctx, wo, own_y, own_a, own_b):
        _, yl, _, _, yh = coords()
        self.ctx, self.wo, self.yl = ctx, wo, yl
        self.all = [(own_y, 1 - yh, 1), (own_a.at[0], 0, 0), (own_a.at[1], 1, 0), (own_b, yh, 1)]

    def product(self, n, y):
        _, half, part = self.all[n]
        left = self.wo[part * 4 * OUT[0]:part * 4 * OUT[0] + 4 * OUT[part], lanes(y * 256, 256)]
        right = self.ctx[pl.ds(half * 8, 8), :, lanes(y * 256, 256)].reshape(512, 256)
        value = lax.dot_general(left, right, (((1,), (1,)), ((), ())), preferred_element_type=F32)
        return value.reshape(4, OUT[part], 512)

    def early(self):
        for n, (dst, _, _) in enumerate(self.all):
            dst[...] = self.product(n, self.yl)

    def late(self, n):
        dst = self.all[n][0]
        dst[...] = dst[...] + self.product(n, 1 - self.yl)


def stage_out(
    new_ref, ctx, xs, wo, gain, out_ref, out_sums, own_y, own_a, own_b,
    a_send, a_got, a_more, a_more_got, b_send, b_got, b_more, b_more_got,
    y_send, y_relay, y_got, h_send, h_relay, h_got, total,
    squares, fresh, f1, f2, f1_got, fin,
    a_s, a_r, b_s, b_r, s_y, r_y, s_h, r_h, s_q, r_q, s_f, r_f, s_g, r_g, s_c, r_c,
):
    x, yl, c, z, yh = coords()
    core = {"c": 1 - c}
    y_one, y_two = {"yl": 1 - yl}, {"yl": 1 - yl, "yh": 1 - yh}
    group = [
        {"z": lax.rem(z + dz, 4), "yl": yl + dy - 2 * yl * dy, "c": c + dc - 2 * c * dc}
        for dz in (0, 2, 1, 3) for dy in (0, 1) for dc in (0, 1)
    ]
    group = group[4:] + group[1:4]
    others = [{"x": lax.rem(x + dx, 4)} for dx in (2, 1, 3)]

    one, two = z + 1 - 2 * lax.rem(z, 2), 3 - z
    wanted = (two + 1 - 2 * lax.rem(two, 2), one, two, z)
    out_sums.late(0)
    for n in range(4):
        y_send[n] = own_y[wanted[n]].astype(BF)
    for n in range(4):
        copy_to(y_send.at[n], y_relay.at[n], s_y.at[0], r_y.at[n // 2], y_two if n % 2 else y_one).start()
    first = Reduce4(z, a_send, a_got, a_more, a_more_got, a_s, a_r)
    for part in range(2):
        out_sums.late(1 + part)
        first.give(part, 1, own_a[part, first.chunk(part, 1)].astype(BF))
    for part in range(2):
        first.give(part, 0, own_a[part, first.chunk(part, 0)].astype(BF))
    out_sums.late(3)

    def forward(step):
        arrived(y_relay.at[pl.ds(0, 2)], r_y.at[step])
        for n in (2 * step, 2 * step + 1):
            copy_to(y_relay.at[n], y_got.at[n], s_y.at[1], r_y.at[2 + step], y_one if n % 2 else y_two).start()

    forward(0)
    first.pass_on([own_a[0, first.two], own_a[1, first.one]])
    forward(1)
    second = Reduce4(z, b_send, b_got, b_more, b_more_got, b_s, b_r)
    cols = (slice(0, 256), slice(256, 512))

    def over_y(step):
        arrived(y_got.at[pl.ds(0, 2)], r_y.at[2 + step])
        for n in (2 * step, 2 * step + 1):
            own_b[wanted[n]] = own_b[wanted[n]] + y_got[n].astype(F32)

    over_y(0)
    second.give(0, 1, own_b[wanted[0], :, cols[0]].astype(BF))
    second.give(1, 1, own_b[wanted[0], :, cols[1]].astype(BF))
    second.give(0, 0, own_b[one, :, cols[0]].astype(BF))
    for part, value in enumerate(first.own([own_a[0, z], own_a[1, z]])):
        own_a[part, z] = value
    h_send[...] = own_a[1 - yh, z].astype(BF)
    spans = (slice(0, 80), slice(80, OUT[0]))
    for n, peer in enumerate((y_one, y_two)):
        copy_to(h_send.at[spans[n]], h_relay.at[spans[n]], s_h.at[0], r_h.at[0], peer).start()
    over_y(1)
    second.give(1, 0, own_b[two, :, cols[1]].astype(BF))
    second.pass_on([own_b[two, :, cols[0]], own_b[one, :, cols[1]]])
    arrived(h_relay, r_h.at[0])
    for n, peer in enumerate((y_two, y_one)):
        copy_to(h_relay.at[spans[n]], h_got.at[spans[n]], s_h.at[1], r_h.at[1], peer).start()
    for part, value in enumerate(second.own([own_b[z, :, cols[0]], own_b[z, :, cols[1]]])):
        total[OUT[0]:, cols[part]] = value
    arrived(h_got, r_h.at[1])
    total[:OUT[0], :] = own_a[yh, z] + h_got[...].astype(F32)
    me = z * 4 + yl * 2 + c
    for m in range(4):
        value = total[:, m * 128:(m + 1) * 128]
        squares[me, m:m + 1, :] = jnp.sum(value * value, axis=0, keepdims=True)
    for peer in group:
        copy_to(squares.at[me], squares.at[me], s_q.at[0], r_q.at[0], peer).start()
    lane = lax.broadcasted_iota(jnp.int32, (96, 128), 1)

    def pair(m, part):
        begin, count = BACK[part]
        low = lane[:count] < 64
        at = pl.ds(pl.multiple_of(z * 288 + begin, 32), count)
        a = xs[at, m * 256:m * 256 + 128].astype(F32)
        b = xs[at, m * 256 + 128:m * 256 + 256].astype(F32)
        upper, lower = pltpu.roll(a, 64, 1), pltpu.roll(b, 64, 1)
        return jnp.where(low, jnp.where(yh == 0, a, upper), jnp.where(yh == 0, lower, b))

    for part in range(PARTS):
        for m in range(4):
            fresh[part][m] = pair(m, part)
    arrived(squares.at[pl.ds(0, 15)], r_q.at[0])
    factor = lax.rsqrt(jnp.sum(squares[...], axis=0) * (1.0 / D) + EPS)
    starts, so_far = [], 0
    for j in range(16):
        starts.append(so_far)
        so_far = so_far + new_ref[j]
    here = pl.ds(x * 2, 2)
    for part, (begin, count) in enumerate(BACK):
        rows_of = slice(begin, begin + count)
        low = lane[:count] < 64
        for m in range(4):
            value = total[rows_of, m * 128:(m + 1) * 128] * factor[m:m + 1, :] * gain[rows_of, :]
            fresh[part][m] = fresh[part][m] + value
        for n in range(8):
            sides = []
            for side in range(2):
                j = 2 * n + side
                within = lax.rem(x - starts[j] + 64, 4)
                i = jnp.minimum(lax.div(starts[j] + within - x, 4), 7)
                at = lax.div(i, 2)
                place = lax.rem(i + at, 2) * 4 + at
                value = fresh[part][lax.div(place, 2)]
                value = jnp.where(lax.rem(place, 2) == side, value, pltpu.roll(value, 64, 1))
                sides.append(jnp.where(within < new_ref[j], value, 0.0))
            f1[part][n] = jnp.where(low, sides[0], sides[1]).astype(BF)
        f1_got[part][here] = f1[part][here]
        for peer in others:
            copy_to(
                f1[part].at[pl.ds(peer["x"] * 2, 2)], f1_got[part].at[here], s_f.at[part], r_f.at[part], peer
            ).start()
    mine = [sum([jnp.where(x * 4 + n > m, new_ref[m], 0) for m in range(15)]) for n in range(4)]
    for part, (begin, count) in enumerate(BACK):
        rows_of = slice(begin, begin + count)
        low = lane[:count] < 64
        arrived(f1_got[part].at[pl.ds(0, 6)], r_f.at[part])
        for e in (5, 4, 3, 7, 2, 6, 1, 0):
            dz, dy = e // 2, e % 2
            tz, ty = lax.rem(z + dz, 4), yl + dy - 2 * yl * dy
            sides = []
            for side in range(2):
                start = jnp.where(ty == 0, mine[side], mine[2 + side])
                sides.append(f1_got[part][lax.rem(start + tz, 4) * 2 + ty].astype(F32))
            value = jnp.where(low, sides[0], sides[1]).astype(BF)
            at = z * 2 + yl
            if e == 0:
                fin[at, c, rows_of, :] = value
            else:
                f2[part][e] = value
                copy_to(
                    f2[part].at[e], fin.at[at, c, rows_of], s_g.at[part], r_g.at[part], {"z": tz, "yl": ty}
                ).start()
    for part, (begin, count) in enumerate(BACK):
        rows_of = slice(begin, begin + count)
        arrived(fin.at[pl.ds(0, 7), c, rows_of], r_g.at[part])
        ref = fin.at[:, c, rows_of]
        copy_to(ref, ref, s_c.at[0], r_c.at[0], core).start()
    arrived(fin.at[:, c], r_c.at[0])
    mine_of = lax.broadcasted_iota(jnp.int32, (64, 128), 0) + c * 64
    pick = jnp.where(lane[:64] == mine_of, 1.0, 0.0).astype(BF)
    for n in range(4):
        block = fin[2 * n:2 * n + 2].reshape(1152, 128)
        value = lax.dot_general(pick, block, (((1,), (1,)), ((), ())), preferred_element_type=F32)
        out_ref[:, n * 1152:(n + 1) * 1152] = value.astype(BF)
    first.sent()
    second.sent()
    gone(y_send, s_y.at[0])
    gone(y_relay, s_y.at[1])
    gone(h_send, s_h.at[0])
    gone(h_relay, s_h.at[1])
    gone(squares.at[pl.ds(0, 15)], s_q.at[0])
    for part in range(PARTS):
        gone(f1[part].at[pl.ds(0, 6)], s_f.at[part])
        gone(f2[part].at[pl.ds(0, 7)], s_g.at[part])
    gone(fin.at[:, c], s_c.at[0])


STAGE_IN = [
    VM((1152, 512), BF), VM((1152, 256), BF), VM((1152, 256), BF),
    VM((1152, 128), F32), VM((128, 128), F32), VM((64, 512), F32), VM((64, 512), F32),
    VM((576, 512), BF), [VM((8, count, 128), BF) for _, count in IN], [VM((24, count, 128), BF) for _, count in IN], VM((1152, 1024), BF), VM((16, 8, 128), F32),
    VM((2, 512, 512), F32), VM((2, 512, 512), F32), VM((512, 512), BF), VM((512, 512), BF), VM((2, 512, 512), F32),
    DMA((2,)), DMA((PARTS,)), DMA((4 * PARTS,)), DMA((PARTS,)), DMA((4 * PARTS,)), DMA((PARTS,)), DMA((PARTS,)),
    DMA((2,)), DMA((3,)), DMA((2,)), DMA((3,)), DMA((2 * PARTS,)), DMA((3 * PARTS,)), DMA((1,)), DMA((1,)),
    DMA((1,)), DMA((4,)), DMA((1,)), DMA((4,)),
]
STAGE_ATTEND = [
    VM((4, 256, 128), BF), VM((4, 256, 128), F32), VM((4, 256, 128), F32),
    DMA((1,)), DMA((2,)), DMA((1,)), DMA((2,)),
]
STAGE_OUT = (
    [VM((2, 2, OUT[0], 512), BF), VM((2, 2, OUT[0], 512), BF), VM((2, OUT[0], 512), BF), VM((2, OUT[0], 512), BF)]
    + [VM((2, 2, OUT[1], 256), BF), VM((2, 2, OUT[1], 256), BF), VM((2, OUT[1], 256), BF), VM((2, OUT[1], 256), BF)]
    + [VM((4, OUT[1], 512), BF)] * 3
    + [VM((OUT[0], 512), BF)] * 3
    + [VM((288, 512), F32), VM((16, 4, 128), F32), [VM((4, count, 128), F32) for _, count in BACK]]
    + [[VM((8, count, 128), BF) for _, count in BACK]] * 3
    + [VM((8, 2, 288, 128), BF)]
    + [DMA((2,)), DMA((3,)), DMA((2,)), DMA((3,))]
    + [DMA((2,)), DMA((4,)), DMA((2,)), DMA((2,)), DMA((1,)), DMA((1,)), DMA((PARTS,)), DMA((PARTS,))]
    + [DMA((PARTS,)), DMA((PARTS,)), DMA((1,)), DMA((1,))]
)
SHARED = [
    VM((256, 512), BF), VM((4, 256, 128), BF), VM((1152, 1024), BF), VM((1152, 512), BF), VM((16, 64, 512), BF),
    VM((288, 128), F32), VM((8, 256, 512), BF), DMA((4,)), DMA((6,)), DMA((1,)), DMA((2,)),
    VM((4, OUT[1], 512), F32), VM((2, 4, OUT[0], 512), F32), VM((4, OUT[1], 512), F32),
]


def kernel(old_ref, new_ref, order_ref, xt_in, pre_ref, post_ref, wq_in, wk_in, wv_in, wo_in, out_ref, *scratch):
    q, kv, xs, wo, ctx, gain_out, kvs, s_x, r_x, s_c, r_c, own_y, own_a, own_b = scratch[:14]
    scratch = scratch[14:]
    out_sums = OutSums(ctx, wo, own_y, own_a, own_b)
    keys_values = KeysValues(kv, kvs, s_x, r_x, s_c, r_c)
    own_in, scratch = scratch[:len(STAGE_IN)], scratch[len(STAGE_IN):]
    own_attend, own_out = scratch[:len(STAGE_ATTEND)], scratch[len(STAGE_ATTEND):]
    out_weights, end_in = stage_in(
        old_ref, order_ref, xt_in, pre_ref, post_ref, wq_in, wk_in, wv_in, wo_in, q, kv, xs, wo, gain_out, *own_in,
        keys_values,
    )

    def early_sums():
        out_weights()
        out_sums.early()

    end_attend = stage_attend(q, ctx, keys_values, kvs, early_sums, *own_attend)
    end_in()
    stage_out(new_ref, ctx, xs, wo, gain_out, out_ref, out_sums, own_y, own_a, own_b, *own_out)
    end_attend()


def run(old_blocks, new_blocks, order, xt, pre_gain, post_gain, w_query, w_key, w_value, w_out_t):
    smem = pl.BlockSpec(memory_space=pltpu.SMEM)
    vmem = pl.BlockSpec(memory_space=pltpu.VMEM)
    hbm = pl.BlockSpec(memory_space=pltpu.HBM)
    return pl.pallas_call(
        kernel,
        name="sublayer",
        out_shape=jax.ShapeDtypeStruct((64, D), BF),
        in_specs=[smem, smem, smem, hbm, vmem, vmem, hbm, hbm, hbm, hbm],
        out_specs=vmem,
        scratch_shapes=SHARED + STAGE_IN + STAGE_ATTEND + STAGE_OUT,
        compiler_params=pltpu.CompilerParams(collective_id=0, has_side_effects=True, vmem_limit_bytes=62 * 2**20),
    )(old_blocks, new_blocks, order, xt, pre_gain, post_gain, w_query, w_key, w_value, w_out_t)


def per_device(
    x_old, old_blocks, new_blocks, order, pre_gain, post_gain, w_query, w_key, w_value, w_out_t
):
    return run(
        old_blocks, new_blocks, order, x_old.T, pre_gain.reshape(36, 128), post_gain.reshape(36, 128),
        w_query, w_key, w_value, w_out_t,
    )


def solution(mesh):
    torus = Mesh(mesh.devices.reshape(4, 2, 2, 4, 2), ("x", "yl", "c", "z", "yh"))
    seq, tp = ("x", "yl", "c"), ("z", "yh")
    both = P(seq, tp)
    in_specs = (both, P(), P(), P(), P(), P(), both, both, both, both)
    return jax.shard_map(
        per_device, mesh=torus, in_specs=in_specs, out_specs=P(seq + tp, None), check_vma=False
    )
```

```python
import functools
import math

import jax
import jax.numpy as jnp
from jax import lax
from jax.experimental import pallas as pl
from jax.experimental.pallas import tpu as pltpu
from jax.sharding import Mesh
from jax.sharding import PartitionSpec as P

D = 4608
HEADS = 32
HEAD = 128
BLOCK = 128
EPS = 1e-06
BF = jnp.bfloat16
F32 = jnp.float32
VM = pltpu.VMEM
OUT = (144, 144)
IN = ((0, 32), (32, 64), (96, 96), (192, 96))
BACK = ((0, 96), (96, 96), (192, 64), (256, 32))
PARTS = 4
DMA = pltpu.SemaphoreType.DMA


def kept(at, c):
    return 2 * at + lax.rem(at + c, 2)


def coords():
    return tuple(lax.axis_index(name) for name in ("x", "yl", "c", "z", "yh"))


def copy_to(src, dst, send_sem, recv_sem, device):
    return pltpu.make_async_remote_copy(
        src_ref=src,
        dst_ref=dst,
        send_sem=send_sem,
        recv_sem=recv_sem,
        device_id=device,
        device_id_type=pl.DeviceIdType.MESH,
    )


def greet(devices):
    sem = pltpu.get_barrier_semaphore()
    for device in devices:
        pl.semaphore_signal(sem, inc=1, device_id=device, device_id_type=pl.DeviceIdType.MESH)


def greeted(devices):
    pl.semaphore_wait(pltpu.get_barrier_semaphore(), len(devices))


def mod4(v):
    return lax.rem(v + 4, 4)


def arrived(ref, sem):
    copy_to(ref, ref, sem, sem, {"c": 1 - lax.axis_index("c")}).wait_recv()


def gone(ref, sem):
    copy_to(ref, ref, sem, sem, {"c": 1 - lax.axis_index("c")}).wait_send()


class Gather4:
    def __init__(self, views, axis, me, send, recv, size):
        one, two = me + 1 - 2 * lax.rem(me, 2), 3 - me
        far = two + 1 - 2 * lax.rem(two, 2)
        self.moves = [
            (me, one, 0, one),
            (me, two, 1, two),
            (me, two, 0, two),
            (me, one, 1, one),
            (one, far, 0, two),
            (two, far, 1, one),
        ]
        self.views, self.axis, self.send, self.recv, self.size = views, axis, send, recv, size

    def go(self, *moves):
        for move in moves:
            sent, _, half, partner = self.moves[move]
            for view in self.views:
                ref = view(sent, half)
                copy_to(ref, ref, self.send(move // 4), self.recv(move // 2), {self.axis: partner}).start()

    def start(self):
        self.go(0, 1, 2, 3)

    def relay(self):
        arrived(self.size(2), self.recv(0))
        self.go(4, 5)

    def near(self):
        arrived(self.size(2), self.recv(1))

    def far(self):
        arrived(self.size(2), self.recv(2))

    def sent(self):
        gone(self.size(4), self.send(0))
        gone(self.size(2), self.send(1))


def some(sems, start):
    return lambda n: sems.at[start + n]


def rows(ref, start, size, unit=16):
    return ref.at[pl.ds(pl.multiple_of(start, unit), size)]


def lanes(start, size):
    return pl.ds(pl.multiple_of(start, 128), size)


def columns(dst, table, chunk_of, count):
    lane = lax.broadcasted_iota(jnp.int32, (32, 128), 1)

    def body(n, _):
        feature = chunk_of(lax.div(n, 9)) * 288 + lax.rem(n, 9) * 32
        part = table[pl.ds(pl.multiple_of(lax.rem(feature, 128), 32), 32), :]
        value = jnp.sum(jnp.where(lane == lax.div(feature, 128), part, 0.0), axis=1, keepdims=True)
        dst[pl.ds(pl.multiple_of(n * 32, 32), 32), :] = jnp.broadcast_to(value, (32, 128))
        return 0

    lax.fori_loop(0, count * 9, body, 0)


def stage_in(
    old_ref, order_ref, xt_in, pre_ref, post_ref, wq_in, wk_in, wv_in, wo_in,
    q_out, kv_out, xs, wo, gain_out,
    wq, wk, wv, gain, table, cos, sin, xt, slots, landed, normed, squares, near, other, to_y, from_y, mine,
    s_w, s_one, r_one, s_two, r_two, s_three, r_three, s_wg, r_wg, s_og, r_og, s_z, r_z, s_q, r_q, s_c, r_c, s_y, r_y,
    keys_values,
):
    x, yl, c, z, yh = coords()
    ring_peers = [
        {"x": lax.rem(x + dx, 4), "c": c + dc - 2 * c * dc} for dx in range(4) for dc in range(2)
    ][1:]
    y_one = {"yl": 1 - yl}
    y_two = {"yl": 1 - yl, "yh": 1 - yh}
    group = [
        {"z": lax.rem(z + dz, 4), "yl": yl + dy - 2 * yl * dy, "c": c + dc - 2 * c * dc}
        for dz in (0, 2, 1, 3) for dy in range(2) for dc in range(2)
    ][1:]
    greet(ring_peers + [y_two] + group)
    into = pltpu.make_async_copy(xt_in, xt, s_w.at[1])
    into.start()
    at = pl.ds(pl.multiple_of(x * 288, 16), 288)
    owns = [
        pltpu.make_async_copy(src, dst.at[at], s_w.at[0]) for src, dst in ((wq_in, wq), (wk_in, wk), (wv_in, wv))
    ]

    def out_rows(chunk, half):
        return rows(wo, half * 4 * OUT[0] + chunk * OUT[half], OUT[half])

    for half in range(2):
        part = wo_in.at[pl.ds(half * OUT[0], OUT[half])]
        owns.append(pltpu.make_async_copy(part, out_rows(x, half), s_w.at[0]))
    for copy in owns:
        copy.start()
    starts, total = [], 0
    for m in range(16):
        starts.append(total)
        total = total + old_ref[m]
    k = order_ref[x * 4 + yl * 2 + c]
    first = sum([jnp.where(k > m, old_ref[m], 0) for m in range(15)])
    into.wait()
    for r in range(4):
        b = lax.rem(r - first + 64, 4)
        for h in range(2):
            for half, (begin, count) in enumerate(IN):
                at_rows = slice(h * 288 + begin, h * 288 + begin + count)
                part = [xt[at_rows, n * 128:(n + 1) * 128] for n in range(4)]
                low = jnp.where(b == 0, part[0], part[1])
                slots[half][r * 2 + h] = jnp.where(b < 2, low, jnp.where(b == 2, part[2], part[3]))
    here = x * 2 + c
    for half in range(PARTS):
        landed[half][here] = slots[half][here]
    greeted(ring_peers + [y_two] + group)
    for half in range(PARTS):
        for d, peer in enumerate(ring_peers, 1):
            copy_to(
                slots[half].at[peer["x"] * 2 + peer["c"]], landed[half].at[here],
                s_one.at[half], r_one.at[half * 4 + d // 2], peer,
            ).start()
    everything = wo.at[pl.ds(0, 864)]
    pltpu.make_async_copy(everything, everything, s_w.at[0]).wait()

    def half_rows(ref):
        return lambda chunk, half: rows(ref, chunk * 288 + half * 144, 144)

    weights = Gather4(
        [half_rows(r) for r in (wq, wk, wv)], "x", x, some(s_wg, 0), some(r_wg, 0), lambda n: wq.at[pl.ds(0, 288 * n)]
    )
    weights.start()
    straight = yl == yh

    def slot_pair(half, dx, where):
        return landed[half].at[pl.ds(where * 8 + mod4(x - dx) * 2, 2)]

    def relay_y(n):
        half, dx = n // 4, n % 4
        arrived(slot_pair(half, dx, 1), r_two.at[n])
        copy = copy_to(slot_pair(half, dx, 1), slot_pair(half, dx, 2), s_three.at[half], r_three.at[half], y_one)
        pl.when(straight)(copy.start)

    for half in range(PARTS):
        for dx in range(4):
            n = half * 4 + dx
            from_x = slot_pair(half, dx, 0) if dx > 0 else landed[half].at[x * 2 + 1 - c]
            arrived(from_x, r_one.at[n])
            copy_to(slot_pair(half, dx, 0), slot_pair(half, dx, 1), s_two.at[half], r_two.at[n], y_two).start()
            copy = copy_to(slot_pair(half, dx, 0), slot_pair(half, dx, 2), s_three.at[half], r_three.at[half], y_one)
            pl.when(jnp.logical_not(straight))(copy.start)
            if half >= 2:
                relay_y(half * 4 - 8 + dx)
    me = z * 4 + yl * 2 + c
    first_buffer = jnp.where(straight, 0, 1)

    def part_rows(part):
        begin, count = IN[part]
        return lambda chunk, half: rows(xs, chunk * 288 + begin + half * (count // 2), count // 2)

    def some_rows(part):
        return lambda n: xs.at[pl.ds(0, IN[part][1] // 2 * n)]

    gathers = [
        Gather4(
            [part_rows(part)], "z", z, some(s_z, 2 * part), some(r_z, 3 * part),
            some_rows(part),
        )
        for part in range(PARTS)
    ]
    sources = []
    for place in range(8):
        g = x + 4 * kept(place % 4, place // 4)
        shard = sum([jnp.where(starts[m] <= g, 1, 0) for m in range(16)]) - 1
        holder = sum([jnp.where(order_ref[p] == shard, p, 0) for p in range(16)])
        y_source = lax.rem(lax.div(holder, 2), 2)
        sources.append(jnp.where(y_source == yh, first_buffer, 2) * 8 + lax.div(holder, 4) * 2 + lax.rem(holder, 2))

    def pick(half):
        arrived(landed[half].at[pl.ds(16, 8)], r_three.at[half])
        for place in range(8):
            block = landed[half][sources[place]]
            begin, count = IN[half]
            xs[pl.ds(pl.multiple_of(z * 288 + begin, 32), count), place * 128:(place + 1) * 128] = block
            wide = block.astype(F32)
            square = jnp.sum(wide * wide, axis=0, keepdims=True)
            if half > 0:
                square = square + squares[me, place:place + 1, :]
            squares[me, place:place + 1, :] = square
        if half == PARTS - 1:
            for peer in group:
                copy_to(squares.at[me], squares.at[me], s_q.at[0], r_q.at[0], peer).start()
        gathers[half].start()

    pick(0)
    for n in range(8, 16):
        if n in (10, 14):
            pick(1 + (n - 10) // 4)
            if n == 10:
                gathers[0].relay()
        relay_y(n)
    pick(3)
    gathers[1].relay()
    weights.relay()
    wo_all = Gather4(
        [out_rows], "x", x, some(s_og, 0), some(r_og, 0), lambda n: wo.at[pl.ds(0, 144 * n)]
    )
    wo_all.start()
    table[...] = jnp.zeros_like(table)
    table[0:36, :] = pre_ref[...]
    table[...] = table[...].T
    columns(gain, table, lambda n: n * 4 + yl * 2 + c, 4)
    table[...] = jnp.zeros_like(table)
    table[0:36, :] = post_ref[...]
    table[...] = table[...].T
    columns(gain_out, table, lambda n: z * 4 + yl * 2 + c, 1)
    gathers[2].relay()
    half_head = HEAD // 2
    inverse = jnp.exp(
        lax.broadcasted_iota(jnp.int32, (half_head, 128), 0).astype(F32) * (-2.0 * math.log(10000.0) / HEAD)
    )
    for p in range(4):
        place_of = (x + 4 * kept(p, c)) * BLOCK + lax.broadcasted_iota(jnp.int32, (half_head, 128), 1)
        angle = inverse * place_of.astype(F32)
        cos[:, p * 128:(p + 1) * 128] = jnp.cos(angle)
        sin[:, p * 128:(p + 1) * 128] = jnp.sin(angle)
    gathers[3].relay()
    arrived(squares.at[pl.ds(0, 15)], r_q.at[0])
    factor = lax.rsqrt(jnp.sum(squares[...], axis=0) * (1.0 / D) + EPS)

    def norm(chunk):
        for place in range(8):
            scale = factor[place:place + 1, :]

            def norm_rows(n, _, place=place, scale=scale):
                part = pl.ds(pl.multiple_of(chunk * 288 + n * 144, 16), 144)
                at = (part, slice(place * 128, (place + 1) * 128))
                normed[at] = (xs[at].astype(F32) * scale * gain[part, :]).astype(BF)
                return 0

            lax.fori_loop(0, 2, norm_rows, 0)

    pieces = {"q": (slice(0, 256), wq, 256), "k": (slice(256, 384), wk, 128), "v": (slice(384, 512), wv, 128)}

    def corner(dst, y, core, late, names="qkv", part=None):
        if not late:
            part = pl.ds(pl.multiple_of(lax.div(z, 2) * 576, 16), 576)
        elif part is None:
            part = pl.ds(pl.multiple_of(far * 288, 16), 288)
        right = normed[part, lanes(core * 512, 512)]
        for name in names:
            to, table_of, width = pieces[name]
            left = table_of[part, lanes(y * width, width)]
            value = lax.dot_general(left, right, (((0,), (0,)), ((), ())), preferred_element_type=F32)
            if late:
                dst[to, :] += value
            else:
                dst[to, :] = value

    norm(z)
    for one_part in gathers:
        one_part.near()
    norm(z + 1 - 2 * lax.rem(z, 2))
    weights.near()
    weights.far()
    corners = [
        (near.at[0], 1 - yl, 1 - c), (mine.at[0], 1 - yl, c), (near.at[1], yl, 1 - c), (mine.at[1], yl, c),
    ]
    for dst, y, core in corners:
        corner(dst, y, core, False)
    far = (3 - z) + 1 - 2 * lax.rem(3 - z, 2)
    norm(3 - z)
    for dst, y, core in corners:
        corner(dst, y, core, True, part=pl.ds(pl.multiple_of((3 - z) * 288, 16), 288))
    wo_all.relay()
    for one_part in gathers:
        one_part.far()
    norm(far)
    core = {"c": 1 - c}

    def over_core(n, name):
        to = pieces[name][0]
        recv = r_c.at["kvq".index(name) if n == 0 else 3]
        copy_to(near.at[n, to], other.at[n, to], s_c.at[0], recv, core).start()

    first_rows, last_rows = slice(0, 256), slice(256, 512)
    k_part, v_part = slice(256, 384), slice(384, 512)
    spans = (
        (0, k_part, first_rows), (1, v_part, first_rows), (2, k_part, last_rows), (3, v_part, last_rows),
        (4, slice(0, 256), first_rows), (5, slice(0, 256), last_rows),
    )

    def over_y(name):
        to = pieces[name][0]
        arrived(other.at[0, to], r_c.at["kvq".index(name)])
        to_y[to, :] = (mine[0, to, :] + other[0, to, :]).astype(BF)
        for at, part, cols in {"k": spans[:1], "v": spans[1:4], "q": spans[4:]}[name]:
            copy_to(to_y.at[part, cols], from_y.at[part, cols], s_y.at[0], r_y.at[at // 2 if at < 4 else at - 2], y_one).start()

    for name in "kv":
        corner(*corners[0], True, name)
        over_core(0, name)
    corner(*corners[1], True, "k")
    over_y("k")
    corner(*corners[1], True, "v")
    corner(*corners[0], True, "q")
    over_core(0, "q")
    over_y("v")
    corner(*corners[1], True, "q")
    over_y("q")
    corner(*corners[2], True)
    for name in "kvq":
        over_core(1, name)
    corner(*corners[3], True)
    arrived(other.at[1], r_c.at[3])
    scale_q = (D // HEADS) ** (-0.5)

    def summed(part, cols):
        return mine[1, part, cols] + other[1, part, cols] + from_y[part, cols].astype(F32)

    def turned(value, cols):
        a, b = value[:64], value[64:]
        return jnp.concatenate(
            [a * cos[:, cols] - b * sin[:, cols], b * cos[:, cols] + a * sin[:, cols]], axis=0
        ).astype(BF)

    for late, cols in enumerate((first_rows, last_rows)):
        arrived(from_y.at[pl.ds(256, 256), cols], r_y.at[late])
        key = turned(summed(k_part, cols), cols)
        value = summed(v_part, cols).astype(BF)
        for p in range(2):
            kv_out[2 * late + p, :128, :] = key[:, p * 128:(p + 1) * 128]
            kv_out[2 * late + p, 128:, :] = value[:, p * 128:(p + 1) * 128]
        keys_values.send(late)
    for late in range(2):
        keys_values.gathers[late].relay()
    for late, cols in enumerate((first_rows, last_rows)):
        arrived(from_y.at[pl.ds(0, 256), cols], r_y.at[2 + late])
        for h in range(2):
            part = slice(h * 128, (h + 1) * 128)
            a, b = summed(slice(h * 128, h * 128 + 64), cols), summed(slice(h * 128 + 64, h * 128 + 128), cols)
            turn_a = a * cos[:, cols] - b * sin[:, cols]
            turn_b = b * cos[:, cols] + a * sin[:, cols]
            q_out[part, cols] = (jnp.concatenate([turn_a, turn_b], axis=0) * scale_q).astype(BF)

    def out_weights():
        wo_all.near()
        wo_all.far()

    def finish():
        for half in range(PARTS):
            gone(slots[half].at[pl.ds(0, 7)], s_one.at[half])
            gone(landed[half].at[pl.ds(0, 8)], s_two.at[half])
            gone(landed[half].at[pl.ds(0, 8)], s_three.at[half])
        gone(squares.at[pl.ds(0, 15)], s_q.at[0])
        gone(near, s_c.at[0])
        gone(to_y, s_y.at[0])
        weights.sent()
        wo_all.sent()
        for one_part in gathers:
            one_part.sent()

    return out_weights, finish


class KeysValues:
    def __init__(self, kv_ref, kvs, s_x, r_x, s_c, r_c):
        x, _, c, _, _ = coords()

        def block(late):
            return lambda chunk, half: kvs.at[kept(2 * late + half, c), :, lanes(chunk * 128, 128)]

        self.gathers = [
            Gather4(
                [block(late)], "x", x, some(s_x, 2 * late), some(r_x, 3 * late),
                lambda n: kvs.at[0, :, pl.ds(0, 128 * n)],
            )
            for late in range(2)
        ]
        self.kv_ref, self.kvs, self.s_c, self.r_c = kv_ref, kvs, s_c, r_c

    def send(self, late):
        x, _, c, _, _ = coords()
        for p in (2 * late, 2 * late + 1):
            self.kvs[kept(p, c), :, lanes(x * 128, 128)] = self.kv_ref[p]
        self.gathers[late].start()

    def to_core(self, late):
        _, _, c, _, _ = coords()
        self.gathers[late].near()
        self.gathers[late].far()
        for p in (2 * late, 2 * late + 1):
            ref = self.kvs.at[kept(p, c)]
            copy_to(ref, ref, self.s_c.at[0], self.r_c.at[late], {"c": 1 - c}).start()

    def from_core(self, late):
        arrived(self.kvs.at[pl.ds(0, 2)], self.r_c.at[late])

    def sent(self):
        gone(self.kvs.at[pl.ds(0, 4)], self.s_c.at[0])
        for gather in self.gathers:
            gather.sent()


def stage_attend(q_ref, ctx, keys_values, kvs, early_sums, qs, acc, den, s_y, r_y, s_o, r_o):
    x, yl, c, z, yh = coords()
    core, y_one = {"c": 1 - c}, {"yl": 1 - yl}
    for p in range(4):
        for h in range(2):
            part = q_ref[h * 128:(h + 1) * 128, p * 128:(p + 1) * 128].astype(F32)
            qs[p, h * 128:(h + 1) * 128, :] = part.T.astype(BF)
    acc[...] = jnp.zeros_like(acc)
    den[...] = jnp.zeros_like(den)
    keys_values.to_core(0)

    def tiles(pairs, core_at, diagonal=()):
        pairs = [(p, kept(e, core_at), n in diagonal) for n, (p, e) in enumerate(pairs)]
        scores = [jnp.dot(qs[p], kvs[group, :128, :], preferred_element_type=F32) for p, group, _ in pairs]
        for (p, group, masked), score in zip(pairs, scores):
            weight = jnp.exp2((50.0 * math.log2(math.e)) * jnp.tanh(score * (1.0 / 50.0)))
            if masked:
                row = lax.rem(lax.broadcasted_iota(jnp.int32, (256, 512), 0), 128)
                col = lax.broadcasted_iota(jnp.int32, (256, 512), 1)
                weight = jnp.where(col - row <= x * 128, weight, 0.0)
            den[p] += sum([weight[:, n:n + 128] for n in range(0, 512, 128)])
            acc[p] += lax.dot_general(
                weight.astype(BF), kvs[group, 128:, :], (((1,), (1,)), ((), ())), preferred_element_type=F32
            )

    def region(core_at, y_at, at, size):
        return ctx.at[pl.ds(at + core_at * 4, size), :, lanes(y_at * 256, 256)]

    def put(step):
        for p in (2 * step, 2 * step + 1):
            for h in range(2):
                part = slice(h * 128, (h + 1) * 128)
                total = jnp.sum(den[p, part, :], axis=1, keepdims=True)
                value = (acc[p, part, :] / total).astype(BF)
                cols = lanes(yl * 256 + h * 128, 128)
                ctx[c * 4 + p, :, cols] = value[:64]
                ctx[8 + c * 4 + p, :, cols] = value[64:]
        for half in range(2):
            ref = region(c, yl, half * 8 + 2 * step, 2)
            copy_to(ref, ref, s_y.at[0], r_y.at[step], y_one).start()
            copy_to(ref, ref, s_o.at[0], r_o.at[0], core).start()

    def pass_on(step):
        arrived(ctx.at[pl.ds(0, 4), :, pl.ds(0, 256)], r_y.at[step])
        for half in range(2):
            ref = region(c, 1 - yl, half * 8 + 2 * step, 2)
            copy_to(ref, ref, s_o.at[0], r_o.at[1], core).start()

    tiles([(0, 0), (1, 0), (1, 1)], c, (0, 2))
    keys_values.from_core(0)
    tiles([(1 - c, 0), (1, 1 - c)], 1 - c)
    put(0)
    tiles([(2, 0), (2, 1), (3, 0), (3, 1)], c)
    keys_values.to_core(1)
    tiles([(2, 0), (2, 1), (3, 0), (3, 1)], 1 - c)
    tiles([(2, 2), (3, 2), (3, 3)], c, (0, 2))
    keys_values.from_core(1)
    tiles([(3 - c, 2), (3, 3 - c)], 1 - c)
    put(1)
    pass_on(0)
    arrived(ctx.at[pl.ds(0, 8), :, pl.ds(0, 256)], r_o.at[0])
    early_sums()
    pass_on(1)
    arrived(ctx.at[pl.ds(0, 8), :, pl.ds(0, 256)], r_o.at[1])

    def finish():
        gone(ctx.at[pl.ds(0, 8), :, pl.ds(0, 256)], s_y.at[0])
        gone(ctx.at[:, :, pl.ds(0, 256)], s_o.at[0])
        keys_values.sent()

    return finish


class Reduce4:
    def __init__(self, z, send, got, more, more_got, s, r):
        self.one, self.two = z + 1 - 2 * lax.rem(z, 2), 3 - z
        self.far = self.two + 1 - 2 * lax.rem(self.two, 2)
        self.send, self.got, self.more, self.more_got, self.s, self.r = send, got, more, more_got, s, r

    def partner(self, part, step):
        return {"z": self.one if part == step else self.two}

    def chunk(self, part, slot):
        return self.far if slot == 1 else (self.two if part else self.one)

    def give(self, part, slot, value):
        self.send[part, slot] = value
        copy_to(
            self.send.at[part, slot], self.got.at[part, slot], self.s.at[0], self.r.at[slot], self.partner(part, 0)
        ).start()

    def pass_on(self, values):
        arrived(self.got.at[0], self.r.at[1])
        for part, value in enumerate(values):
            self.more[part] = (value + self.got[part, 1].astype(F32)).astype(BF)
            copy_to(
                self.more.at[part], self.more_got.at[part], self.s.at[1], self.r.at[2], self.partner(part, 1)
            ).start()

    def own(self, values):
        arrived(self.got.at[0], self.r.at[0])
        arrived(self.more_got, self.r.at[2])
        return [
            value + self.got[part, 0].astype(F32) + self.more_got[part].astype(F32) for part, value in enumerate(values)
        ]

    def sent(self):
        gone(self.send, self.s.at[0])
        gone(self.more, self.s.at[1])


class OutSums:
    def __init__(self, ctx, wo, own_y, own_a, own_b):
        _, yl, _, _, yh = coords()
        self.ctx, self.wo, self.yl = ctx, wo, yl
        self.all = [(own_y, 1 - yh, 1), (own_a.at[0], 0, 0), (own_a.at[1], 1, 0), (own_b, yh, 1)]

    def product(self, n, y):
        _, half, part = self.all[n]
        left = self.wo[part * 4 * OUT[0]:part * 4 * OUT[0] + 4 * OUT[part], lanes(y * 256, 256)]
        right = self.ctx[pl.ds(half * 8, 8), :, lanes(y * 256, 256)].reshape(512, 256)
        value = lax.dot_general(left, right, (((1,), (1,)), ((), ())), preferred_element_type=F32)
        return value.reshape(4, OUT[part], 512)

    def early(self):
        for n, (dst, _, _) in enumerate(self.all):
            dst[...] = self.product(n, self.yl)

    def late(self, n):
        dst = self.all[n][0]
        dst[...] = dst[...] + self.product(n, 1 - self.yl)


def stage_out(
    new_ref, ctx, xs, wo, gain, out_ref, out_sums, own_y, own_a, own_b,
    a_send, a_got, a_more, a_more_got, b_send, b_got, b_more, b_more_got,
    y_send, y_relay, y_got, h_send, h_relay, h_got, total,
    squares, fresh, f1, f2, f1_got, fin,
    a_s, a_r, b_s, b_r, s_y, r_y, s_h, r_h, s_q, r_q, s_f, r_f, s_g, r_g, s_c, r_c,
):
    x, yl, c, z, yh = coords()
    core = {"c": 1 - c}
    y_one, y_two = {"yl": 1 - yl}, {"yl": 1 - yl, "yh": 1 - yh}
    group = [
        {"z": lax.rem(z + dz, 4), "yl": yl + dy - 2 * yl * dy, "c": c + dc - 2 * c * dc}
        for dz in (0, 2, 1, 3) for dy in (0, 1) for dc in (0, 1)
    ]
    group = group[4:] + group[1:4]
    others = [{"x": lax.rem(x + dx, 4)} for dx in (2, 1, 3)]

    one, two = z + 1 - 2 * lax.rem(z, 2), 3 - z
    wanted = (two + 1 - 2 * lax.rem(two, 2), one, two, z)
    out_sums.late(0)
    for n in range(4):
        y_send[n] = own_y[wanted[n]].astype(BF)
    for n in range(4):
        copy_to(y_send.at[n], y_relay.at[n], s_y.at[0], r_y.at[n // 2], y_two if n % 2 else y_one).start()
    first = Reduce4(z, a_send, a_got, a_more, a_more_got, a_s, a_r)
    for part in range(2):
        out_sums.late(1 + part)
        first.give(part, 1, own_a[part, first.chunk(part, 1)].astype(BF))
    for part in range(2):
        first.give(part, 0, own_a[part, first.chunk(part, 0)].astype(BF))
    out_sums.late(3)

    def forward(step):
        arrived(y_relay.at[pl.ds(0, 2)], r_y.at[step])
        for n in (2 * step, 2 * step + 1):
            copy_to(y_relay.at[n], y_got.at[n], s_y.at[1], r_y.at[2 + step], y_one if n % 2 else y_two).start()

    forward(0)
    first.pass_on([own_a[0, first.two], own_a[1, first.one]])
    forward(1)
    second = Reduce4(z, b_send, b_got, b_more, b_more_got, b_s, b_r)
    cols = (slice(0, 256), slice(256, 512))

    def over_y(step):
        arrived(y_got.at[pl.ds(0, 2)], r_y.at[2 + step])
        for n in (2 * step, 2 * step + 1):
            own_b[wanted[n]] = own_b[wanted[n]] + y_got[n].astype(F32)

    over_y(0)
    second.give(0, 1, own_b[wanted[0], :, cols[0]].astype(BF))
    second.give(1, 1, own_b[wanted[0], :, cols[1]].astype(BF))
    second.give(0, 0, own_b[one, :, cols[0]].astype(BF))
    for part, value in enumerate(first.own([own_a[0, z], own_a[1, z]])):
        own_a[part, z] = value
    h_send[...] = own_a[1 - yh, z].astype(BF)
    spans = (slice(0, 80), slice(80, OUT[0]))
    for n, peer in enumerate((y_one, y_two)):
        copy_to(h_send.at[spans[n]], h_relay.at[spans[n]], s_h.at[0], r_h.at[0], peer).start()
    over_y(1)
    second.give(1, 0, own_b[two, :, cols[1]].astype(BF))
    second.pass_on([own_b[two, :, cols[0]], own_b[one, :, cols[1]]])
    arrived(h_relay, r_h.at[0])
    for n, peer in enumerate((y_two, y_one)):
        copy_to(h_relay.at[spans[n]], h_got.at[spans[n]], s_h.at[1], r_h.at[1], peer).start()
    for part, value in enumerate(second.own([own_b[z, :, cols[0]], own_b[z, :, cols[1]]])):
        total[OUT[0]:, cols[part]] = value
    arrived(h_got, r_h.at[1])
    total[:OUT[0], :] = own_a[yh, z] + h_got[...].astype(F32)
    me = z * 4 + yl * 2 + c
    for m in range(4):
        value = total[:, m * 128:(m + 1) * 128]
        squares[me, m:m + 1, :] = jnp.sum(value * value, axis=0, keepdims=True)
    for peer in group:
        copy_to(squares.at[me], squares.at[me], s_q.at[0], r_q.at[0], peer).start()
    lane = lax.broadcasted_iota(jnp.int32, (96, 128), 1)

    def pair(m, part):
        begin, count = BACK[part]
        low = lane[:count] < 64
        at = pl.ds(pl.multiple_of(z * 288 + begin, 32), count)
        a = xs[at, m * 256:m * 256 + 128].astype(F32)
        b = xs[at, m * 256 + 128:m * 256 + 256].astype(F32)
        upper, lower = pltpu.roll(a, 64, 1), pltpu.roll(b, 64, 1)
        return jnp.where(low, jnp.where(yh == 0, a, upper), jnp.where(yh == 0, lower, b))

    for part in range(PARTS):
        for m in range(4):
            fresh[part][m] = pair(m, part)
    arrived(squares.at[pl.ds(0, 15)], r_q.at[0])
    factor = lax.rsqrt(jnp.sum(squares[...], axis=0) * (1.0 / D) + EPS)
    starts, so_far = [], 0
    for j in range(16):
        starts.append(so_far)
        so_far = so_far + new_ref[j]
    here = pl.ds(x * 2, 2)
    for part, (begin, count) in enumerate(BACK):
        rows_of = slice(begin, begin + count)
        low = lane[:count] < 64
        for m in range(4):
            value = total[rows_of, m * 128:(m + 1) * 128] * factor[m:m + 1, :] * gain[rows_of, :]
            fresh[part][m] = fresh[part][m] + value
        for n in range(8):
            sides = []
            for side in range(2):
                j = 2 * n + side
                within = lax.rem(x - starts[j] + 64, 4)
                i = jnp.minimum(lax.div(starts[j] + within - x, 4), 7)
                at = lax.div(i, 2)
                place = lax.rem(i + at, 2) * 4 + at
                value = fresh[part][lax.div(place, 2)]
                value = jnp.where(lax.rem(place, 2) == side, value, pltpu.roll(value, 64, 1))
                sides.append(jnp.where(within < new_ref[j], value, 0.0))
            f1[part][n] = jnp.where(low, sides[0], sides[1]).astype(BF)
        f1_got[part][here] = f1[part][here]
        for peer in others:
            copy_to(
                f1[part].at[pl.ds(peer["x"] * 2, 2)], f1_got[part].at[here], s_f.at[part], r_f.at[part], peer
            ).start()
    mine = [sum([jnp.where(x * 4 + n > m, new_ref[m], 0) for m in range(15)]) for n in range(4)]
    for part, (begin, count) in enumerate(BACK):
        rows_of = slice(begin, begin + count)
        low = lane[:count] < 64
        arrived(f1_got[part].at[pl.ds(0, 6)], r_f.at[part])
        for e in (5, 4, 3, 7, 2, 6, 1, 0):
            dz, dy = e // 2, e % 2
            tz, ty = lax.rem(z + dz, 4), yl + dy - 2 * yl * dy
            sides = []
            for side in range(2):
                start = jnp.where(ty == 0, mine[side], mine[2 + side])
                sides.append(f1_got[part][lax.rem(start + tz, 4) * 2 + ty].astype(F32))
            value = jnp.where(low, sides[0], sides[1]).astype(BF)
            at = z * 2 + yl
            if e == 0:
                fin[at, c, rows_of, :] = value
            else:
                f2[part][e] = value
                copy_to(
                    f2[part].at[e], fin.at[at, c, rows_of], s_g.at[part], r_g.at[part], {"z": tz, "yl": ty}
                ).start()
    for part, (begin, count) in enumerate(BACK):
        rows_of = slice(begin, begin + count)
        arrived(fin.at[pl.ds(0, 7), c, rows_of], r_g.at[part])
        ref = fin.at[:, c, rows_of]
        copy_to(ref, ref, s_c.at[0], r_c.at[0], core).start()
    arrived(fin.at[:, c], r_c.at[0])
    mine_of = lax.broadcasted_iota(jnp.int32, (64, 128), 0) + c * 64
    pick = jnp.where(lane[:64] == mine_of, 1.0, 0.0).astype(BF)
    for n in range(4):
        block = fin[2 * n:2 * n + 2].reshape(1152, 128)
        value = lax.dot_general(pick, block, (((1,), (1,)), ((), ())), preferred_element_type=F32)
        out_ref[:, n * 1152:(n + 1) * 1152] = value.astype(BF)
    first.sent()
    second.sent()
    gone(y_send, s_y.at[0])
    gone(y_relay, s_y.at[1])
    gone(h_send, s_h.at[0])
    gone(h_relay, s_h.at[1])
    gone(squares.at[pl.ds(0, 15)], s_q.at[0])
    for part in range(PARTS):
        gone(f1[part].at[pl.ds(0, 6)], s_f.at[part])
        gone(f2[part].at[pl.ds(0, 7)], s_g.at[part])
    gone(fin.at[:, c], s_c.at[0])


STAGE_IN = [
    VM((1152, 512), BF), VM((1152, 256), BF), VM((1152, 256), BF),
    VM((1152, 128), F32), VM((128, 128), F32), VM((64, 512), F32), VM((64, 512), F32),
    VM((576, 512), BF), [VM((8, count, 128), BF) for _, count in IN], [VM((24, count, 128), BF) for _, count in IN], VM((1152, 1024), BF), VM((16, 8, 128), F32),
    VM((2, 512, 512), F32), VM((2, 512, 512), F32), VM((512, 512), BF), VM((512, 512), BF), VM((2, 512, 512), F32),
    DMA((2,)), DMA((PARTS,)), DMA((4 * PARTS,)), DMA((PARTS,)), DMA((4 * PARTS,)), DMA((PARTS,)), DMA((PARTS,)),
    DMA((2,)), DMA((3,)), DMA((2,)), DMA((3,)), DMA((2 * PARTS,)), DMA((3 * PARTS,)), DMA((1,)), DMA((1,)),
    DMA((1,)), DMA((4,)), DMA((1,)), DMA((4,)),
]
STAGE_ATTEND = [
    VM((4, 256, 128), BF), VM((4, 256, 128), F32), VM((4, 256, 128), F32),
    DMA((1,)), DMA((2,)), DMA((1,)), DMA((2,)),
]
STAGE_OUT = (
    [VM((2, 2, OUT[0], 512), BF), VM((2, 2, OUT[0], 512), BF), VM((2, OUT[0], 512), BF), VM((2, OUT[0], 512), BF)]
    + [VM((2, 2, OUT[1], 256), BF), VM((2, 2, OUT[1], 256), BF), VM((2, OUT[1], 256), BF), VM((2, OUT[1], 256), BF)]
    + [VM((4, OUT[1], 512), BF)] * 3
    + [VM((OUT[0], 512), BF)] * 3
    + [VM((288, 512), F32), VM((16, 4, 128), F32), [VM((4, count, 128), F32) for _, count in BACK]]
    + [[VM((8, count, 128), BF) for _, count in BACK]] * 3
    + [VM((8, 2, 288, 128), BF)]
    + [DMA((2,)), DMA((3,)), DMA((2,)), DMA((3,))]
    + [DMA((2,)), DMA((4,)), DMA((2,)), DMA((2,)), DMA((1,)), DMA((1,)), DMA((PARTS,)), DMA((PARTS,))]
    + [DMA((PARTS,)), DMA((PARTS,)), DMA((1,)), DMA((1,))]
)
SHARED = [
    VM((256, 512), BF), VM((4, 256, 128), BF), VM((1152, 1024), BF), VM((1152, 512), BF), VM((16, 64, 512), BF),
    VM((288, 128), F32), VM((8, 256, 512), BF), DMA((4,)), DMA((6,)), DMA((1,)), DMA((2,)),
    VM((4, OUT[1], 512), F32), VM((2, 4, OUT[0], 512), F32), VM((4, OUT[1], 512), F32),
]


def kernel(old_ref, new_ref, order_ref, xt_in, pre_ref, post_ref, wq_in, wk_in, wv_in, wo_in, out_ref, *scratch):
    q, kv, xs, wo, ctx, gain_out, kvs, s_x, r_x, s_c, r_c, own_y, own_a, own_b = scratch[:14]
    scratch = scratch[14:]
    out_sums = OutSums(ctx, wo, own_y, own_a, own_b)
    keys_values = KeysValues(kv, kvs, s_x, r_x, s_c, r_c)
    own_in, scratch = scratch[:len(STAGE_IN)], scratch[len(STAGE_IN):]
    own_attend, own_out = scratch[:len(STAGE_ATTEND)], scratch[len(STAGE_ATTEND):]
    out_weights, end_in = stage_in(
        old_ref, order_ref, xt_in, pre_ref, post_ref, wq_in, wk_in, wv_in, wo_in, q, kv, xs, wo, gain_out, *own_in,
        keys_values,
    )

    def early_sums():
        out_weights()
        out_sums.early()

    end_attend = stage_attend(q, ctx, keys_values, kvs, early_sums, *own_attend)
    end_in()
    stage_out(new_ref, ctx, xs, wo, gain_out, out_ref, out_sums, own_y, own_a, own_b, *own_out)
    end_attend()


def run(old_blocks, new_blocks, order, xt, pre_gain, post_gain, w_query, w_key, w_value, w_out_t):
    smem = pl.BlockSpec(memory_space=pltpu.SMEM)
    vmem = pl.BlockSpec(memory_space=pltpu.VMEM)
    hbm = pl.BlockSpec(memory_space=pltpu.HBM)
    return pl.pallas_call(
        kernel,
        name="sublayer",
        out_shape=jax.ShapeDtypeStruct((64, D), BF),
        in_specs=[smem, smem, smem, hbm, vmem, vmem, hbm, hbm, hbm, hbm],
        out_specs=vmem,
        scratch_shapes=SHARED + STAGE_IN + STAGE_ATTEND + STAGE_OUT,
        compiler_params=pltpu.CompilerParams(collective_id=0, has_side_effects=True, vmem_limit_bytes=62 * 2**20),
    )(old_blocks, new_blocks, order, xt, pre_gain, post_gain, w_query, w_key, w_value, w_out_t)


def per_device(
    x_old, old_blocks, new_blocks, order, pre_gain, post_gain, w_query, w_key, w_value, w_out_t
):
    return run(
        old_blocks, new_blocks, order, x_old.T, pre_gain.reshape(36, 128), post_gain.reshape(36, 128),
        w_query, w_key, w_value, w_out_t,
    )


def solution(mesh):
    torus = Mesh(mesh.devices.reshape(4, 2, 2, 4, 2), ("x", "yl", "c", "z", "yh"))
    seq, tp = ("x", "yl", "c"), ("z", "yh")
    both = P(seq, tp)
    in_specs = (both, P(), P(), P(), P(), P(), both, both, both, both)
    return jax.shard_map(
        per_device, mesh=torus, in_specs=in_specs, out_specs=P(seq + tp, None), check_vma=False
    )
```
